32 devices in a mesh: dp: 8 (over z, y), seq: 4 (over x, core).
Axes of the slice: x: 2, y: 2, z: 4, core: 2. Of those that a mesh axis runs over, the one named last changes fastest.
Arguments:
- inputs: bfloat16 [48, 1024, 256], P('dp', 'seq')
- cotangent: bfloat16 [48, 1024, 256], P('dp', 'seq')
- owner_list: int32 [7], replicated, may hold values from 0 to 7, as said below
- master_rows: float32 [8, 524288], P('dp'), as said below
- moment1_rows: float32 [8, 524288], P('dp'), as said below
- moment2_rows: float32 [8, 524288], P('dp'), as said below
Outputs:
- final_state: float32 [48, 1024, 256], P('dp', 'seq')
- input_grad: float32 [48, 1024, 256], P('dp', 'seq')
- state_stats: float32 [2, 48], replicated
- new_moment1: float32 [8, 524288], P('dp')
- new_moment2: float32 [8, 524288], P('dp')
- new_master: float32 [8, 524288], P('dp')
The draws below stay inside these ranges and needn't reach their ends.
Inputs may be any that keep to these rules, and one draw needn't show every extreme that they name: Tensor t goes to dp index owner_list[t]. W_up and W_down share one owner that holds no other tensor, so the busiest owner holds 524288 entries; the other five tensors are dealt among the other indices, several may share one. `master_rows`: entries of a row beyond the tensors its owner holds are not read. `moment1_rows`: entries of a row beyond the tensors its owner holds are not read. `moment2_rows`: Positive. Entries beyond the tensors an owner holds are not read.
All inputs are finite; a program needn't handle non-finite values.
Results may differ from the reference program's by a relative error of at most 0.02.
The reference program's roundings to bfloat16 on the way count: a program that leaves them out, or rounds other values in their place, can miss the bound.
Values may be sent and summed in bfloat16 or wider, within the bound.
A program may use at most 192 MiB of HBM per device.

```python
import math
from functools import partial
import jax
import jax.numpy as jnp
from jax import lax

D = 256
HEADS = 4
HD = 64
FF = 1024
LOOPS = 2
STEP = 3
LEN = 1024
SEQS = 48
TOKENS = 49152
OWNERS = 8
SMALL = 9
CAP = 524288


grad_factors = [0.2, 0.2, 0.6, 0.6, 1.0, 0.8, 1.5]


def tensor_shapes_drawn():
    return [(D, D), (D, D), (D, D), (D, D), (D, FF), (FF, D), (SMALL, D)]


def owner_starts_drawn(owner_list):
    shapes = tensor_shapes_drawn()
    starts = []
    for tensor_id in range(7):
        offset = jnp.zeros((), jnp.int32)
        for earlier in range(tensor_id):
            shared = (owner_list[earlier] == owner_list[tensor_id]).astype(jnp.int32)
            offset = offset + shared * (shapes[earlier][0] * shapes[earlier][1])
        starts.append(offset)
    return starts


def owners_from(key):
    inner = jax.random.fold_in(key, 11)
    heavy_key, other_key = jax.random.split(inner)
    heavy = jax.random.randint(heavy_key, (), 0, OWNERS, dtype=jnp.int32)
    others = jax.random.randint(other_key, (5,), 0, OWNERS - 1, dtype=jnp.int32)
    others = others + (others >= heavy).astype(jnp.int32)
    return jnp.concatenate([others[:4], jnp.stack([heavy, heavy]), others[4:]])


def place(background, pieces, owner_list):
    starts = owner_starts_drawn(owner_list)
    filled = background
    for tensor_id in range(7):
        filled = lax.dynamic_update_slice(filled, pieces[tensor_id].reshape(1, -1), (owner_list[tensor_id], starts[tensor_id]))
    return filled


def signed_factor(key, shape):
    sign_key, size_key = jax.random.split(key)
    signs = jnp.where(jax.random.bernoulli(sign_key, 0.5, shape), 1.0, -1.0)
    return signs * jax.random.uniform(size_key, shape, jnp.float32, 0.5, 1.5)


def draw_owner_list(key, part):
    return owners_from(key)


def draw_master_rows(key, part):
    owner_list = owners_from(key)
    inner = jax.random.fold_in(key, 103)
    shapes = tensor_shapes_drawn()
    scales = [1.5 * D ** (-0.5), 1.5 * D ** (-0.5), D ** (-0.5), 3.0 * D ** (-0.5), D ** (-0.5), FF ** (-0.5)]
    pieces = []
    for tensor_id in range(6):
        pieces.append(scales[tensor_id] * jax.random.normal(jax.random.fold_in(inner, tensor_id), shapes[tensor_id], jnp.float32))
    noise = jax.random.normal(jax.random.fold_in(inner, 6), (SMALL, D), jnp.float32)
    row_ids = jnp.arange(SMALL)
    gain_rows = (row_ids == 0) | (row_ids == 2)
    pieces.append(jnp.where(gain_rows[:, None], 1.0 + 0.15 * jnp.clip(noise, -2.0, 2.0), 0.3 * noise))
    background = 0.05 * jax.random.normal(jax.random.fold_in(inner, 7), (OWNERS, CAP), jnp.float32)
    return place(background, pieces, owner_list)


def draw_moment1_rows(key, part):
    owner_list = owners_from(key)
    inner = jax.random.fold_in(key, 101)
    shapes = tensor_shapes_drawn()
    scale_root = math.sqrt(TOKENS)
    pieces = []
    for tensor_id in range(7):
        pieces.append(grad_factors[tensor_id] * scale_root * signed_factor(jax.random.fold_in(inner, tensor_id), shapes[tensor_id]))
    background = 0.5 * scale_root * signed_factor(jax.random.fold_in(inner, 7), (OWNERS, CAP))
    return place(background, pieces, owner_list)


def draw_moment2_rows(key, part):
    owner_list = owners_from(key)
    inner = jax.random.fold_in(key, 102)
    shapes = tensor_shapes_drawn()
    pieces = []
    for tensor_id in range(7):
        magnitude = grad_factors[tensor_id] ** 2 * TOKENS
        factor = jnp.exp(jax.random.uniform(jax.random.fold_in(inner, tensor_id), shapes[tensor_id], jnp.float32, 0.0, math.log(4.0)))
        pieces.append(magnitude * factor)
    background = 0.25 * TOKENS * jnp.exp(jax.random.uniform(jax.random.fold_in(inner, 7), (OWNERS, CAP), jnp.float32, 0.0, math.log(4.0)))
    return place(background, pieces, owner_list)


def draw_inputs(key, part):
    inner = jax.random.fold_in(key, 201)
    base_key = jax.random.fold_in(inner, 0)
    ramp = 0.6 * jnp.exp(math.log(3.0) * jnp.arange(LEN, dtype=jnp.float32) / max(LEN - 1, 1))
    base = jax.random.normal(base_key, (SEQS, LEN, D), jnp.float32)
    return (base * ramp[None, :, None]).astype(jnp.bfloat16)


def draw_cotangent(key, part):
    inner = jax.random.fold_in(key, 301)
    base_key = jax.random.fold_in(inner, 0)
    ramp = 0.6 * jnp.exp(math.log(3.0) * jnp.arange(SEQS, dtype=jnp.float32) / max(SEQS - 1, 1))
    base = jax.random.normal(base_key, (SEQS, LEN, D), jnp.float32)
    return (base * ramp[:, None, None]).astype(jnp.bfloat16)


def setup_inputs(seed: int = 0) -> dict:
    arg_keys = jax.random.split(jax.random.key(seed), 7)
    inputs = draw_inputs(jax.random.fold_in(arg_keys[6], 71), 0)
    cotangent = draw_cotangent(jax.random.fold_in(arg_keys[6], 71), 0)
    owner_list = draw_owner_list(jax.random.fold_in(arg_keys[6], 71), 0)
    master_rows = draw_master_rows(jax.random.fold_in(arg_keys[6], 71), 0)
    moment1_rows = draw_moment1_rows(jax.random.fold_in(arg_keys[6], 71), 0)
    moment2_rows = draw_moment2_rows(jax.random.fold_in(arg_keys[6], 71), 0)
    return dict(inputs=inputs, cotangent=cotangent, owner_list=owner_list, master_rows=master_rows, moment1_rows=moment1_rows, moment2_rows=moment2_rows)


@jax.custom_vjp
def low(v):
    return lax.optimization_barrier(v.astype(jnp.bfloat16)).astype(jnp.float32)

@jax.custom_vjp
def low_back(v):
    return v

def low_keep(v):
    return (low(v), None)

def low_pass(kept, grad):
    return (grad,)

def back_keep(v):
    return (v, None)

def back_low(kept, grad):
    return (low(grad),)
low.defvjp(low_keep, low_pass)
low_back.defvjp(back_keep, back_low)
norm_eps = 1e-05
stat_eps = 1e-06
adam_eps = 1e-08
masked_score = -1e+30
highest = lax.Precision.HIGHEST

def tensor_shapes():
    return [(D, D), (D, D), (D, D), (D, D), (D, FF), (FF, D), (SMALL, D)]

def owner_starts(owner_list):
    shapes = tensor_shapes()
    starts = []
    for tensor_id in range(7):
        offset = jnp.zeros((), jnp.int32)
        for earlier in range(tensor_id):
            shared = (owner_list[earlier] == owner_list[tensor_id]).astype(jnp.int32)
            offset = offset + shared * (shapes[earlier][0] * shapes[earlier][1])
        starts.append(offset)
    return starts

def layer_norm(values, norm_gain, norm_shift):
    average = lax.optimization_barrier(jnp.mean(values, axis=-1, keepdims=True))
    centered = values - average
    spread = lax.optimization_barrier(jnp.mean(centered * centered, axis=-1, keepdims=True))
    return centered * lax.rsqrt(spread + norm_eps) * norm_gain + norm_shift

def matmul(first_operand, second_operand):
    return jnp.einsum('gtd,de->gte', first_operand, second_operand, precision=highest)

def attend(parts):
    queries, keys_part, values_part = parts
    length = queries.shape[0]
    scores = jnp.einsum('qhd,khd->hqk', queries, keys_part, precision=highest) * HD ** (-0.5)
    causal = jnp.arange(length)[:, None] >= jnp.arange(length)[None, :]
    scores = low_back(jnp.where(causal[None], scores, masked_score))
    attention_probs = low(jax.nn.softmax(scores, axis=-1))
    return jnp.einsum('hqk,khd->qhd', attention_probs, values_part, precision=highest)

def loop_block(loop_state, weights):
    w_query, w_key, w_value, output_weight, up_weight, down_weight, small_piece = weights
    group_size = loop_state.shape[0]
    normalized_input = low(layer_norm(loop_state, small_piece[0], small_piece[1]))
    queries = low(low_back(matmul(normalized_input, w_query)))
    keys_part = low(low_back(matmul(normalized_input, w_key)))
    values_part = low(low_back(matmul(normalized_input, w_value)))
    head_shape = (group_size, LEN, HEADS, HD)
    attention_output = lax.map(jax.checkpoint(attend), (queries.reshape(head_shape), keys_part.reshape(head_shape), values_part.reshape(head_shape)))
    attention_output = low(low_back(attention_output.reshape(group_size, LEN, D)))
    middle_state = loop_state + low_back(matmul(attention_output, output_weight))
    normalized_middle = low(layer_norm(middle_state, small_piece[2], small_piece[3]))
    before = low_back(matmul(normalized_middle, up_weight) + small_piece[5:].reshape(FF))
    hidden_units = low(jax.nn.gelu(before, approximate=False))
    return middle_state + low_back(matmul(hidden_units, down_weight) + small_piece[4])

def loss_of(target_block, start_block, params):
    rounded = [low(matrix) for matrix in params[:6]] + [params[6]]
    first_state = loop_block(start_block, rounded)
    second_state = loop_block(first_state + start_block, rounded)
    return (jnp.sum(target_block * second_state), (first_state, second_state))

def root_mean(loop_state):
    return jnp.sqrt(lax.optimization_barrier(jnp.mean(loop_state * loop_state, axis=(1, 2))) + stat_eps)

def reference(inputs, cotangent, owner_list, master_rows, moment1_rows, moment2_rows):
    shapes = tensor_shapes()
    starts = owner_starts(owner_list)
    masters = []
    for tensor_id in range(7):
        entries = shapes[tensor_id][0] * shapes[tensor_id][1]
        sliced = lax.dynamic_slice(master_rows, (owner_list[tensor_id], starts[tensor_id]), (1, entries))
        masters.append(sliced.reshape(shapes[tensor_id]))
    group_size = 4
    group_count = SEQS // group_size
    source = inputs.astype(jnp.float32).reshape(group_count, group_size, LEN, D)
    target = cotangent.astype(jnp.float32).reshape(group_count, group_size, LEN, D)

    def group_step(totals, item):
        start_block, target_block = item
        loss_value, pullback, states = jax.vjp(partial(loss_of, target_block), start_block, masters, has_aux=True)
        start_grad, param_grads = pullback(jnp.ones((), loss_value.dtype))
        totals = [total + gradient for total, gradient in zip(totals, param_grads)]
        stats = jnp.stack([root_mean(states[0]), root_mean(states[1])])
        return (totals, (states[1], start_grad, stats))
    zero_totals = [jnp.zeros(shape, jnp.float32) for shape in shapes]
    totals, outputs = lax.scan(group_step, zero_totals, (source, target))
    final_state = outputs[0].reshape(SEQS, LEN, D)
    input_grad = outputs[1].reshape(SEQS, LEN, D)
    state_stats = jnp.transpose(outputs[2], (1, 0, 2)).reshape(LOOPS, SEQS)
    learning_rates = [D ** (-0.5)] * 5 + [FF ** (-0.5), 0.5]
    decays_list = [0.1] * 6 + [0.0]
    correction = 1.0 - 0.5 ** STEP
    new_moment1 = jnp.zeros_like(moment1_rows)
    new_moment2 = jnp.zeros_like(moment2_rows)
    new_master = jnp.zeros_like(master_rows)
    for tensor_id in range(7):
        entries = shapes[tensor_id][0] * shapes[tensor_id][1]
        corner = (owner_list[tensor_id], starts[tensor_id])
        gradient = totals[tensor_id].reshape(1, entries)
        old_first = lax.dynamic_slice(moment1_rows, corner, (1, entries))
        old_second = lax.dynamic_slice(moment2_rows, corner, (1, entries))
        old_weight = lax.dynamic_slice(master_rows, corner, (1, entries))
        first_new = 0.5 * old_first + 0.5 * gradient
        second_new = 0.5 * old_second + 0.5 * gradient * gradient
        update = first_new / correction / (jnp.sqrt(second_new / correction) + adam_eps) + decays_list[tensor_id] * old_weight
        weight_new = old_weight - learning_rates[tensor_id] * update
        new_moment1 = lax.dynamic_update_slice(new_moment1, first_new, corner)
        new_moment2 = lax.dynamic_update_slice(new_moment2, second_new, corner)
        new_master = lax.dynamic_update_slice(new_master, weight_new, corner)
    return (final_state, input_grad, state_stats, new_moment1, new_moment2, new_master)
```

```python
import math
from functools import partial

import jax
import jax.numpy as jnp
from jax import lax
from jax.experimental import pallas as pl
from jax.experimental.pallas import tpu as pltpu
from jax.sharding import PartitionSpec as P

D = 256
HEADS = 4
HD = 64
FF = 1024
STEP = 3
SMALL = 9
BLK = 256
OWN = 4
UNITS = 6
ALL = 8
F32 = jnp.float32
BF16 = jnp.bfloat16
MESH = pl.DeviceIdType.MESH

norm_eps = 1e-05
stat_eps = 1e-06
adam_eps = 1e-08
masked_score = -1e30


def dot(left, right):
    return lax.dot_general(left, right, (((1,), (0,)), ((), ())), preferred_element_type=F32)


def dot_nt(left, right):
    return lax.dot_general(left, right, (((1,), (1,)), ((), ())), preferred_element_type=F32)


def wide(column):
    return jnp.concatenate([column, column], axis=1)


def fold(values):
    return values[:, :128] + values[:, 128:]


def standardize(values):
    average = jnp.mean(values, axis=0, keepdims=True)
    centered = values - average
    spread = jnp.mean(centered * centered, axis=0, keepdims=True)
    inverse = lax.rsqrt(spread + norm_eps)
    return centered * inverse, inverse


def standardize_back(grad, unit_values, inverse):
    average = jnp.mean(grad, axis=0, keepdims=True)
    inner = jnp.mean(grad * unit_values, axis=0, keepdims=True)
    return (grad - average - unit_values * inner) * inverse


def param(small_ref, row):
    return wide(small_ref[row * D : (row + 1) * D, :])


def gelu_parts(e):
    cdf = 0.5 * lax.erf(e * math.sqrt(0.5)) + 0.5
    hid = e * cdf
    slope = cdf + e * (jnp.exp(-0.5 * e * e) * (1.0 / math.sqrt(2.0 * math.pi)))
    return hid, slope


def full(shape):
    return pl.BlockSpec(shape, lambda *args: (0,) * len(shape), pipeline_mode=pl.Buffered(1))


def params_of(ndims=1, mib=56):
    return pltpu.CompilerParams(
        dimension_semantics=("arbitrary",) * ndims, vmem_limit_bytes=mib << 20
    )


def cost(flops, nbytes, trans=0):
    return pl.CostEstimate(flops=int(flops), bytes_accessed=int(nbytes), transcendentals=int(trans))


def project(a, wt_ref, q_ref, kt_ref, vt_ref, k_ref, v_ref):
    q_ref[0] = (dot(wt_ref[0:D], a) * HD ** (-0.5)).astype(BF16)
    kt = dot(wt_ref[D : 2 * D], a).astype(BF16)
    kt_ref[0] = kt
    k_ref[0] = kt.T
    vt = dot(wt_ref[2 * D : 3 * D], a).astype(BF16)
    vt_ref[0] = vt
    v_ref[0] = vt.T


def first_body(x_ref, small_ref, wt_ref, xt_ref, a_ref, q_ref, kt_ref, vt_ref, k_ref, v_ref):
    xt = x_ref[0].T
    xt_ref[0] = xt
    unit_values, _ = standardize(xt.astype(F32))
    a = (unit_values * param(small_ref, 0) + param(small_ref, 1)).astype(BF16)
    a_ref[0] = a
    project(a, wt_ref, q_ref, kt_ref, vt_ref, k_ref, v_ref)


def second_body(a_ref, wt_ref, q_ref, kt_ref, vt_ref, k_ref, v_ref):
    project(a_ref[0], wt_ref, q_ref, kt_ref, vt_ref, k_ref, v_ref)


def tile_spec(blocks=None):
    if blocks is None:
        return pl.BlockSpec((1, BLK, BLK), lambda j, *t: (j, 0, 0))
    return blocks


def first_projection(x, small, wt):
    tile = pl.BlockSpec((1, BLK, BLK), lambda j: (j, 0, 0))
    out = jax.ShapeDtypeStruct((ALL, BLK, BLK), BF16)
    return pl.pallas_call(
        first_body,
        grid=(ALL,),
        in_specs=[tile, full(small.shape), full(wt.shape)],
        out_specs=[tile] * 7,
        out_shape=[out] * 7,
        compiler_params=params_of(),
        cost_estimate=cost(2 * 2048 * 256 * 768, 9 << 20),
        name="first_projection",
    )(x, small, wt)


def second_projection(a, wt):
    tile = pl.BlockSpec((1, BLK, BLK), lambda j: (j, 0, 0))
    out = jax.ShapeDtypeStruct((ALL, BLK, BLK), BF16)
    return pl.pallas_call(
        second_body,
        grid=(ALL,),
        in_specs=[tile, full(wt.shape)],
        out_specs=[tile] * 5,
        out_shape=[out] * 5,
        compiler_params=params_of(),
        cost_estimate=cost(2 * 2048 * 256 * 768, 6 << 20),
        name="second_projection",
    )(a, wt)


def head_rows(values, half):
    rows = lax.broadcasted_iota(jnp.int32, values.shape, 0)
    keep = (rows < HD) if half == 0 else (rows >= HD)
    return jnp.where(keep, values, jnp.zeros_like(values))


def causal_mask():
    keys = lax.broadcasted_iota(jnp.int32, (BLK, BLK), 0)
    queries = lax.broadcasted_iota(jnp.int32, (BLK, BLK), 1)
    return keys <= queries


def attend_body(table, q_ref, k_ref, vt_ref, o_ref, log_ref, score_ref):
    unit = pl.program_id(1)
    base = table[UNITS + unit]
    place = table[2 * UNITS + unit]

    def branch(last):
        for half in range(2):
            lo, hi = half * HD, (half + 1) * HD
            q = head_rows(q_ref[0], half)
            top = None
            for kb in range(last + 1):
                score = dot(k_ref[base + kb], q)
                if kb == last:
                    score = jnp.where(causal_mask(), score, masked_score)
                score_ref[half, kb] = score
                peak = jnp.max(score, axis=0, keepdims=True)
                top = peak if top is None else jnp.maximum(top, peak)
            total = jnp.zeros((1, BLK), F32)
            acc = jnp.zeros((HD, BLK), F32)
            for kb in range(last + 1):
                weight = jnp.exp(score_ref[half, kb] - top)
                total = total + jnp.sum(weight, axis=0, keepdims=True)
                acc = acc + dot(vt_ref[base + kb, lo:hi, :], weight.astype(BF16))
            o_ref[0, lo:hi, :] = (acc / total).astype(BF16)
            log_ref[0, 0, half : half + 1, :] = top + jnp.log(total)

    for last in range(OWN):
        pl.when(place == last)(partial(branch, last))


def attend(table, q, k, vt):
    spec = pltpu.PrefetchScalarGridSpec(
        num_scalar_prefetch=1,
        grid=(2, UNITS),
        in_specs=[
            pl.BlockSpec((1, 128, BLK), lambda h, u, t: (t[u], h, 0)),
            pl.BlockSpec((ALL, BLK, 128), lambda h, u, t: (0, 0, h)),
            pl.BlockSpec((ALL, 128, BLK), lambda h, u, t: (0, h, 0)),
        ],
        out_specs=[
            pl.BlockSpec((1, 128, BLK), lambda h, u, t: (u, h, 0)),
            pl.BlockSpec((1, 1, 8, BLK), lambda h, u, t: (u, h, 0, 0)),
        ],
        scratch_shapes=[pltpu.VMEM((2, OWN, BLK, BLK), F32)],
    )
    return pl.pallas_call(
        attend_body,
        grid_spec=spec,
        out_shape=[
            jax.ShapeDtypeStruct((UNITS, BLK, BLK), BF16),
            jax.ShapeDtypeStruct((UNITS, 2, 8, BLK), F32),
        ],
        compiler_params=params_of(2),
        cost_estimate=cost(4 * 4 * 15 * BLK * BLK * HD, 5 << 20, 4 * 15 * BLK * BLK),
        name="attend",
    )(table, q, k, vt)


def attend_back_body(
    table, q_ref, k_ref, kt_ref, v_ref, go_ref, o_ref, log_ref, dq_ref, dk_ref, dv_ref, dk_acc, dv_acc
):
    unit = pl.program_id(1)
    base = table[UNITS + unit]
    place = table[2 * UNITS + unit]

    @pl.when(unit == 0)
    def _():
        dk_acc[...] = jnp.zeros_like(dk_acc)
        dv_acc[...] = jnp.zeros_like(dv_acc)

    def branch(last):
        for half in range(2):
            lo, hi = half * HD, (half + 1) * HD
            q = head_rows(q_ref[0], half)
            go = head_rows(go_ref[0], half)
            q_head = q_ref[0, lo:hi, :]
            go_head = go_ref[0, lo:hi, :]
            log_total = log_ref[0, 0, half : half + 1, :]
            inner = jnp.sum(
                go_head.astype(F32) * o_ref[0, lo:hi, :].astype(F32), axis=0, keepdims=True
            )
            dq = jnp.zeros((HD, BLK), F32)
            for kb in range(last + 1):
                score = dot(k_ref[base + kb], q)
                if kb == last:
                    score = jnp.where(causal_mask(), score, masked_score)
                weight = jnp.exp(score - log_total)
                slope = dot(v_ref[base + kb], go)
                dscore = (weight * (slope - inner)).astype(BF16)
                dv_acc[base + kb, lo:hi, :] += dot_nt(go_head, weight.astype(BF16))
                dk_acc[base + kb, lo:hi, :] += dot_nt(q_head, dscore)
                dq = dq + dot(kt_ref[base + kb, lo:hi, :], dscore)
            dq_ref[0, lo:hi, :] = (dq * HD ** (-0.5)).astype(BF16)

    for last in range(OWN):
        pl.when(place == last)(partial(branch, last))

    @pl.when(unit == UNITS - 1)
    def _():
        dk_ref[...] = dk_acc[...].astype(BF16)
        dv_ref[...] = dv_acc[...].astype(BF16)


def attend_back(table, q, k, kt, v, go, o, log_total):
    spec = pltpu.PrefetchScalarGridSpec(
        num_scalar_prefetch=1,
        grid=(2, UNITS),
        in_specs=[
            pl.BlockSpec((1, 128, BLK), lambda h, u, t: (t[u], h, 0)),
            pl.BlockSpec((ALL, BLK, 128), lambda h, u, t: (0, 0, h)),
            pl.BlockSpec((ALL, 128, BLK), lambda h, u, t: (0, h, 0)),
            pl.BlockSpec((ALL, BLK, 128), lambda h, u, t: (0, 0, h)),
            pl.BlockSpec((1, 128, BLK), lambda h, u, t: (u, h, 0)),
            pl.BlockSpec((1, 128, BLK), lambda h, u, t: (u, h, 0)),
            pl.BlockSpec((1, 1, 8, BLK), lambda h, u, t: (u, h, 0, 0)),
        ],
        out_specs=[
            pl.BlockSpec((1, 128, BLK), lambda h, u, t: (u, h, 0)),
            pl.BlockSpec((ALL, 128, BLK), lambda h, u, t: (0, h, 0)),
            pl.BlockSpec((ALL, 128, BLK), lambda h, u, t: (0, h, 0)),
        ],
        scratch_shapes=[pltpu.VMEM((ALL, 128, BLK), F32)] * 2,
    )
    return pl.pallas_call(
        attend_back_body,
        grid_spec=spec,
        out_shape=[
            jax.ShapeDtypeStruct((UNITS, BLK, BLK), BF16),
            jax.ShapeDtypeStruct((ALL, BLK, BLK), BF16),
            jax.ShapeDtypeStruct((ALL, BLK, BLK), BF16),
        ],
        compiler_params=params_of(2),
        cost_estimate=cost(10 * 4 * 15 * BLK * BLK * HD, 8 << 20, 4 * 15 * BLK * BLK),
        name="attend_back",
    )(table, q, k, kt, v, go, o, log_total)


def middle(z, o_ref, wot_ref, small_ref):
    r = z + dot(wot_ref[...], o_ref[0])
    unit_values, inverse = standardize(r)
    m = (unit_values * param(small_ref, 2) + param(small_ref, 3)).astype(BF16)
    return r, unit_values, inverse, m


def feed_first_body(
    table, xt_ref, o_ref, small_ref, wot_ref, wut_ref, wdt_ref, r_ref, hid_ref, slope_ref, z_ref, a_ref, sq_ref
):
    x = xt_ref[0].astype(F32)
    r, _, _, m = middle(x, o_ref, wot_ref, small_ref)
    r_ref[0] = r
    out = r + param(small_ref, 4)
    for c in range(FF // BLK):
        rows = slice(c * BLK, (c + 1) * BLK)
        e = dot(wut_ref[rows, :], m) + param(small_ref, 5 + c)
        hid, slope = gelu_parts(e)
        hid = hid.astype(BF16)
        hid_ref[0, rows, :] = hid
        slope_ref[0, rows, :] = slope.astype(BF16)
        out = out + dot(wdt_ref[:, rows], hid)
    sq_ref[0] = jnp.broadcast_to(jnp.sum(out * out, axis=0, keepdims=True), (8, BLK))
    z = out + x
    z_ref[0] = z
    unit_values, _ = standardize(z)
    a_ref[0] = (unit_values * param(small_ref, 0) + param(small_ref, 1)).astype(BF16)


def feed_first(table, xt, o, small, wot, wut, wdt):
    spec = pltpu.PrefetchScalarGridSpec(
        num_scalar_prefetch=1,
        grid=(UNITS,),
        in_specs=[
            pl.BlockSpec((1, BLK, BLK), lambda u, t: (t[u], 0, 0)),
            pl.BlockSpec((1, BLK, BLK), lambda u, t: (u, 0, 0)),
            full(small.shape),
            full(wot.shape),
            full(wut.shape),
            full(wdt.shape),
        ],
        out_specs=[
            pl.BlockSpec((1, BLK, BLK), lambda u, t: (u, 0, 0)),
            pl.BlockSpec((1, FF, BLK), lambda u, t: (u, 0, 0)),
            pl.BlockSpec((1, FF, BLK), lambda u, t: (u, 0, 0)),
            pl.BlockSpec((1, BLK, BLK), lambda u, t: (u, 0, 0)),
            pl.BlockSpec((1, BLK, BLK), lambda u, t: (u, 0, 0)),
            pl.BlockSpec((1, 8, BLK), lambda u, t: (u, 0, 0)),
        ],
    )
    tile = (UNITS, BLK, BLK)
    return pl.pallas_call(
        feed_first_body,
        grid_spec=spec,
        out_shape=[
            jax.ShapeDtypeStruct(tile, F32),
            jax.ShapeDtypeStruct((UNITS, FF, BLK), BF16),
            jax.ShapeDtypeStruct((UNITS, FF, BLK), BF16),
            jax.ShapeDtypeStruct(tile, F32),
            jax.ShapeDtypeStruct(tile, BF16),
            jax.ShapeDtypeStruct((UNITS, 8, BLK), F32),
        ],
        compiler_params=params_of(),
        cost_estimate=cost(2 * 1536 * 256 * 2304, 14 << 20),
        name="feed_first",
    )(table, xt, o, small, wot, wut, wdt)


def feed_back_tail(
    g, gy, r_unit, r_inv, m, o, small_ref, parts, wu_ref, wd_ref, wo_ref, gr_ref, go_ref, gd_acc, gu_acc, go_acc, tail_acc
):
    tail_acc[2 * D : 3 * D, :] += fold(gy.astype(F32))
    gm = jnp.zeros((D, BLK), F32)
    for c in range(FF // BLK):
        rows = slice(c * BLK, (c + 1) * BLK)
        hid, slope = parts(c)
        gd_acc[rows, :] += dot_nt(hid, gy)
        ge = (dot(wd_ref[rows, :], gy) * slope).astype(BF16)
        gu_acc[:, rows] += dot_nt(m, ge)
        tail_acc[3 * D + c * BLK : 3 * D + (c + 1) * BLK, :] += fold(ge.astype(F32))
        gm = gm + dot(wu_ref[:, rows], ge)
    tail_acc[0:D, :] += fold(gm * r_unit)
    tail_acc[D : 2 * D, :] += fold(gm)
    gr = g + standardize_back(gm * param(small_ref, 2), r_unit, r_inv)
    gr_ref[0] = gr
    ga = gr.astype(BF16)
    go_acc[...] += dot_nt(o, ga)
    go_ref[0] = dot(wo_ref[...], ga).astype(BF16)


def feed_second_body(
    z_ref, o_ref, cot_ref, small_ref, wot_ref, wut_ref, wdt_ref, wo_ref, wu_ref, wd_ref,
    final_ref, sq_ref, gr_ref, go_ref, gd_acc, gu_acc, go_acc, tail_acc, hid_buf, slope_buf,
):
    @pl.when(pl.program_id(0) == 0)
    def _():
        for acc in (gd_acc, gu_acc, go_acc, tail_acc):
            acc[...] = jnp.zeros_like(acc)

    r, r_unit, r_inv, m = middle(z_ref[0], o_ref, wot_ref, small_ref)
    out = r + param(small_ref, 4)
    for c in range(FF // BLK):
        rows = slice(c * BLK, (c + 1) * BLK)
        e = dot(wut_ref[rows, :], m) + param(small_ref, 5 + c)
        hid, slope = gelu_parts(e)
        hid = hid.astype(BF16)
        hid_buf[rows, :] = hid
        slope_buf[rows, :] = slope
        out = out + dot(wdt_ref[:, rows], hid)
    sq_ref[0] = jnp.broadcast_to(jnp.sum(out * out, axis=0, keepdims=True), (8, BLK))
    final_ref[0] = out.T.astype(BF16)
    gy = cot_ref[0].T
    feed_back_tail(
        gy.astype(F32), gy, r_unit, r_inv, m, o_ref[0], small_ref,
        lambda c: (hid_buf[c * BLK : (c + 1) * BLK, :], slope_buf[c * BLK : (c + 1) * BLK, :]),
        wu_ref, wd_ref, wo_ref, gr_ref, go_ref, gd_acc, gu_acc, go_acc, tail_acc,
    )


TAIL = 3 * D + FF


def feed_second(z, o, cot, small, wot, wut, wdt, wo, wu, wd):
    tile = pl.BlockSpec((1, BLK, BLK), lambda u: (u, 0, 0))
    whole = lambda shape: pl.BlockSpec(shape, lambda u: (0,) * len(shape))
    return pl.pallas_call(
        feed_second_body,
        grid=(UNITS,),
        in_specs=[tile, tile, tile] + [full(w.shape) for w in (small, wot, wut, wdt, wo, wu, wd)],
        out_specs=[
            tile,
            pl.BlockSpec((1, 8, BLK), lambda u: (u, 0, 0)),
            tile,
            tile,
            whole((FF, D)),
            whole((D, FF)),
            whole((D, D)),
            whole((TAIL, 128)),
        ],
        out_shape=[
            jax.ShapeDtypeStruct((UNITS, BLK, BLK), BF16),
            jax.ShapeDtypeStruct((UNITS, 8, BLK), F32),
            jax.ShapeDtypeStruct((UNITS, BLK, BLK), F32),
            jax.ShapeDtypeStruct((UNITS, BLK, BLK), BF16),
            jax.ShapeDtypeStruct((FF, D), F32),
            jax.ShapeDtypeStruct((D, FF), F32),
            jax.ShapeDtypeStruct((D, D), F32),
            jax.ShapeDtypeStruct((TAIL, 128), F32),
        ],
        scratch_shapes=[pltpu.VMEM((FF, BLK), BF16), pltpu.VMEM((FF, BLK), F32)],
        compiler_params=params_of(),
        cost_estimate=cost(2 * 1536 * 256 * 2304 * 3, 12 << 20),
        name="feed_second",
    )(z, o, cot, small, wot, wut, wdt, wo, wu, wd)


def project_back(z, a, dq, dk, dv, gr, small_ref, wqkv_ref, gqkv_acc, head_acc):
    grad = dot(wqkv_ref[0], dq) + dot(wqkv_ref[1], dk) + dot(wqkv_ref[2], dv)
    gqkv_acc[0] += dot_nt(a, dq)
    gqkv_acc[1] += dot_nt(a, dk)
    gqkv_acc[2] += dot_nt(a, dv)
    unit_values, inverse = standardize(z)
    head_acc[0:D, :] += fold(grad * unit_values)
    head_acc[D : 2 * D, :] += fold(grad)
    return gr + standardize_back(grad * param(small_ref, 0), unit_values, inverse)


def turn_body(
    table, dq_ref, dk_ref, dv_ref, a_ref, z_ref, gr_ref, hid_ref, slope_ref, r_ref, o_ref, small_ref, wqkv_ref,
    wo_ref, wu_ref, wd_ref, gd_in, gu_in, go_in, tail_in,
    gz_ref, gr_out, go_out, gd_acc, gu_acc, go_acc, tail_acc, gqkv_acc, head_acc,
):
    @pl.when(pl.program_id(0) == 0)
    def _():
        gd_acc[...] = gd_in[...]
        gu_acc[...] = gu_in[...]
        go_acc[...] = go_in[...]
        tail_acc[...] = tail_in[...]
        gqkv_acc[...] = jnp.zeros_like(gqkv_acc)
        head_acc[...] = jnp.zeros_like(head_acc)

    g = project_back(
        z_ref[0], a_ref[0], dq_ref[0], dk_ref[0], dv_ref[0], gr_ref[0], small_ref, wqkv_ref, gqkv_acc, head_acc
    )
    gz_ref[0] = g
    r_unit, r_inv = standardize(r_ref[0])
    m = (r_unit * param(small_ref, 2) + param(small_ref, 3)).astype(BF16)
    feed_back_tail(
        g, g.astype(BF16), r_unit, r_inv, m, o_ref[0], small_ref,
        lambda c: (hid_ref[0, c * BLK : (c + 1) * BLK, :], slope_ref[0, c * BLK : (c + 1) * BLK, :].astype(F32)),
        wu_ref, wd_ref, wo_ref, gr_out, go_out, gd_acc, gu_acc, go_acc, tail_acc,
    )


def turn(table, dq, dk, dv, a, z, gr, hid, slope, r, o, small, wqkv, wo, wu, wd, gd, gu, go, tail):
    tile = pl.BlockSpec((1, BLK, BLK), lambda u, t: (u, 0, 0))
    moved = pl.BlockSpec((1, BLK, BLK), lambda u, t: (t[u], 0, 0))
    tall = pl.BlockSpec((1, FF, BLK), lambda u, t: (u, 0, 0))
    whole = lambda shape: pl.BlockSpec(shape, lambda u, t: (0,) * len(shape))
    spec = pltpu.PrefetchScalarGridSpec(
        num_scalar_prefetch=1,
        grid=(UNITS,),
        in_specs=[tile, tile, tile, moved, tile, tile, tall, tall, tile, tile]
        + [full(w.shape) for w in (small, wqkv, wo, wu, wd, gd, gu, go, tail)],
        out_specs=[tile, tile, tile]
        + [whole(s) for s in ((FF, D), (D, FF), (D, D), (TAIL, 128), (3, D, D), (2 * D, 128))],
    )
    shape = (UNITS, BLK, BLK)
    return pl.pallas_call(
        turn_body,
        grid_spec=spec,
        out_shape=[
            jax.ShapeDtypeStruct(shape, F32),
            jax.ShapeDtypeStruct(shape, F32),
            jax.ShapeDtypeStruct(shape, BF16),
        ]
        + [jax.ShapeDtypeStruct(s, F32) for s in ((FF, D), (D, FF), (D, D), (TAIL, 128), (3, D, D), (2 * D, 128))],
        compiler_params=params_of(),
        cost_estimate=cost(2 * 1536 * 256 * 3840 * 2, 20 << 20),
        name="turn",
    )(table, dq, dk, dv, a, z, gr, hid, slope, r, o, small, wqkv, wo, wu, wd, gd, gu, go, tail)


def last_body(
    table, dq_ref, dk_ref, dv_ref, a_ref, xt_ref, gr_ref, gz_ref, small_ref, wqkv_ref, gqkv_in, head_in,
    grad_ref, gqkv_acc, head_acc,
):
    @pl.when(pl.program_id(0) == 0)
    def _():
        gqkv_acc[...] = gqkv_in[...]
        head_acc[...] = head_in[...]

    g = project_back(
        xt_ref[0].astype(F32), a_ref[0], dq_ref[0], dk_ref[0], dv_ref[0], gr_ref[0], small_ref, wqkv_ref,
        gqkv_acc, head_acc,
    )
    grad_ref[0] = (g + gz_ref[0]).T.astype(BF16)


def last(table, dq, dk, dv, a, xt, gr, gz, small, wqkv, gqkv, head):
    tile = pl.BlockSpec((1, BLK, BLK), lambda u, t: (u, 0, 0))
    moved = pl.BlockSpec((1, BLK, BLK), lambda u, t: (t[u], 0, 0))
    whole = lambda shape: pl.BlockSpec(shape, lambda u, t: (0,) * len(shape))
    spec = pltpu.PrefetchScalarGridSpec(
        num_scalar_prefetch=1,
        grid=(UNITS,),
        in_specs=[tile, tile, tile, moved, moved, tile, tile]
        + [full(w.shape) for w in (small, wqkv, gqkv, head)],
        out_specs=[tile, whole((3, D, D)), whole((2 * D, 128))],
    )
    return pl.pallas_call(
        last_body,
        grid_spec=spec,
        out_shape=[
            jax.ShapeDtypeStruct((UNITS, BLK, BLK), BF16),
            jax.ShapeDtypeStruct((3, D, D), F32),
            jax.ShapeDtypeStruct((2 * D, 128), F32),
        ],
        compiler_params=params_of(),
        cost_estimate=cost(2 * 1536 * 256 * 768 * 2, 10 << 20),
        name="last",
    )(table, dq, dk, dv, a, xt, gr, gz, small, wqkv, gqkv, head)


def prepare_body(w_ref, p_ref, wt_ref, wot_ref, wut_ref, wdt_ref, wqkv_ref, wo_ref, wu_ref, wd_ref, small_ref):
    for t in range(3):
        matrix = w_ref[0, t]
        wqkv_ref[t] = matrix
        wt_ref[t * D : (t + 1) * D, :] = matrix.T
    matrix = w_ref[0, 3]
    wo_ref[...] = matrix
    wot_ref[...] = matrix.T
    for c in range(4):
        part = slice(c * D, (c + 1) * D)
        matrix = w_ref[1, c]
        wu_ref[:, part] = matrix
        wut_ref[part, :] = matrix.T
        matrix = w_ref[2, c]
        wd_ref[part, :] = matrix
        wdt_ref[:, part] = matrix.T
    for row in range(SMALL):
        for side in range(2):
            line = jnp.broadcast_to(p_ref[2 * row + side : 2 * row + side + 1, :], (128, 128))
            small_ref[row * D + side * 128 : row * D + (side + 1) * 128, :] = line.T


def prepare(w, p):
    shapes = [(3 * D, D), (D, D), (FF, D), (D, FF), (3, D, D), (D, D), (D, FF), (FF, D)]
    return pl.pallas_call(
        prepare_body,
        in_specs=[pl.BlockSpec(memory_space=pltpu.VMEM)] * 2,
        out_specs=[pl.BlockSpec(memory_space=pltpu.VMEM)] * 9,
        out_shape=[jax.ShapeDtypeStruct(s, BF16) for s in shapes] + [jax.ShapeDtypeStruct((SMALL * D, 128), F32)],
        compiler_params=pltpu.CompilerParams(vmem_limit_bytes=40 << 20),
        cost_estimate=cost(1, 6 << 20),
        name="prepare",
    )(w, p)


def owner_scalars(owner_ref):
    sizes = [D * D] * 4 + [D * FF, FF * D, SMALL * D]
    starts = []
    for t in range(7):
        offset = jnp.int32(0)
        for u in range(t):
            offset = offset + jnp.where(owner_ref[u] == owner_ref[t], sizes[u], 0).astype(jnp.int32)
        starts.append(offset)
    return starts


def pack_body(owner_ref, row_ref, w_ref, p_ref):
    dp = lax.axis_index("dp")
    seq = lax.axis_index("seq")
    starts = owner_scalars(owner_ref)
    square = jnp.where(seq == 0, starts[0], jnp.where(seq == 1, starts[1], jnp.where(seq == 2, starts[2], starts[3])))
    plans = (
        (owner_ref[seq], square // 128, 2),
        (owner_ref[4], starts[4] // 128 + 2 * seq, FF // 128),
        (owner_ref[5], starts[5] // 128 + 2 * D * seq, 2),
    )
    for kind, (owner, base, stride) in enumerate(plans):
        keep = jnp.where(owner == dp, 1.0, 0.0).astype(F32)
        for side in range(2):
            values = row_ref[pl.ds(base + side, D, stride=stride), :]
            w_ref[kind, :, side * 128 : (side + 1) * 128] = (values * keep).astype(BF16)
    keep = jnp.where(owner_ref[6] == dp, 1.0, 0.0).astype(F32)
    values = row_ref[pl.ds(pl.multiple_of(starts[6] // 128, 8), 24), :] * keep
    rows = lax.broadcasted_iota(jnp.int32, (24, 128), 0)
    p_ref[...] = jnp.where(rows < 2 * SMALL, values, 0.0)


def pack(owner_list, row):
    return pl.pallas_call(
        pack_body,
        in_specs=[pl.BlockSpec(memory_space=pltpu.SMEM), pl.BlockSpec(memory_space=pltpu.VMEM)],
        out_specs=[pl.BlockSpec(memory_space=pltpu.VMEM)] * 2,
        out_shape=[jax.ShapeDtypeStruct((3, D, D), BF16), jax.ShapeDtypeStruct((24, 128), F32)],
        compiler_params=pltpu.CompilerParams(vmem_limit_bytes=20 << 20),
        cost_estimate=cost(1, 3 << 20),
        name="pack",
    )(owner_list, row)


def peers_of(seq):
    return {1: seq + 1 - 2 * (seq % 2), 2: (seq + 2) % 4, 3: 3 - seq}


def greet(n, dp, peers, wide_group):
    barrier = pltpu.get_barrier_semaphore()
    count = 0
    for peer in peers:
        pl.semaphore_signal(barrier, inc=1, device_id={"seq": peer}, device_id_type=MESH)
        count += 1
    if wide_group:
        for k in range(1, n):
            pl.semaphore_signal(barrier, inc=1, device_id={"dp": (dp + k) % n}, device_id_type=MESH)
            count += 1
    pl.semaphore_wait(barrier, count)


def send(source, target, sems, index, device):
    return pltpu.make_async_remote_copy(
        src_ref=source,
        dst_ref=target,
        send_sem=sems[0].at[index],
        recv_sem=sems[1].at[index],
        device_id=device,
        device_id_type=MESH,
    )


def spread(n, dp, seq, peers, kind, w_ref, chunk_ref, row_sems):
    copies = []
    for k in range(1, n):
        copies.append(
            send(chunk_ref.at[kind], w_ref.at[kind, seq, dp], row_sems, (kind, k), {"dp": (dp + k) % n})
        )
        copies[-1].start()
    return copies


def share(seq, peers, kind, w_ref, side_sems):
    copies = [
        send(w_ref.at[kind, seq], w_ref.at[kind, seq], side_sems, (kind, 0), {"seq": peers[2]}),
        send(w_ref.at[kind, seq], w_ref.at[kind, seq], side_sems, (kind, 1), {"seq": peers[1]}),
    ]
    for copy in copies:
        copy.start()
    return copies


def forward(seq, peers, kind, w_ref, side_sems):
    copy = send(w_ref.at[kind, peers[2]], w_ref.at[kind, peers[2]], side_sems, (kind, 2), {"seq": peers[1]})
    copy.start()
    return copy


def entry_body(
    n, pk_ref, pp_ref, x_ref, c_ref, w_ref, p_ref, xo_ref, co_ref, slot_ref, pslot_ref, chunk_ref,
    ss0, ss1, rs0, rs1, ps0, ps1, gs0, gs1, xs0, xs1, cs0, cs1,
):
    dp = lax.axis_index("dp")
    seq = lax.axis_index("seq")
    chip, core = seq // 2, seq % 2
    peers = peers_of(seq)
    greet(n, dp, [peers[1], peers[2], peers[3]], True)
    done = []
    small = []
    scatter = [[] for _ in range(3)]
    for kind in range(3):
        for k in range(1, n):
            to = (dp + k) % n
            copy = send(pk_ref.at[kind, to], slot_ref.at[kind, k], (ss0, ss1), (kind, k), {"dp": to})
            copy.start()
            scatter[kind].append(copy)
        if kind == 0:
            for k in range(1, n):
                copy = send(pp_ref, pslot_ref.at[k], (ps0, ps1), k, {"dp": (dp + k) % n})
                copy.start()
                small.append(copy)
    for o in (2, 3, 1):
        to = peers[o]
        for part, (source, target) in enumerate(((3 * (to // 2) + to % 2, seq), (3 * (to // 2) + 2, OWN + seq))):
            copy = send(x_ref.at[source], xo_ref.at[target], (xs0, xs1), (o, part), {"seq": to})
            copy.start()
            done.append(copy)
    for o in (2, 3, 1):
        to = peers[o]
        copy = send(c_ref.at[3 * (to // 2) + to % 2], co_ref.at[seq], (cs0, cs1), o, {"seq": to})
        copy.start()
        done.append(copy)

    @pl.when(chip == 0)
    def _():
        send(c_ref.at[5], co_ref.at[4], (cs0, cs1), 4 + 2, {"seq": peers[2]}).start()

    @pl.when(chip == 1)
    def _():
        send(c_ref.at[2], co_ref.at[5], (cs0, cs1), 4 + 3, {"seq": peers[3]}).start()
        send(c_ref.at[5], co_ref.at[5], (cs0, cs1), 4 + 1, {"seq": peers[1]}).start()

    xo_ref[seq] = x_ref[3 * chip + core]
    xo_ref[OWN + seq] = x_ref[3 * chip + 2]
    co_ref[seq] = c_ref[3 * chip + core]

    @pl.when(chip == 0)
    def _():
        co_ref[4] = c_ref[2]

    gathers = []
    for kind in range(3):
        total = pk_ref[kind, dp].astype(F32)
        for k in range(1, n):
            scatter[kind][k - 1].wait_recv()
            total = total + slot_ref[kind, k].astype(F32)
        chunk_ref[kind] = total.astype(BF16)
        w_ref[kind, seq, dp] = total.astype(BF16)
        gathers.append(spread(n, dp, seq, peers, kind, w_ref, chunk_ref, (rs0, rs1)))
    sides = []
    for kind in range(3):
        for copy in gathers[kind]:
            copy.wait_recv()
        sides.append(share(seq, peers, kind, w_ref, (gs0, gs1)))
    total = pp_ref[...]
    for copy in small:
        copy.wait_recv()
    for k in range(1, n):
        total = total + pslot_ref[k]
    p_ref[...] = total
    for kind in range(3):
        sides[kind][0].wait_recv()
        sides[kind].append(forward(seq, peers, kind, w_ref, (gs0, gs1)))
    for kind in range(3):
        sides[kind][1].wait_recv()
        sides[kind][2].wait_recv()

    @pl.when(chip == 0)
    def _():
        send(c_ref.at[5], co_ref.at[4], (cs0, cs1), 4 + 2, {"seq": peers[2]}).wait_send()
        send(c_ref.at[2], co_ref.at[5], (cs0, cs1), 4 + 3, {"seq": peers[3]}).wait_recv()

    @pl.when(chip == 1)
    def _():
        send(c_ref.at[2], co_ref.at[5], (cs0, cs1), 4 + 3, {"seq": peers[3]}).wait_send()
        send(c_ref.at[5], co_ref.at[5], (cs0, cs1), 4 + 1, {"seq": peers[1]}).wait_send()
        send(c_ref.at[5], co_ref.at[4], (cs0, cs1), 4 + 2, {"seq": peers[2]}).wait_recv()
        send(c_ref.at[5], co_ref.at[5], (cs0, cs1), 4 + 1, {"seq": peers[1]}).wait_recv()

    for copy in done:
        copy.wait()
    for kind in range(3):
        for copy in scatter[kind] + gathers[kind] + sides[kind]:
            copy.wait_send()
    for copy in small:
        copy.wait_send()


def pair_of_sems(shape):
    return [pltpu.SemaphoreType.DMA(shape), pltpu.SemaphoreType.DMA(shape)]


def entry(n, pk, pp, x, c):
    rows = D // n
    vmem = pl.BlockSpec(memory_space=pltpu.VMEM)
    return pl.pallas_call(
        partial(entry_body, n),
        in_specs=[vmem] * 4,
        out_specs=[vmem] * 4,
        out_shape=[
            jax.ShapeDtypeStruct((3, 4, n, rows, D), BF16),
            jax.ShapeDtypeStruct((24, 128), F32),
            jax.ShapeDtypeStruct((ALL, BLK, BLK), BF16),
            jax.ShapeDtypeStruct((UNITS, BLK, BLK), BF16),
        ],
        scratch_shapes=[
            pltpu.VMEM((3, n, rows, D), BF16),
            pltpu.VMEM((n, 24, 128), F32),
            pltpu.VMEM((3, rows, D), BF16),
            *pair_of_sems((3, n)),
            *pair_of_sems((3, n)),
            *pair_of_sems((n,)),
            *pair_of_sems((3, 3)),
            *pair_of_sems((4, 2)),
            *pair_of_sems((8,)),
        ],
        compiler_params=pltpu.CompilerParams(collective_id=0, has_side_effects=True, vmem_limit_bytes=40 << 20),
        cost_estimate=cost(1, 12 << 20),
        name="entry",
    )(pk, pp, x, c)


def swap_inputs_body(a_ref, out_ref, s0, s1):
    seq = lax.axis_index("seq")
    core = seq % 2
    peers = peers_of(seq)
    greet(1, 0, [peers[1]], False)
    copies = [
        send(a_ref.at[4], out_ref.at[4 + core], (s0, s1), 0, {"seq": peers[1]}),
        send(a_ref.at[5], out_ref.at[7 - core], (s0, s1), 1, {"seq": peers[1]}),
    ]
    for copy in copies:
        copy.start()
    for j in range(OWN):
        out_ref[j] = a_ref[j]
    out_ref[4 + core] = a_ref[4]
    out_ref[7 - core] = a_ref[5]
    for copy in copies:
        copy.wait()


def swap_inputs(a):
    vmem = pl.BlockSpec(memory_space=pltpu.VMEM)
    return pl.pallas_call(
        swap_inputs_body,
        in_specs=[vmem],
        out_specs=vmem,
        out_shape=jax.ShapeDtypeStruct((ALL, BLK, BLK), BF16),
        scratch_shapes=pair_of_sems((2,)),
        compiler_params=pltpu.CompilerParams(collective_id=1, has_side_effects=True, vmem_limit_bytes=16 << 20),
        cost_estimate=cost(1, 2 << 20),
        name="swap_inputs",
    )(a)


def swap_grads_body(dk_ref, dv_ref, dk_out, dv_out, slot_ref, s0, s1):
    seq = lax.axis_index("seq")
    core = seq % 2
    peers = peers_of(seq)
    greet(1, 0, [peers[1]], False)
    copies = []
    for which, ref in enumerate((dk_ref, dv_ref)):
        for place, position in enumerate((5 - core, 6 + core)):
            copies.append(
                send(ref.at[position], slot_ref.at[which, place], (s0, s1), (which, place), {"seq": peers[1]})
            )
            copies[-1].start()
    for ref, out in ((dk_ref, dk_out), (dv_ref, dv_out)):
        for j in range(OWN):
            out[j] = ref[j]
    for copy in copies:
        copy.wait()
    for which, (ref, out) in enumerate(((dk_ref, dk_out), (dv_ref, dv_out))):
        for place, position in enumerate((4 + core, 7 - core)):
            out[4 + place] = (ref[position].astype(F32) + slot_ref[which, place].astype(F32)).astype(BF16)


def swap_grads(dk, dv):
    vmem = pl.BlockSpec(memory_space=pltpu.VMEM)
    out = jax.ShapeDtypeStruct((UNITS, BLK, BLK), BF16)
    return pl.pallas_call(
        swap_grads_body,
        in_specs=[vmem] * 2,
        out_specs=[vmem] * 2,
        out_shape=[out, out],
        scratch_shapes=[pltpu.VMEM((2, 2, BLK, BLK), BF16), *pair_of_sems((2, 2))],
        compiler_params=pltpu.CompilerParams(collective_id=2, has_side_effects=True, vmem_limit_bytes=16 << 20),
        cost_estimate=cost(1, 4 << 20),
        name="swap_grads",
    )(dk, dv)


def collect_body(n, gqkv_ref, go_ref, gu_ref, gd_ref, head_ref, tail_ref, sq1_ref, sq2_ref, g_ref, p_ref):
    dp = lax.axis_index("dp")
    seq = lax.axis_index("seq")
    chip, core = seq // 2, seq % 2
    for t in range(3):
        g_ref[0, t] = gqkv_ref[t].astype(BF16)
    g_ref[0, 3] = go_ref[...].astype(BF16)
    for c in range(4):
        g_ref[1, c] = gu_ref[:, c * D : (c + 1) * D].astype(BF16)
        g_ref[2, c] = gd_ref[c * D : (c + 1) * D, :].astype(BF16)
    for row in range(SMALL):
        for side in range(2):
            ref, first = (head_ref, row) if row < 2 else (tail_ref, row - 2)
            first = first * D + side * 128
            p_ref[2 * row + side : 2 * row + side + 1, :] = jnp.sum(ref[first : first + 128, :].T, axis=0, keepdims=True)
    sequences = 6 * n
    place = lax.broadcasted_iota(jnp.int32, (6, 128), 0) * 128 + lax.broadcasted_iota(jnp.int32, (6, 128), 1)
    stats = jnp.zeros((6, 128), F32)
    for i, ref in enumerate((sq1_ref, sq2_ref)):
        lines = [ref[u, 0:1, :] for u in range(UNITS)]
        own = jnp.sum(lines[0] + lines[1] + lines[2] + lines[3], axis=1, keepdims=True)
        half = jnp.sum(lines[4] + lines[5], axis=1, keepdims=True)
        start = i * sequences + 6 * dp + 3 * chip
        stats = jnp.where(place == start + core, jnp.broadcast_to(own, (6, 128)), stats)
        stats = jnp.where(place == start + 2, jnp.broadcast_to(half, (6, 128)), stats)
    p_ref[18:24, :] = stats


def collect(n, gqkv, go, gu, gd, head, tail, sq1, sq2):
    vmem = pl.BlockSpec(memory_space=pltpu.VMEM)
    return pl.pallas_call(
        partial(collect_body, n),
        in_specs=[vmem] * 8,
        out_specs=[vmem] * 2,
        out_shape=[jax.ShapeDtypeStruct((3, 4, D, D), BF16), jax.ShapeDtypeStruct((24, 128), F32)],
        compiler_params=pltpu.CompilerParams(vmem_limit_bytes=24 << 20),
        cost_estimate=cost(1, 6 << 20),
        name="collect",
    )(gqkv, go, gu, gd, head, tail, sq1, sq2)


def leave_body(
    n, g_ref, pp_ref, f_ref, i_ref, w_ref, p_ref, fo_ref, io_ref,
    half_ref, quarter_ref, out_ref, mine_ref, slot_ref, chunk_ref, pslot_ref, psum_ref,
    as0, as1, bs0, bs1, ss0, ss1, rs0, rs1, gs0, gs1, ps0, ps1, xs0, xs1,
):
    dp = lax.axis_index("dp")
    seq = lax.axis_index("seq")
    chip, core = seq // 2, seq % 2
    peers = peers_of(seq)
    greet(n, dp, [peers[1], peers[2], peers[3]], True)
    finish = []

    first = []
    for kind in range(3):
        copies = []
        for j, quarter in enumerate((peers[1], peers[3])):
            copies.append(
                send(g_ref.at[kind, quarter], half_ref.at[kind, j], (as0, as1), (kind, j), {"seq": peers[1]})
            )
            copies[-1].start()
        first.append(copies)
        finish += copies
    small = [send(pp_ref, pslot_ref.at[0], (ps0, ps1), 0, {"seq": peers[1]})]
    small[0].start()

    moves = []
    own = 3 * chip + core

    def move(which, source_ref, target_ref):
        for o in (2, 3, 1):
            copy = send(source_ref.at[peers[o]], target_ref.at[own], (xs0, xs1), (which, o), {"seq": peers[o]})
            copy.start()
            moves.append(copy)

        @pl.when(chip == 0)
        def _():
            send(source_ref.at[5], target_ref.at[2], (xs0, xs1), (which, 4 + 3), {"seq": peers[3]}).start()

        @pl.when(chip == 1)
        def _():
            send(source_ref.at[4], target_ref.at[5], (xs0, xs1), (which, 4 + 2), {"seq": peers[2]}).start()
            send(source_ref.at[5], target_ref.at[5], (xs0, xs1), (which, 4 + 1), {"seq": peers[1]}).start()

        target_ref[own] = source_ref[seq]

        @pl.when(chip == 0)
        def _():
            target_ref[2] = source_ref[4]

    def settle(which, source_ref, target_ref):
        @pl.when(chip == 0)
        def _():
            send(source_ref.at[5], target_ref.at[2], (xs0, xs1), (which, 4 + 3), {"seq": peers[3]}).wait_send()
            send(source_ref.at[4], target_ref.at[5], (xs0, xs1), (which, 4 + 2), {"seq": peers[2]}).wait_recv()

        @pl.when(chip == 1)
        def _():
            send(source_ref.at[4], target_ref.at[5], (xs0, xs1), (which, 4 + 2), {"seq": peers[2]}).wait_send()
            send(source_ref.at[5], target_ref.at[5], (xs0, xs1), (which, 4 + 1), {"seq": peers[1]}).wait_send()
            send(source_ref.at[5], target_ref.at[2], (xs0, xs1), (which, 4 + 3), {"seq": peers[3]}).wait_recv()
            send(source_ref.at[5], target_ref.at[5], (xs0, xs1), (which, 4 + 1), {"seq": peers[1]}).wait_recv()

    second = []
    for kind in range(3):
        for copy in first[kind]:
            copy.wait_recv()
        out_ref[kind] = (g_ref[kind, peers[2]].astype(F32) + half_ref[kind, 1].astype(F32)).astype(BF16)
        second.append(send(out_ref.at[kind], quarter_ref.at[kind], (bs0, bs1), kind, {"seq": peers[2]}))
        second[-1].start()
    finish += second
    small[0].wait_recv()
    psum_ref[0] = pp_ref[...] + pslot_ref[0]
    small.append(send(psum_ref.at[0], pslot_ref.at[1], (ps0, ps1), 1, {"seq": peers[2]}))
    small[1].start()
    move(0, f_ref, fo_ref)
    move(1, i_ref, io_ref)

    scatter = []
    for kind in range(3):
        second[kind].wait_recv()
        mine_ref[kind] = (
            g_ref[kind, seq].astype(F32) + half_ref[kind, 0].astype(F32) + quarter_ref[kind].astype(F32)
        ).astype(BF16)
        copies = []
        for k in range(1, n):
            to = (dp + k) % n
            copies.append(send(mine_ref.at[kind, to], slot_ref.at[kind, k], (ss0, ss1), (kind, k), {"dp": to}))
            copies[-1].start()
        scatter.append(copies)
        finish += copies
    small[1].wait_recv()
    psum_ref[1] = psum_ref[0] + pslot_ref[1]
    for k in range(1, n):
        copy = send(psum_ref.at[1], pslot_ref.at[1 + k], (ps0, ps1), 1 + k, {"dp": (dp + k) % n})
        copy.start()
        small.append(copy)
    gathers = []
    for kind in range(3):
        total = mine_ref[kind, dp].astype(F32)
        for k in range(1, n):
            scatter[kind][k - 1].wait_recv()
            total = total + slot_ref[kind, k].astype(F32)
        chunk_ref[kind] = total.astype(BF16)
        w_ref[kind, seq, dp] = total.astype(BF16)
        gathers.append(spread(n, dp, seq, peers, kind, w_ref, chunk_ref, (rs0, rs1)))
    sides = []
    for kind in range(3):
        for copy in gathers[kind]:
            copy.wait_recv()
        sides.append(share(seq, peers, kind, w_ref, (gs0, gs1)))
        finish += gathers[kind]
    total = psum_ref[1]
    for k in range(1, n):
        small[1 + k].wait_recv()
        total = total + pslot_ref[1 + k]
    p_ref[...] = total
    for kind in range(3):
        sides[kind][0].wait_recv()
        sides[kind].append(forward(seq, peers, kind, w_ref, (gs0, gs1)))
    for kind in range(3):
        sides[kind][1].wait_recv()
        sides[kind][2].wait_recv()
        finish += sides[kind]
    settle(0, f_ref, fo_ref)
    settle(1, i_ref, io_ref)
    for copy in moves:
        copy.wait()
    for copy in finish + small:
        copy.wait_send()


def leave(n, g, pp, f, i):
    rows = D // n
    vmem = pl.BlockSpec(memory_space=pltpu.VMEM)
    return pl.pallas_call(
        partial(leave_body, n),
        in_specs=[vmem] * 4,
        out_specs=[vmem] * 4,
        out_shape=[
            jax.ShapeDtypeStruct((3, 4, n, rows, D), BF16),
            jax.ShapeDtypeStruct((24, 128), F32),
            jax.ShapeDtypeStruct((UNITS, BLK, BLK), BF16),
            jax.ShapeDtypeStruct((UNITS, BLK, BLK), BF16),
        ],
        scratch_shapes=[
            pltpu.VMEM((3, 2, n, rows, D), BF16),
            pltpu.VMEM((3, n, rows, D), BF16),
            pltpu.VMEM((3, n, rows, D), BF16),
            pltpu.VMEM((3, n, rows, D), BF16),
            pltpu.VMEM((3, n, rows, D), BF16),
            pltpu.VMEM((3, rows, D), BF16),
            pltpu.VMEM((1 + n, 24, 128), F32),
            pltpu.VMEM((2, 24, 128), F32),
            *pair_of_sems((3, 2)),
            *pair_of_sems((3,)),
            *pair_of_sems((3, n)),
            *pair_of_sems((3, n)),
            *pair_of_sems((3, 3)),
            *pair_of_sems((1 + n,)),
            *pair_of_sems((2, 8)),
        ],
        compiler_params=pltpu.CompilerParams(collective_id=3, has_side_effects=True, vmem_limit_bytes=48 << 20),
        cost_estimate=cost(1, 20 << 20),
        name="leave",
    )(g, pp, f, i)


ROWS = D * D // 128


def adam_body(owner_ref, g_ref, p_ref, m_ref, v_ref, w_ref, m_out, v_out, w_out, grad_ref):
    dp = lax.axis_index("dp")
    block = pl.program_id(0)
    starts = owner_scalars(owner_ref)
    counts = [1, 1, 1, 1, 4, 4, 1]
    rate = jnp.float32(D ** (-0.5))
    decay = jnp.float32(0.1)
    limit = jnp.int32(0)
    for t in range(7):
        first = starts[t] // (D * D)
        here = (owner_ref[t] == dp) & (block >= first) & (block < first + counts[t])
        part = block - first
        limit = jnp.where(here, 2 * SMALL if t == 6 else ROWS, limit)
        if t == 5:
            rate = jnp.where(here, FF ** (-0.5), rate)
        if t == 6:
            rate = jnp.where(here, 0.5, rate)
            decay = jnp.where(here, 0.0, decay)

        @pl.when(here)
        def _(t=t, part=part):
            if t == 6:
                grad_ref[0:24, :] = p_ref[...]
            elif t == 4:
                for c in range(4):
                    piece = g_ref[4 + c, pl.ds(pl.multiple_of(part * 64, 64), 64), :].astype(F32)
                    for side in range(2):
                        grad_ref[pl.ds(2 * c + side, 64, stride=8), :] = piece[:, side * 128 : (side + 1) * 128]
            else:
                piece = g_ref[8 + part if t == 5 else t].astype(F32)
                for side in range(2):
                    grad_ref[pl.ds(side, D, stride=2), :] = piece[:, side * 128 : (side + 1) * 128]

    @pl.when(limit == 0)
    def _():
        for out in (m_out, v_out, w_out):
            out[...] = jnp.zeros_like(out)

    @pl.when(limit > 0)
    def _():
        correction = 1.0 - 0.5**STEP
        grad = grad_ref[...]
        valid = lax.broadcasted_iota(jnp.int32, (ROWS, 128), 0) < limit
        first_new = 0.5 * m_ref[...] + 0.5 * grad
        second_new = 0.5 * v_ref[...] + 0.5 * grad * grad
        old = w_ref[...]
        update = first_new / correction / (jnp.sqrt(second_new / correction) + adam_eps) + decay * old
        m_out[...] = jnp.where(valid, first_new, 0.0)
        v_out[...] = jnp.where(valid, second_new, 0.0)
        w_out[...] = jnp.where(valid, old - rate * update, 0.0)


def adam(owner_list, g, p, m, v, w):
    tile = pl.BlockSpec((ROWS, 128), lambda b, t: (b, 0))
    out = jax.ShapeDtypeStruct(m.shape, F32)
    spec = pltpu.PrefetchScalarGridSpec(
        num_scalar_prefetch=1,
        grid=(m.shape[0] // ROWS,),
        in_specs=[full(g.shape), full(p.shape), tile, tile, tile],
        out_specs=[tile, tile, tile],
        scratch_shapes=[pltpu.VMEM((ROWS, 128), F32)],
    )
    return pl.pallas_call(
        adam_body,
        grid_spec=spec,
        out_shape=[out, out, out],
        compiler_params=params_of(),
        cost_estimate=cost(20 * 524288, 14 << 20),
        name="adam",
    )(owner_list, g, p, m, v, w)


def per_device(inputs, cotangent, owner_list, master_rows, moment1_rows, moment2_rows):
    n = lax.axis_size("dp")
    seq = lax.axis_index("seq")
    core = seq % 2
    rows = D // n
    flat = [r.reshape(-1, 128) for r in (master_rows, moment1_rows, moment2_rows)]
    pk, pp = pack(owner_list, flat[0])
    w, p, x, cot = entry(n, pk.reshape(3, n, rows, D), pp, inputs, cotangent)
    wt, wot, wut, wdt, wqkv, wo, wu, wd, small = prepare(w.reshape(3, 4, D, D), p)
    lane = jnp.arange(UNITS, dtype=jnp.int32)
    place = jnp.where(lane < OWN, lane, jnp.where(lane == OWN, core, 3 - core))
    base = jnp.where(lane < OWN, 0, OWN)
    table = jnp.concatenate([base + place, base, place]).astype(jnp.int32)

    xt, a1, q1, kt1, vt1, k1, v1 = first_projection(x, small, wt)
    o1, log1 = attend(table, q1, k1, vt1)
    r1, hid, slope, z2, a2, sq1 = feed_first(table, xt, o1, small, wot, wut, wdt)
    a2 = swap_inputs(a2)
    q2, kt2, vt2, k2, v2 = second_projection(a2, wt)
    o2, log2 = attend(table, q2, k2, vt2)
    final, sq2, gr, go, gd, gu, gout, tail = feed_second(z2, o2, cot, small, wot, wut, wdt, wo, wu, wd)
    dq, dk, dv = attend_back(table, q2, k2, kt2, v2, go, o2, log2)
    dk, dv = swap_grads(dk, dv)
    gz, gr, go, gd, gu, gout, tail, gqkv, head = turn(
        table, dq, dk, dv, a2, z2, gr, hid, slope, r1, o1, small, wqkv, wo, wu, wd, gd, gu, gout, tail
    )
    dq, dk, dv = attend_back(table, q1, k1, kt1, v1, go, o1, log1)
    dk, dv = swap_grads(dk, dv)
    grad, gqkv, head = last(table, dq, dk, dv, a1, xt, gr, gz, small, wqkv, gqkv, head)
    g, pp = collect(n, gqkv, gout, gu, gd, head, tail, sq1, sq2)
    g, p, final, grad = leave(n, g.reshape(3, 4, n, rows, D), pp, final, grad)
    m_new, v_new, w_new = adam(owner_list, g.reshape(12, D, D), p, flat[1], flat[2], flat[0])
    sequences = inputs.shape[0] * n
    entries = inputs.shape[1] * lax.axis_size("seq") * D
    squares = p[18:].reshape(-1)[: 2 * sequences].reshape(2, sequences)
    stats = jnp.sqrt(squares / entries + stat_eps)
    back = lambda r: r.reshape(master_rows.shape)
    return (final.astype(F32), grad.astype(F32), stats, back(m_new), back(v_new), back(w_new))


def solution(mesh):
    placed = (P("dp", "seq", None), P("dp", "seq", None), P(), P("dp", None), P("dp", None), P("dp", None))
    return jax.shard_map(
        per_device,
        mesh=mesh,
        in_specs=placed,
        out_specs=(P("dp", "seq", None), P("dp", "seq", None), P(), P("dp", None), P("dp", None), P("dp", None)),
        check_vma=False,
    )
```

```python
import math
from functools import partial

import jax
import jax.numpy as jnp
from jax import lax
from jax.experimental import pallas as pl
from jax.experimental.pallas import tpu as pltpu
from jax.sharding import PartitionSpec as P

D = 256
HEADS = 4
HD = 64
FF = 1024
STEP = 3
SMALL = 9
BLK = 256
OWN = 4
UNITS = 6
ALL = 8
F32 = jnp.float32
BF16 = jnp.bfloat16
MESH = pl.DeviceIdType.MESH

norm_eps = 1e-05
stat_eps = 1e-06
adam_eps = 1e-08
masked_score = -1e30


def dot(left, right):
    return lax.dot_general(left, right, (((1,), (0,)), ((), ())), preferred_element_type=F32)


def dot_nt(left, right):
    return lax.dot_general(left, right, (((1,), (1,)), ((), ())), preferred_element_type=F32)


def wide(column):
    return jnp.concatenate([column, column], axis=1)


def fold(values):
    return values[:, :128] + values[:, 128:]


def standardize(values):
    average = jnp.mean(values, axis=0, keepdims=True)
    centered = values - average
    spread = jnp.mean(centered * centered, axis=0, keepdims=True)
    inverse = lax.rsqrt(spread + norm_eps)
    return centered * inverse, inverse


def standardize_back(grad, unit_values, inverse):
    average = jnp.mean(grad, axis=0, keepdims=True)
    inner = jnp.mean(grad * unit_values, axis=0, keepdims=True)
    return (grad - average - unit_values * inner) * inverse


def param(small_ref, row):
    return wide(small_ref[row * D : (row + 1) * D, :])


def gelu_parts(e):
    cdf = 0.5 * lax.erf(e * math.sqrt(0.5)) + 0.5
    hid = e * cdf
    slope = cdf + e * (jnp.exp(-0.5 * e * e) * (1.0 / math.sqrt(2.0 * math.pi)))
    return hid, slope


def full(shape):
    return pl.BlockSpec(shape, lambda *args: (0,) * len(shape), pipeline_mode=pl.Buffered(1))


def params_of(ndims=1, mib=56):
    return pltpu.CompilerParams(
        dimension_semantics=("arbitrary",) * ndims, vmem_limit_bytes=mib << 20
    )


def cost(flops, nbytes, trans=0):
    return pl.CostEstimate(flops=int(flops), bytes_accessed=int(nbytes), transcendentals=int(trans))


LOG2E = math.log2(math.e)
VROWS = HD + 16


def unit_place(unit, core):
    place = jnp.where(unit < OWN, unit, jnp.where(unit == OWN, core, 3 - core))
    base = jnp.where(unit < OWN, 0, OWN)
    return place, base


def lanes(start, size):
    return pl.ds(pl.multiple_of(start, BLK), size)


def matrix(w_ref, kind, part):
    n, rows = w_ref.shape[2:4]
    if rows % 16 == 0:
        return w_ref[kind, part].reshape(D, D)
    return jnp.concatenate([w_ref[kind, part, i] for i in range(n)], axis=0)


def project(j, a, wt_ref, q_ref, kt_ref, vt_ref, k_ref, v_ref):
    where = lanes(j * BLK, BLK)
    q_ref[j] = (dot(wt_ref[0:D], a) * HD ** (-0.5)).astype(BF16)
    kt = dot(wt_ref[D : 2 * D], a).astype(BF16)
    vt = dot(wt_ref[2 * D : 3 * D], a).astype(BF16)
    for h in range(HEADS):
        kt_ref[h, :, where] = kt[h * HD : (h + 1) * HD]
        vt_ref[h, 0:HD, where] = vt[h * HD : (h + 1) * HD]
    k = kt.T
    v = vt.T
    for h in range(2):
        k_ref[h, j] = k[:, h * 128 : (h + 1) * 128]
        v_ref[h, j] = v[:, h * 128 : (h + 1) * 128]


def head_rows(values, half):
    rows = lax.broadcasted_iota(jnp.int32, values.shape, 0)
    keep = (rows < HD) if half == 0 else (rows >= HD)
    return jnp.where(keep, values, jnp.zeros_like(values))


def set_mask(mask_ref):
    keys = lax.broadcasted_iota(jnp.int32, (BLK, BLK), 0)
    queries = lax.broadcasted_iota(jnp.int32, (BLK, BLK), 1)
    mask_ref[...] = jnp.where(keys <= queries, 0.0, masked_score)


def groups(values, op):
    out = values[0:8]
    for i in range(1, values.shape[0] // 8):
        out = op(out, values[i * 8 : (i + 1) * 8])
    return out


SUB = 128


def attend(core, q_ref, k_ref, vt_ref, o_ref, log_ref, mask_ref, score_ref, prob_ref):
    def step(i, carry):
        pair, unit = i // UNITS, i % UNITS
        place, base = unit_place(unit, core)

        def branch(last):
            block = q_ref[base + place, lanes(pair * 128, 128), :]
            for half in range(2):
                q = head_rows(block, half)
                top = None
                for kb in range(last + 1):
                    for sub in range(BLK // SUB):
                        rows = slice(sub * SUB, (sub + 1) * SUB)
                        score = dot(k_ref[pair, base + kb, rows, :], q)
                        if kb == last:
                            score = score + mask_ref[rows, :]
                        score_ref[half, kb, rows, :] = score
                        peak = groups(score, jnp.maximum)
                        top = peak if top is None else jnp.maximum(top, peak)
                top = jnp.max(top, axis=0, keepdims=True)
                for kb in range(last + 1):
                    for sub in range(BLK // SUB):
                        rows = slice(sub * SUB, (sub + 1) * SUB)
                        weight = jnp.exp(score_ref[half, kb, rows, :] - top)
                        prob_ref[half, kb * BLK + sub * SUB : kb * BLK + (sub + 1) * SUB, :] = weight.astype(BF16)
                keys = (last + 1) * BLK
                out = dot(vt_ref[2 * pair + half, :, lanes(base * BLK, keys)], prob_ref[half, 0:keys, :])
                total = out[HD : HD + 1]
                o_ref[unit, pl.ds(pl.multiple_of(pair * 128 + half * HD, HD), HD), :] = (out[0:HD] / total).astype(BF16)
                log_ref[unit, pair, half : half + 1, :] = top + jnp.log(total)

        for last in range(OWN):
            pl.when(place == last)(partial(branch, last))
        return carry

    lax.fori_loop(0, 2 * UNITS, step, 0)


def attend_back(
    core, q_ref, k_ref, kt_ref, v_ref, go_ref, o_ref, log_ref, dq_ref, dk_ref, dv_ref, mask_ref, prob_ref, slope_ref, dk_acc, dv_acc
):
    dk_acc[...] = jnp.zeros_like(dk_acc)
    dv_acc[...] = jnp.zeros_like(dv_acc)

    def step(i, carry):
        pair, unit = i // UNITS, i % UNITS
        place, base = unit_place(unit, core)

        def branch(last):
            block = q_ref[base + place, lanes(pair * 128, 128), :]
            go_block = go_ref[unit, lanes(pair * 128, 128), :]
            o_block = o_ref[unit, lanes(pair * 128, 128), :]
            keys = (last + 1) * BLK
            for half in range(2):
                lo, hi = half * HD, (half + 1) * HD
                q = head_rows(block, half)
                go = head_rows(go_block, half)
                q_head = block[lo:hi]
                go_head = go_block[lo:hi]
                log_total = log_ref[unit, pair, half : half + 1, :]
                inner = jnp.sum(go_head.astype(F32) * o_block[lo:hi].astype(F32), axis=0, keepdims=True)
                for kb in range(last + 1):
                    for sub in range(BLK // SUB):
                        rows = slice(sub * SUB, (sub + 1) * SUB)
                        to = slice(kb * BLK + sub * SUB, kb * BLK + (sub + 1) * SUB)
                        score = dot(k_ref[pair, base + kb, rows, :], q)
                        if kb == last:
                            score = score + mask_ref[rows, :]
                        weight = jnp.exp(score - log_total)
                        slope = dot(v_ref[pair, base + kb, rows, :], go)
                        prob_ref[half, to, :] = weight.astype(BF16)
                        slope_ref[half, to, :] = (weight * (slope - inner)).astype(BF16)
                head = 2 * pair + half
                where = lanes(base * BLK, keys)
                dv_acc[head, :, where] += dot_nt(go_head, prob_ref[half, 0:keys, :])
                dk_acc[head, :, where] += dot_nt(q_head, slope_ref[half, 0:keys, :])
                dq = dot(kt_ref[head, :, where], slope_ref[half, 0:keys, :])
                dq_ref[unit, pl.ds(pl.multiple_of(pair * 128 + lo, HD), HD), :] = (dq * HD ** (-0.5)).astype(BF16)

        for last in range(OWN):
            pl.when(place == last)(partial(branch, last))
        return carry

    lax.fori_loop(0, 2 * UNITS, step, 0)
    for j in range(ALL):
        for ref, acc in ((dk_ref, dk_acc), (dv_ref, dv_acc)):
            ref[j] = acc[:, :, j * BLK : (j + 1) * BLK].reshape(D, BLK).astype(BF16)


def forward_parts(z, o, wot_ref, small_ref):
    r = z + dot(wot_ref[...], o)
    unit_values, inverse = standardize(r)
    m = (unit_values * param(small_ref, 2) + param(small_ref, 3)).astype(BF16)
    return r, unit_values, inverse, m


def squares_of(out):
    return groups(out * out, jnp.add)


def first_stage_body(
    x_ref, w_ref, p_ref,
    xt_ref, a_ref, q_ref, kt_ref, k_ref, v_ref, o_ref, log_ref, r_ref, hid_ref, slope_ref, z_ref, a2_ref, sq_ref,
    wt_ref, wot_ref, wut_ref, wdt_ref, small_ref, vt_ref, mask_ref, score_ref, prob_ref,
):
    core = lax.axis_index("seq") % 2
    for t in range(3):
        wt_ref[t * D : (t + 1) * D, :] = matrix(w_ref, 0, t).T
    for row in range(SMALL):
        for side in range(2):
            line = jnp.broadcast_to(p_ref[2 * row + side : 2 * row + side + 1, :], (128, 128))
            small_ref[row * D + side * 128 : row * D + (side + 1) * 128, :] = line.T
    set_mask(mask_ref)
    vt_ref[:, HD:, :] = jnp.ones((HEADS, VROWS - HD, ALL * BLK), BF16)

    def begin(j, carry):
        xt = x_ref[j].T
        xt_ref[j] = xt
        unit_values, _ = standardize(xt.astype(F32))
        a = (unit_values * param(small_ref, 0) + param(small_ref, 1)).astype(BF16)
        a_ref[j] = a
        project(j, a, wt_ref, q_ref, kt_ref, vt_ref, k_ref, v_ref)
        return carry

    lax.fori_loop(0, ALL, begin, 0)
    attend(core, q_ref, k_ref, vt_ref, o_ref, log_ref, mask_ref, score_ref, prob_ref)
    wot_ref[...] = matrix(w_ref, 0, 3).T
    for c in range(4):
        part = slice(c * D, (c + 1) * D)
        wut_ref[part, :] = matrix(w_ref, 1, c).T
        wdt_ref[:, part] = matrix(w_ref, 2, c).T

    def feed(u, carry):
        place, base = unit_place(u, core)
        x = xt_ref[base + place].astype(F32)
        r, _, _, m = forward_parts(x, o_ref[u], wot_ref, small_ref)
        r_ref[u] = r
        out = r + param(small_ref, 4)
        for c in range(FF // BLK):
            rows = slice(c * BLK, (c + 1) * BLK)
            e = dot(wut_ref[rows, :], m) + param(small_ref, 5 + c)
            hid, slope = gelu_parts(e)
            hid = hid.astype(BF16)
            hid_ref[u, rows, :] = hid
            slope_ref[u, rows, :] = slope.astype(BF16)
            out = out + dot(wdt_ref[:, rows], hid)
        sq_ref[u] = squares_of(out)
        z = out + x
        z_ref[u] = z
        unit_values, _ = standardize(z)
        a2_ref[u] = (unit_values * param(small_ref, 0) + param(small_ref, 1)).astype(BF16)
        return carry

    lax.fori_loop(0, UNITS, feed, 0)


VM = pl.BlockSpec(memory_space=pltpu.VMEM)


def shape_of(shape, dtype=BF16):
    return jax.ShapeDtypeStruct(shape, dtype)


KEYS = [
    shape_of((HEADS, HD, ALL * BLK)),
    shape_of((2, ALL, BLK, 128)),
    shape_of((2, ALL, BLK, 128)),
]
ATTEND_SCRATCH = [
    pltpu.VMEM((BLK, BLK), F32),
    pltpu.VMEM((2, OWN, BLK, BLK), F32),
    pltpu.VMEM((2, OWN * BLK, BLK), BF16),
]
BACK_SCRATCH = [
    pltpu.VMEM((BLK, BLK), F32),
    pltpu.VMEM((2, OWN * BLK, BLK), BF16),
    pltpu.VMEM((2, OWN * BLK, BLK), BF16),
    pltpu.VMEM((HEADS, HD, ALL * BLK), F32),
    pltpu.VMEM((HEADS, HD, ALL * BLK), F32),
]


def stage_call(body, name, args, outs, scratch, mib, flops):
    return pl.pallas_call(
        body,
        in_specs=[VM] * len(args),
        out_specs=[VM] * len(outs),
        out_shape=outs,
        scratch_shapes=scratch,
        compiler_params=pltpu.CompilerParams(vmem_limit_bytes=mib << 20),
        cost_estimate=cost(flops, 1 << 20),
        name=name,
    )(*args)


def first_stage(x, w, p):
    tile, eight = (UNITS, BLK, BLK), (ALL, BLK, BLK)
    outs = [shape_of(eight), shape_of(eight), shape_of(eight)] + KEYS
    outs += [shape_of(tile), shape_of((UNITS, 2, 8, BLK), F32), shape_of(tile, F32)]
    outs += [shape_of((UNITS, FF, BLK)), shape_of((UNITS, FF, BLK)), shape_of(tile, F32), shape_of(tile)]
    outs += [shape_of((UNITS, 8, BLK), F32), shape_of((3 * D, D)), shape_of((D, D)), shape_of((FF, D))]
    outs += [shape_of((D, FF)), shape_of((SMALL * D, 128), F32)]
    scratch = [pltpu.VMEM((HEADS, VROWS, ALL * BLK), BF16)] + ATTEND_SCRATCH
    return stage_call(first_stage_body, "first_stage", [x, w, p], outs, scratch, FIRST_MIB, 8e9)


def feed_back_tail(
    u, g, gy, r_unit, r_inv, m, o, small_ref, parts, w_ref, gr_ref, go_ref, gd_acc, gu_acc, go_acc, tail_acc
):
    tail_acc[2 * D : 3 * D, :] += fold(gy.astype(F32))
    gm = jnp.zeros((D, BLK), F32)
    for c in range(FF // BLK):
        rows = slice(c * BLK, (c + 1) * BLK)
        hid, slope = parts(c)
        gd_acc[rows, :] += dot_nt(hid, gy)
        ge = (dot(matrix(w_ref, 2, c), gy) * slope).astype(BF16)
        gu_acc[:, rows] += dot_nt(m, ge)
        tail_acc[3 * D + c * BLK : 3 * D + (c + 1) * BLK, :] += fold(ge.astype(F32))
        gm = gm + dot(matrix(w_ref, 1, c), ge)
    tail_acc[0:D, :] += fold(gm * r_unit)
    tail_acc[D : 2 * D, :] += fold(gm)
    gr = g + standardize_back(gm * param(small_ref, 2), r_unit, r_inv)
    gr_ref[u] = gr
    ga = gr.astype(BF16)
    go_acc[...] += dot_nt(o, ga)
    go_ref[u] = dot(matrix(w_ref, 0, 3), ga).astype(BF16)


TAIL = 3 * D + FF


def second_stage_body(
    a_ref, z_ref, cot_ref, w_ref, wt_ref, wot_ref, wut_ref, wdt_ref, small_ref,
    final_ref, sq_ref, gr_ref, gd_acc, gu_acc, go_acc, tail_acc, dq_ref, dk_ref, dv_ref,
    q_ref, kt_ref, k_ref, v_ref, vt_ref, o_ref, log_ref, go_ref, score_ref, hid_buf, slope_buf,
    mask_ref, prob_ref, ds_ref, dk_acc, dv_acc,
):
    core = lax.axis_index("seq") % 2
    set_mask(mask_ref)
    vt_ref[:, HD:, :] = jnp.ones((HEADS, VROWS - HD, ALL * BLK), BF16)
    for acc in (gd_acc, gu_acc, go_acc, tail_acc):
        acc[...] = jnp.zeros_like(acc)

    def begin(j, carry):
        project(j, a_ref[j], wt_ref, q_ref, kt_ref, vt_ref, k_ref, v_ref)
        return carry

    lax.fori_loop(0, ALL, begin, 0)
    attend(core, q_ref, k_ref, vt_ref, o_ref, log_ref, mask_ref, score_ref, prob_ref)

    def feed(u, carry):
        r, r_unit, r_inv, m = forward_parts(z_ref[u], o_ref[u], wot_ref, small_ref)
        out = r + param(small_ref, 4)
        for c in range(FF // BLK):
            rows = slice(c * BLK, (c + 1) * BLK)
            e = dot(wut_ref[rows, :], m) + param(small_ref, 5 + c)
            hid, slope = gelu_parts(e)
            hid = hid.astype(BF16)
            hid_buf[rows, :] = hid
            slope_buf[rows, :] = slope
            out = out + dot(wdt_ref[:, rows], hid)
        sq_ref[u] = squares_of(out)
        final_ref[u] = out.T.astype(BF16)
        gy = cot_ref[u].T
        feed_back_tail(
            u, gy.astype(F32), gy, r_unit, r_inv, m, o_ref[u], small_ref,
            lambda c: (hid_buf[c * BLK : (c + 1) * BLK, :], slope_buf[c * BLK : (c + 1) * BLK, :]),
            w_ref, gr_ref, go_ref, gd_acc, gu_acc, go_acc, tail_acc,
        )
        return carry

    lax.fori_loop(0, UNITS, feed, 0)
    attend_back(
        core, q_ref, k_ref, kt_ref, v_ref, go_ref, o_ref, log_ref, dq_ref, dk_ref, dv_ref, mask_ref, prob_ref, ds_ref, dk_acc, dv_acc
    )


def second_stage(a, z, cot, w, wt, wot, wut, wdt, small):
    tile, eight = (UNITS, BLK, BLK), (ALL, BLK, BLK)
    outs = [shape_of(tile), shape_of((UNITS, 8, BLK), F32), shape_of(tile, F32), shape_of((FF, D), F32)]
    outs += [shape_of((D, FF), F32), shape_of((D, D), F32), shape_of((TAIL, 128), F32), shape_of(tile)]
    outs += [shape_of(eight), shape_of(eight)]
    scratch = [pltpu.VMEM(eight, BF16)] + [pltpu.VMEM(s.shape, s.dtype) for s in KEYS]
    scratch += [pltpu.VMEM((HEADS, VROWS, ALL * BLK), BF16), pltpu.VMEM(tile, BF16)]
    scratch += [pltpu.VMEM((UNITS, 2, 8, BLK), F32), pltpu.VMEM(tile, BF16), ATTEND_SCRATCH[1]]
    scratch += [pltpu.VMEM((FF, BLK), BF16), pltpu.VMEM((FF, BLK), F32)] + BACK_SCRATCH
    return stage_call(
        second_stage_body, "second_stage", [a, z, cot, w, wt, wot, wut, wdt, small], outs, scratch, SECOND_MIB, 20e9
    )


def project_back(z, a, dq, dk, dv, gr, small_ref, w_ref, gqkv_acc, head_acc):
    grad = dot(matrix(w_ref, 0, 0), dq) + dot(matrix(w_ref, 0, 1), dk) + dot(matrix(w_ref, 0, 2), dv)
    gqkv_acc[0] += dot_nt(a, dq)
    gqkv_acc[1] += dot_nt(a, dk)
    gqkv_acc[2] += dot_nt(a, dv)
    unit_values, inverse = standardize(z)
    head_acc[0:D, :] += fold(grad * unit_values)
    head_acc[D : 2 * D, :] += fold(grad)
    return gr + standardize_back(grad * param(small_ref, 0), unit_values, inverse)


def third_stage_body(
    dq_in, dk_in, dv_in, a2_ref, z_ref, gr_in, hid_ref, slope_ref, r_ref, o_ref, log_ref, q_ref, kt_ref, k_ref, v_ref,
    small_ref, w_ref, gd_in, gu_in, go_in, tail_in,
    gz_ref, gr_ref, gd_acc, gu_acc, go_acc, tail_acc, gqkv_acc, head_acc, dq_ref, dk_ref, dv_ref,
    go_ref, mask_ref, prob_ref, ds_ref, dk_acc, dv_acc,
):
    core = lax.axis_index("seq") % 2
    set_mask(mask_ref)
    gqkv_acc[...] = jnp.zeros_like(gqkv_acc)
    head_acc[...] = jnp.zeros_like(head_acc)
    for acc, given in ((gd_acc, gd_in), (gu_acc, gu_in), (go_acc, go_in), (tail_acc, tail_in)):
        acc[...] = given[...]

    def feed(u, carry):
        place, base = unit_place(u, core)
        g = project_back(
            z_ref[u], a2_ref[base + place], dq_in[u], dk_in[u], dv_in[u], gr_in[u], small_ref, w_ref, gqkv_acc, head_acc
        )
        gz_ref[u] = g
        r_unit, r_inv = standardize(r_ref[u])
        m = (r_unit * param(small_ref, 2) + param(small_ref, 3)).astype(BF16)
        feed_back_tail(
            u, g, g.astype(BF16), r_unit, r_inv, m, o_ref[u], small_ref,
            lambda c: (hid_ref[u, c * BLK : (c + 1) * BLK, :], slope_ref[u, c * BLK : (c + 1) * BLK, :].astype(F32)),
            w_ref, gr_ref, go_ref, gd_acc, gu_acc, go_acc, tail_acc,
        )
        return carry

    lax.fori_loop(0, UNITS, feed, 0)
    attend_back(
        core, q_ref, k_ref, kt_ref, v_ref, go_ref, o_ref, log_ref, dq_ref, dk_ref, dv_ref, mask_ref, prob_ref, ds_ref, dk_acc, dv_acc
    )


def third_stage(*args):
    tile, eight = (UNITS, BLK, BLK), (ALL, BLK, BLK)
    outs = [shape_of(tile, F32), shape_of(tile, F32), shape_of((FF, D), F32), shape_of((D, FF), F32)]
    outs += [shape_of((D, D), F32), shape_of((TAIL, 128), F32), shape_of((3, D, D), F32), shape_of((2 * D, 128), F32)]
    outs += [shape_of(tile), shape_of(eight), shape_of(eight)]
    scratch = [pltpu.VMEM(tile, BF16)] + BACK_SCRATCH
    return stage_call(third_stage_body, "third_stage", args, outs, scratch, THIRD_MIB, 16e9)


def last_stage_body(
    n, dq_ref, dk_ref, dv_ref, a_ref, xt_ref, gr_ref, gz_ref, small_ref, w_ref, gqkv_in, head_in,
    gout_ref, gu_ref, gd_ref, tail_ref, sq1_ref, sq2_ref,
    grad_ref, g_ref, p_ref, gqkv_acc, head_acc,
):
    dp = lax.axis_index("dp")
    seq = lax.axis_index("seq")
    chip, core = seq // 2, seq % 2
    gqkv_acc[...] = gqkv_in[...]
    head_acc[...] = head_in[...]

    def end(u, carry):
        place, base = unit_place(u, core)
        g = project_back(
            xt_ref[base + place].astype(F32), a_ref[base + place], dq_ref[u], dk_ref[u], dv_ref[u], gr_ref[u],
            small_ref, w_ref, gqkv_acc, head_acc,
        )
        grad_ref[u] = (g + gz_ref[u]).T.astype(BF16)
        return carry

    lax.fori_loop(0, UNITS, end, 0)
    split = lambda values: values.astype(BF16).reshape(g_ref.shape[2:])
    for t in range(3):
        g_ref[0, t] = split(gqkv_acc[t])
    g_ref[0, 3] = split(gout_ref[...])
    for c in range(4):
        g_ref[1, c] = split(gu_ref[:, c * D : (c + 1) * D])
        g_ref[2, c] = split(gd_ref[c * D : (c + 1) * D, :])
    for row in range(SMALL):
        for side in range(2):
            ref, first = (head_acc, row) if row < 2 else (tail_ref, row - 2)
            first = first * D + side * 128
            p_ref[2 * row + side : 2 * row + side + 1, :] = jnp.sum(ref[first : first + 128, :].T, axis=0, keepdims=True)
    sequences = 6 * n
    place = lax.broadcasted_iota(jnp.int32, (6, 128), 0) * 128 + lax.broadcasted_iota(jnp.int32, (6, 128), 1)
    stats = jnp.zeros((6, 128), F32)
    for i, ref in enumerate((sq1_ref, sq2_ref)):
        lines = [jnp.sum(ref[u], axis=0, keepdims=True) for u in range(UNITS)]
        own = jnp.sum(lines[0] + lines[1] + lines[2] + lines[3], axis=1, keepdims=True)
        half = jnp.sum(lines[4] + lines[5], axis=1, keepdims=True)
        start = i * sequences + 6 * dp + 3 * chip
        stats = jnp.where(place == start + core, jnp.broadcast_to(own, (6, 128)), stats)
        stats = jnp.where(place == start + 2, jnp.broadcast_to(half, (6, 128)), stats)
    p_ref[18:24, :] = stats


def last_stage(n, *args):
    rows = D // n
    outs = [shape_of((UNITS, BLK, BLK)), shape_of((3, 4, n, rows, D)), shape_of((24, 128), F32)]
    scratch = [pltpu.VMEM((3, D, D), F32), pltpu.VMEM((2 * D, 128), F32)]
    return stage_call(partial(last_stage_body, n), "last_stage", args, outs, scratch, LAST_MIB, 3e9)


FIRST_MIB, SECOND_MIB, THIRD_MIB, LAST_MIB = 14, 24, 14, 8


def owner_scalars(owner_ref):
    sizes = [D * D] * 4 + [D * FF, FF * D, SMALL * D]
    starts = []
    for t in range(7):
        offset = jnp.int32(0)
        for u in range(t):
            offset = offset + jnp.where(owner_ref[u] == owner_ref[t], sizes[u], 0).astype(jnp.int32)
        starts.append(offset)
    return starts


def pack_body(owner_ref, row_ref, w_ref, p_ref):
    dp = lax.axis_index("dp")
    seq = lax.axis_index("seq")
    starts = owner_scalars(owner_ref)
    square = jnp.where(seq == 0, starts[0], jnp.where(seq == 1, starts[1], jnp.where(seq == 2, starts[2], starts[3])))
    plans = (
        (owner_ref[seq], square // 128, 2),
        (owner_ref[4], starts[4] // 128 + 2 * seq, FF // 128),
        (owner_ref[5], starts[5] // 128 + 2 * D * seq, 2),
    )
    for kind, (owner, base, stride) in enumerate(plans):
        keep = jnp.where(owner == dp, 1.0, 0.0).astype(F32)
        for side in range(2):
            values = row_ref[pl.ds(base + side, D, stride=stride), :]
            w_ref[kind, :, side * 128 : (side + 1) * 128] = (values * keep).astype(BF16)
    keep = jnp.where(owner_ref[6] == dp, 1.0, 0.0).astype(F32)
    values = row_ref[pl.ds(pl.multiple_of(starts[6] // 128, 8), 24), :] * keep
    rows = lax.broadcasted_iota(jnp.int32, (24, 128), 0)
    p_ref[...] = jnp.where(rows < 2 * SMALL, values, 0.0)


def pack(owner_list, row):
    return pl.pallas_call(
        pack_body,
        in_specs=[pl.BlockSpec(memory_space=pltpu.SMEM), pl.BlockSpec(memory_space=pltpu.VMEM)],
        out_specs=[pl.BlockSpec(memory_space=pltpu.VMEM)] * 2,
        out_shape=[jax.ShapeDtypeStruct((3, D, D), BF16), jax.ShapeDtypeStruct((24, 128), F32)],
        compiler_params=pltpu.CompilerParams(vmem_limit_bytes=20 << 20),
        cost_estimate=cost(1, 3 << 20),
        name="pack",
    )(owner_list, row)


def peers_of(seq):
    return {1: seq + 1 - 2 * (seq % 2), 2: (seq + 2) % 4, 3: 3 - seq}


def greet(n, dp, peers, wide_group):
    barrier = pltpu.get_barrier_semaphore()
    count = 0
    for peer in peers:
        pl.semaphore_signal(barrier, inc=1, device_id={"seq": peer}, device_id_type=MESH)
        count += 1
    if wide_group:
        for k in range(1, n):
            pl.semaphore_signal(barrier, inc=1, device_id={"dp": (dp + k) % n}, device_id_type=MESH)
            count += 1
    pl.semaphore_wait(barrier, count)


def send(source, target, sems, index, device):
    return pltpu.make_async_remote_copy(
        src_ref=source,
        dst_ref=target,
        send_sem=sems[0].at[index],
        recv_sem=sems[1].at[index],
        device_id=device,
        device_id_type=MESH,
    )


def spread(n, dp, seq, peers, kind, w_ref, chunk_ref, row_sems):
    copies = []
    for k in range(1, n):
        copies.append(
            send(chunk_ref.at[kind], w_ref.at[kind, seq, dp], row_sems, (kind, k), {"dp": (dp + k) % n})
        )
        copies[-1].start()
    return copies


def share(seq, peers, kind, w_ref, side_sems):
    copies = [
        send(w_ref.at[kind, seq], w_ref.at[kind, seq], side_sems, (kind, 0), {"seq": peers[2]}),
        send(w_ref.at[kind, seq], w_ref.at[kind, seq], side_sems, (kind, 1), {"seq": peers[1]}),
    ]
    for copy in copies:
        copy.start()
    return copies


def forward(seq, peers, kind, w_ref, side_sems):
    copy = send(w_ref.at[kind, peers[2]], w_ref.at[kind, peers[2]], side_sems, (kind, 2), {"seq": peers[1]})
    copy.start()
    return copy


def entry_body(
    n, pk_ref, pp_ref, x_ref, c_ref, w_ref, p_ref, xo_ref, co_ref, slot_ref, pslot_ref, chunk_ref,
    ss0, ss1, rs0, rs1, ps0, ps1, gs0, gs1, xs0, xs1, cs0, cs1,
):
    dp = lax.axis_index("dp")
    seq = lax.axis_index("seq")
    chip, core = seq // 2, seq % 2
    peers = peers_of(seq)
    greet(n, dp, [peers[1], peers[2], peers[3]], True)
    done = []
    small = []
    scatter = [[] for _ in range(3)]
    for kind in range(3):
        for k in range(1, n):
            to = (dp + k) % n
            copy = send(pk_ref.at[kind, to], slot_ref.at[kind, k], (ss0, ss1), (kind, k), {"dp": to})
            copy.start()
            scatter[kind].append(copy)
        if kind == 0:
            for k in range(1, n):
                copy = send(pp_ref, pslot_ref.at[k], (ps0, ps1), k, {"dp": (dp + k) % n})
                copy.start()
                small.append(copy)
    for o in (2, 3, 1):
        to = peers[o]
        for part, (source, target) in enumerate(((3 * (to // 2) + to % 2, seq), (3 * (to // 2) + 2, OWN + seq))):
            copy = send(x_ref.at[source], xo_ref.at[target], (xs0, xs1), (o, part), {"seq": to})
            copy.start()
            done.append(copy)
    for o in (2, 3, 1):
        to = peers[o]
        copy = send(c_ref.at[3 * (to // 2) + to % 2], co_ref.at[seq], (cs0, cs1), o, {"seq": to})
        copy.start()
        done.append(copy)

    @pl.when(chip == 0)
    def _():
        send(c_ref.at[5], co_ref.at[4], (cs0, cs1), 4 + 2, {"seq": peers[2]}).start()

    @pl.when(chip == 1)
    def _():
        send(c_ref.at[2], co_ref.at[5], (cs0, cs1), 4 + 3, {"seq": peers[3]}).start()
        send(c_ref.at[5], co_ref.at[5], (cs0, cs1), 4 + 1, {"seq": peers[1]}).start()

    xo_ref[seq] = x_ref[3 * chip + core]
    xo_ref[OWN + seq] = x_ref[3 * chip + 2]
    co_ref[seq] = c_ref[3 * chip + core]

    @pl.when(chip == 0)
    def _():
        co_ref[4] = c_ref[2]

    gathers = []
    for kind in range(3):
        total = pk_ref[kind, dp].astype(F32)
        for k in range(1, n):
            scatter[kind][k - 1].wait_recv()
            total = total + slot_ref[kind, k].astype(F32)
        chunk_ref[kind] = total.astype(BF16)
        w_ref[kind, seq, dp] = total.astype(BF16)
        gathers.append(spread(n, dp, seq, peers, kind, w_ref, chunk_ref, (rs0, rs1)))
    sides = []
    for kind in range(3):
        for copy in gathers[kind]:
            copy.wait_recv()
        sides.append(share(seq, peers, kind, w_ref, (gs0, gs1)))
    total = pp_ref[...]
    for copy in small:
        copy.wait_recv()
    for k in range(1, n):
        total = total + pslot_ref[k]
    p_ref[...] = total
    for kind in range(3):
        sides[kind][0].wait_recv()
        sides[kind].append(forward(seq, peers, kind, w_ref, (gs0, gs1)))
    for kind in range(3):
        sides[kind][1].wait_recv()
        sides[kind][2].wait_recv()

    @pl.when(chip == 0)
    def _():
        send(c_ref.at[5], co_ref.at[4], (cs0, cs1), 4 + 2, {"seq": peers[2]}).wait_send()
        send(c_ref.at[2], co_ref.at[5], (cs0, cs1), 4 + 3, {"seq": peers[3]}).wait_recv()

    @pl.when(chip == 1)
    def _():
        send(c_ref.at[2], co_ref.at[5], (cs0, cs1), 4 + 3, {"seq": peers[3]}).wait_send()
        send(c_ref.at[5], co_ref.at[5], (cs0, cs1), 4 + 1, {"seq": peers[1]}).wait_send()
        send(c_ref.at[5], co_ref.at[4], (cs0, cs1), 4 + 2, {"seq": peers[2]}).wait_recv()
        send(c_ref.at[5], co_ref.at[5], (cs0, cs1), 4 + 1, {"seq": peers[1]}).wait_recv()

    for copy in done:
        copy.wait()
    for kind in range(3):
        for copy in scatter[kind] + gathers[kind] + sides[kind]:
            copy.wait_send()
    for copy in small:
        copy.wait_send()


def pair_of_sems(shape):
    return [pltpu.SemaphoreType.DMA(shape), pltpu.SemaphoreType.DMA(shape)]


def entry(n, pk, pp, x, c):
    rows = D // n
    vmem = pl.BlockSpec(memory_space=pltpu.VMEM)
    return pl.pallas_call(
        partial(entry_body, n),
        in_specs=[vmem] * 4,
        out_specs=[vmem] * 4,
        out_shape=[
            jax.ShapeDtypeStruct((3, 4, n, rows, D), BF16),
            jax.ShapeDtypeStruct((24, 128), F32),
            jax.ShapeDtypeStruct((ALL, BLK, BLK), BF16),
            jax.ShapeDtypeStruct((UNITS, BLK, BLK), BF16),
        ],
        scratch_shapes=[
            pltpu.VMEM((3, n, rows, D), BF16),
            pltpu.VMEM((n, 24, 128), F32),
            pltpu.VMEM((3, rows, D), BF16),
            *pair_of_sems((3, n)),
            *pair_of_sems((3, n)),
            *pair_of_sems((n,)),
            *pair_of_sems((3, 3)),
            *pair_of_sems((4, 2)),
            *pair_of_sems((8,)),
        ],
        compiler_params=pltpu.CompilerParams(collective_id=0, has_side_effects=True, vmem_limit_bytes=40 << 20),
        cost_estimate=cost(1, 12 << 20),
        name="entry",
    )(pk, pp, x, c)


def swap_inputs_body(a_ref, out_ref, s0, s1):
    seq = lax.axis_index("seq")
    core = seq % 2
    peers = peers_of(seq)
    greet(1, 0, [peers[1]], False)
    copies = [
        send(a_ref.at[4], out_ref.at[4 + core], (s0, s1), 0, {"seq": peers[1]}),
        send(a_ref.at[5], out_ref.at[7 - core], (s0, s1), 1, {"seq": peers[1]}),
    ]
    for copy in copies:
        copy.start()
    for j in range(OWN):
        out_ref[j] = a_ref[j]
    out_ref[4 + core] = a_ref[4]
    out_ref[7 - core] = a_ref[5]
    for copy in copies:
        copy.wait()


def swap_inputs(a):
    vmem = pl.BlockSpec(memory_space=pltpu.VMEM)
    return pl.pallas_call(
        swap_inputs_body,
        in_specs=[vmem],
        out_specs=vmem,
        out_shape=jax.ShapeDtypeStruct((ALL, BLK, BLK), BF16),
        scratch_shapes=pair_of_sems((2,)),
        compiler_params=pltpu.CompilerParams(collective_id=1, has_side_effects=True, vmem_limit_bytes=16 << 20),
        cost_estimate=cost(1, 2 << 20),
        name="swap_inputs",
    )(a)


def swap_grads_body(dk_ref, dv_ref, dk_out, dv_out, slot_ref, s0, s1):
    seq = lax.axis_index("seq")
    core = seq % 2
    peers = peers_of(seq)
    greet(1, 0, [peers[1]], False)
    copies = []
    for which, ref in enumerate((dk_ref, dv_ref)):
        for place, position in enumerate((5 - core, 6 + core)):
            copies.append(
                send(ref.at[position], slot_ref.at[which, place], (s0, s1), (which, place), {"seq": peers[1]})
            )
            copies[-1].start()
    for ref, out in ((dk_ref, dk_out), (dv_ref, dv_out)):
        for j in range(OWN):
            out[j] = ref[j]
    for copy in copies:
        copy.wait()
    for which, (ref, out) in enumerate(((dk_ref, dk_out), (dv_ref, dv_out))):
        for place, position in enumerate((4 + core, 7 - core)):
            out[4 + place] = (ref[position].astype(F32) + slot_ref[which, place].astype(F32)).astype(BF16)


def swap_grads(dk, dv):
    vmem = pl.BlockSpec(memory_space=pltpu.VMEM)
    out = jax.ShapeDtypeStruct((UNITS, BLK, BLK), BF16)
    return pl.pallas_call(
        swap_grads_body,
        in_specs=[vmem] * 2,
        out_specs=[vmem] * 2,
        out_shape=[out, out],
        scratch_shapes=[pltpu.VMEM((2, 2, BLK, BLK), BF16), *pair_of_sems((2, 2))],
        compiler_params=pltpu.CompilerParams(collective_id=2, has_side_effects=True, vmem_limit_bytes=16 << 20),
        cost_estimate=cost(1, 4 << 20),
        name="swap_grads",
    )(dk, dv)


def leave_body(
    n, g_ref, pp_ref, f_ref, i_ref, w_ref, p_ref, fo_ref, io_ref,
    half_ref, quarter_ref, out_ref, mine_ref, slot_ref, chunk_ref, pslot_ref, psum_ref,
    as0, as1, bs0, bs1, ss0, ss1, rs0, rs1, gs0, gs1, ps0, ps1, xs0, xs1,
):
    dp = lax.axis_index("dp")
    seq = lax.axis_index("seq")
    chip, core = seq // 2, seq % 2
    peers = peers_of(seq)
    greet(n, dp, [peers[1], peers[2], peers[3]], True)
    finish = []

    first = []
    for kind in range(3):
        copies = []
        for j, quarter in enumerate((peers[1], peers[3])):
            copies.append(
                send(g_ref.at[kind, quarter], half_ref.at[kind, j], (as0, as1), (kind, j), {"seq": peers[1]})
            )
            copies[-1].start()
        first.append(copies)
        finish += copies
    small = [send(pp_ref, pslot_ref.at[0], (ps0, ps1), 0, {"seq": peers[1]})]
    small[0].start()

    moves = []
    own = 3 * chip + core

    def move(which, source_ref, target_ref):
        for o in (2, 3, 1):
            copy = send(source_ref.at[peers[o]], target_ref.at[own], (xs0, xs1), (which, o), {"seq": peers[o]})
            copy.start()
            moves.append(copy)

        @pl.when(chip == 0)
        def _():
            send(source_ref.at[5], target_ref.at[2], (xs0, xs1), (which, 4 + 3), {"seq": peers[3]}).start()

        @pl.when(chip == 1)
        def _():
            send(source_ref.at[4], target_ref.at[5], (xs0, xs1), (which, 4 + 2), {"seq": peers[2]}).start()
            send(source_ref.at[5], target_ref.at[5], (xs0, xs1), (which, 4 + 1), {"seq": peers[1]}).start()

        target_ref[own] = source_ref[seq]

        @pl.when(chip == 0)
        def _():
            target_ref[2] = source_ref[4]

    def settle(which, source_ref, target_ref):
        @pl.when(chip == 0)
        def _():
            send(source_ref.at[5], target_ref.at[2], (xs0, xs1), (which, 4 + 3), {"seq": peers[3]}).wait_send()
            send(source_ref.at[4], target_ref.at[5], (xs0, xs1), (which, 4 + 2), {"seq": peers[2]}).wait_recv()

        @pl.when(chip == 1)
        def _():
            send(source_ref.at[4], target_ref.at[5], (xs0, xs1), (which, 4 + 2), {"seq": peers[2]}).wait_send()
            send(source_ref.at[5], target_ref.at[5], (xs0, xs1), (which, 4 + 1), {"seq": peers[1]}).wait_send()
            send(source_ref.at[5], target_ref.at[2], (xs0, xs1), (which, 4 + 3), {"seq": peers[3]}).wait_recv()
            send(source_ref.at[5], target_ref.at[5], (xs0, xs1), (which, 4 + 1), {"seq": peers[1]}).wait_recv()

    second = []
    for kind in range(3):
        for copy in first[kind]:
            copy.wait_recv()
        out_ref[kind] = (g_ref[kind, peers[2]].astype(F32) + half_ref[kind, 1].astype(F32)).astype(BF16)
        second.append(send(out_ref.at[kind], quarter_ref.at[kind], (bs0, bs1), kind, {"seq": peers[2]}))
        second[-1].start()
    finish += second
    small[0].wait_recv()
    psum_ref[0] = pp_ref[...] + pslot_ref[0]
    small.append(send(psum_ref.at[0], pslot_ref.at[1], (ps0, ps1), 1, {"seq": peers[2]}))
    small[1].start()
    move(0, f_ref, fo_ref)
    move(1, i_ref, io_ref)

    scatter = []
    for kind in range(3):
        second[kind].wait_recv()
        mine_ref[kind] = (
            g_ref[kind, seq].astype(F32) + half_ref[kind, 0].astype(F32) + quarter_ref[kind].astype(F32)
        ).astype(BF16)
        copies = []
        for k in range(1, n):
            to = (dp + k) % n
            copies.append(send(mine_ref.at[kind, to], slot_ref.at[kind, k], (ss0, ss1), (kind, k), {"dp": to}))
            copies[-1].start()
        scatter.append(copies)
        finish += copies
    small[1].wait_recv()
    psum_ref[1] = psum_ref[0] + pslot_ref[1]
    for k in range(1, n):
        copy = send(psum_ref.at[1], pslot_ref.at[1 + k], (ps0, ps1), 1 + k, {"dp": (dp + k) % n})
        copy.start()
        small.append(copy)
    gathers = []
    for kind in range(3):
        total = mine_ref[kind, dp].astype(F32)
        for k in range(1, n):
            scatter[kind][k - 1].wait_recv()
            total = total + slot_ref[kind, k].astype(F32)
        chunk_ref[kind] = total.astype(BF16)
        w_ref[kind, seq, dp] = total.astype(BF16)
        gathers.append(spread(n, dp, seq, peers, kind, w_ref, chunk_ref, (rs0, rs1)))
    sides = []
    for kind in range(3):
        for copy in gathers[kind]:
            copy.wait_recv()
        sides.append(share(seq, peers, kind, w_ref, (gs0, gs1)))
        finish += gathers[kind]
    total = psum_ref[1]
    for k in range(1, n):
        small[1 + k].wait_recv()
        total = total + pslot_ref[1 + k]
    p_ref[...] = total
    for kind in range(3):
        sides[kind][0].wait_recv()
        sides[kind].append(forward(seq, peers, kind, w_ref, (gs0, gs1)))
    for kind in range(3):
        sides[kind][1].wait_recv()
        sides[kind][2].wait_recv()
        finish += sides[kind]
    settle(0, f_ref, fo_ref)
    settle(1, i_ref, io_ref)
    for copy in moves:
        copy.wait()
    for copy in finish + small:
        copy.wait_send()


def leave(n, g, pp, f, i):
    rows = D // n
    vmem = pl.BlockSpec(memory_space=pltpu.VMEM)
    return pl.pallas_call(
        partial(leave_body, n),
        in_specs=[vmem] * 4,
        out_specs=[vmem] * 4,
        out_shape=[
            jax.ShapeDtypeStruct((3, 4, n, rows, D), BF16),
            jax.ShapeDtypeStruct((24, 128), F32),
            jax.ShapeDtypeStruct((UNITS, BLK, BLK), BF16),
            jax.ShapeDtypeStruct((UNITS, BLK, BLK), BF16),
        ],
        scratch_shapes=[
            pltpu.VMEM((3, 2, n, rows, D), BF16),
            pltpu.VMEM((3, n, rows, D), BF16),
            pltpu.VMEM((3, n, rows, D), BF16),
            pltpu.VMEM((3, n, rows, D), BF16),
            pltpu.VMEM((3, n, rows, D), BF16),
            pltpu.VMEM((3, rows, D), BF16),
            pltpu.VMEM((1 + n, 24, 128), F32),
            pltpu.VMEM((2, 24, 128), F32),
            *pair_of_sems((3, 2)),
            *pair_of_sems((3,)),
            *pair_of_sems((3, n)),
            *pair_of_sems((3, n)),
            *pair_of_sems((3, 3)),
            *pair_of_sems((1 + n,)),
            *pair_of_sems((2, 8)),
        ],
        compiler_params=pltpu.CompilerParams(collective_id=3, has_side_effects=True, vmem_limit_bytes=48 << 20),
        cost_estimate=cost(1, 20 << 20),
        name="leave",
    )(g, pp, f, i)


ROWS = D * D // 128


def adam_body(owner_ref, g_ref, p_ref, m_ref, v_ref, w_ref, m_out, v_out, w_out, grad_ref):
    dp = lax.axis_index("dp")
    block = pl.program_id(0)
    starts = owner_scalars(owner_ref)
    counts = [1, 1, 1, 1, 4, 4, 1]
    rate = jnp.float32(D ** (-0.5))
    decay = jnp.float32(0.1)
    limit = jnp.int32(0)
    for t in range(7):
        first = starts[t] // (D * D)
        here = (owner_ref[t] == dp) & (block >= first) & (block < first + counts[t])
        part = block - first
        limit = jnp.where(here, 2 * SMALL if t == 6 else ROWS, limit)
        if t == 5:
            rate = jnp.where(here, FF ** (-0.5), rate)
        if t == 6:
            rate = jnp.where(here, 0.5, rate)
            decay = jnp.where(here, 0.0, decay)

        @pl.when(here)
        def _(t=t, part=part):
            if t == 6:
                grad_ref[0:24, :] = p_ref[...]
            elif t == 4:
                for c in range(4):
                    piece = g_ref[4 + c, pl.ds(pl.multiple_of(part * 64, 64), 64), :].astype(F32)
                    for side in range(2):
                        grad_ref[pl.ds(2 * c + side, 64, stride=8), :] = piece[:, side * 128 : (side + 1) * 128]
            else:
                piece = g_ref[8 + part if t == 5 else t].astype(F32)
                for side in range(2):
                    grad_ref[pl.ds(side, D, stride=2), :] = piece[:, side * 128 : (side + 1) * 128]

    @pl.when(limit == 0)
    def _():
        for out in (m_out, v_out, w_out):
            out[...] = jnp.zeros_like(out)

    @pl.when(limit > 0)
    def _():
        correction = 1.0 - 0.5**STEP
        grad = grad_ref[...]
        valid = lax.broadcasted_iota(jnp.int32, (ROWS, 128), 0) < limit
        first_new = 0.5 * m_ref[...] + 0.5 * grad
        second_new = 0.5 * v_ref[...] + 0.5 * grad * grad
        old = w_ref[...]
        update = first_new / correction / (jnp.sqrt(second_new / correction) + adam_eps) + decay * old
        m_out[...] = jnp.where(valid, first_new, 0.0)
        v_out[...] = jnp.where(valid, second_new, 0.0)
        w_out[...] = jnp.where(valid, old - rate * update, 0.0)


def adam(owner_list, g, p, m, v, w):
    tile = pl.BlockSpec((ROWS, 128), lambda b, t: (b, 0))
    out = jax.ShapeDtypeStruct(m.shape, F32)
    spec = pltpu.PrefetchScalarGridSpec(
        num_scalar_prefetch=1,
        grid=(m.shape[0] // ROWS,),
        in_specs=[full(g.shape), full(p.shape), tile, tile, tile],
        out_specs=[tile, tile, tile],
        scratch_shapes=[pltpu.VMEM((ROWS, 128), F32)],
    )
    return pl.pallas_call(
        adam_body,
        grid_spec=spec,
        out_shape=[out, out, out],
        compiler_params=params_of(),
        cost_estimate=cost(20 * 524288, 14 << 20),
        name="adam",
    )(owner_list, g, p, m, v, w)


def per_device(inputs, cotangent, owner_list, master_rows, moment1_rows, moment2_rows):
    n = lax.axis_size("dp")
    rows = D // n
    flat = [r.reshape(-1, 128) for r in (master_rows, moment1_rows, moment2_rows)]
    pk, pp = pack(owner_list, flat[0])
    w, p, x, cot = entry(n, pk.reshape(3, n, rows, D), pp, inputs, cotangent)
    (xt, a1, q1, kt1, k1, v1, o1, log1, r1, hid, slope, z2, a2, sq1, wt, wot, wut, wdt, small) = first_stage(x, w, p)
    a2 = swap_inputs(a2)
    final, sq2, gr, gd, gu, gout, tail, dq, dk, dv = second_stage(a2, z2, cot, w, wt, wot, wut, wdt, small)
    dk, dv = swap_grads(dk, dv)
    gz, gr, gd, gu, gout, tail, gqkv, head, dq, dk, dv = third_stage(
        dq, dk, dv, a2, z2, gr, hid, slope, r1, o1, log1, q1, kt1, k1, v1, small, w, gd, gu, gout, tail
    )
    dk, dv = swap_grads(dk, dv)
    grad, g, pp = last_stage(n, dq, dk, dv, a1, xt, gr, gz, small, w, gqkv, head, gout, gu, gd, tail, sq1, sq2)
    g, p, final, grad = leave(n, g, pp, final, grad)
    m_new, v_new, w_new = adam(owner_list, g.reshape(12, D, D), p, flat[1], flat[2], flat[0])
    sequences = inputs.shape[0] * n
    entries = inputs.shape[1] * lax.axis_size("seq") * D
    squares = p[18:].reshape(-1)[: 2 * sequences].reshape(2, sequences)
    stats = jnp.sqrt(squares / entries + stat_eps)
    back = lambda r: r.reshape(master_rows.shape)
    return (final.astype(F32), grad.astype(F32), stats, back(m_new), back(v_new), back(w_new))


def solution(mesh):
    placed = (P("dp", "seq", None), P("dp", "seq", None), P(), P("dp", None), P("dp", None), P("dp", None))
    return jax.shard_map(
        per_device,
        mesh=mesh,
        in_specs=placed,
        out_specs=(P("dp", "seq", None), P("dp", "seq", None), P(), P("dp", None), P("dp", None), P("dp", None)),
        check_vma=False,
    )
```

```python
import math
from functools import partial

import jax
import jax.numpy as jnp
from jax import lax
from jax.experimental import pallas as pl
from jax.experimental.pallas import tpu as pltpu
from jax.sharding import PartitionSpec as P

D = 256
HEADS = 4
HD = 64
FF = 1024
STEP = 3
SMALL = 9
BLK = 256
OWN = 4
UNITS = 6
ALL = 8
F32 = jnp.float32
BF16 = jnp.bfloat16
MESH = pl.DeviceIdType.MESH

norm_eps = 1e-05
stat_eps = 1e-06
adam_eps = 1e-08
masked_score = -1e30


def dot(left, right):
    return lax.dot_general(left, right, (((1,), (0,)), ((), ())), preferred_element_type=F32)


def dot_nt(left, right):
    return lax.dot_general(left, right, (((1,), (1,)), ((), ())), preferred_element_type=F32)


def wide(column):
    return jnp.concatenate([column, column], axis=1)


def fold(values):
    return values[:, :128] + values[:, 128:]


def standardize(values):
    average = jnp.mean(values, axis=0, keepdims=True)
    centered = values - average
    spread = jnp.mean(centered * centered, axis=0, keepdims=True)
    inverse = lax.rsqrt(spread + norm_eps)
    return centered * inverse, inverse


def standardize_back(grad, unit_values, inverse):
    average = jnp.mean(grad, axis=0, keepdims=True)
    inner = jnp.mean(grad * unit_values, axis=0, keepdims=True)
    return (grad - average - unit_values * inner) * inverse


def param(small_ref, row):
    return wide(small_ref[row * D : (row + 1) * D, :])


def gelu_parts(e):
    cdf = 0.5 * lax.erf(e * math.sqrt(0.5)) + 0.5
    hid = e * cdf
    slope = cdf + e * (jnp.exp(-0.5 * e * e) * (1.0 / math.sqrt(2.0 * math.pi)))
    return hid, slope


def full(shape):
    return pl.BlockSpec(shape, lambda *args: (0,) * len(shape), pipeline_mode=pl.Buffered(1))


def params_of(ndims=1, mib=56):
    return pltpu.CompilerParams(
        dimension_semantics=("arbitrary",) * ndims, vmem_limit_bytes=mib << 20
    )


def cost(flops, nbytes, trans=0):
    return pl.CostEstimate(flops=int(flops), bytes_accessed=int(nbytes), transcendentals=int(trans))


LOG2E = math.log2(math.e)
VROWS = HD + 16


def unit_place(unit, core):
    later = unit // OWN
    place = (1 - later) * unit + later * (core + (unit - OWN) * (3 - 2 * core))
    return place, later * OWN


def lanes(start, size):
    return pl.ds(pl.multiple_of(start, BLK), size)


def pair_rows(pair):
    return pl.ds(pl.multiple_of(pair * 128, 128), 128)


def matrix(w_ref, kind, part):
    n, rows = w_ref.shape[2:4]
    if rows % 16 == 0:
        return w_ref[kind, part].reshape(D, D)
    return jnp.concatenate([w_ref[kind, part, i] for i in range(n)], axis=0)


def project(j, a, wt_ref, q_ref, kt_ref, vt_ref, k_ref, v_ref):
    where = lanes(j * BLK, BLK)
    q_ref[j] = (dot(wt_ref[0:D], a) * HD ** (-0.5)).astype(BF16)
    kt = dot(wt_ref[D : 2 * D], a).astype(BF16)
    vt = dot(wt_ref[2 * D : 3 * D], a).astype(BF16)
    for h in range(HEADS):
        kt_ref[h, :, where] = kt[h * HD : (h + 1) * HD]
        vt_ref[h, 0:HD, where] = vt[h * HD : (h + 1) * HD]
    k = kt.T
    v = vt.T
    for h in range(2):
        k_ref[h, j] = k[:, h * 128 : (h + 1) * 128]
        v_ref[h, j] = v[:, h * 128 : (h + 1) * 128]


def head_rows(values, half):
    rows = lax.broadcasted_iota(jnp.int32, values.shape, 0)
    keep = (rows < HD) if half == 0 else (rows >= HD)
    return jnp.where(keep, values, jnp.zeros_like(values))


def set_mask(mask_ref):
    keys = lax.broadcasted_iota(jnp.int32, (BLK, BLK), 0)
    queries = lax.broadcasted_iota(jnp.int32, (BLK, BLK), 1)
    mask_ref[...] = jnp.where(keys <= queries, 0.0, masked_score)


def groups(values, op):
    out = values[0:8]
    for i in range(1, values.shape[0] // 8):
        out = op(out, values[i * 8 : (i + 1) * 8])
    return out


SUB = 128


def attend(core, q_ref, k_ref, vt_ref, o_ref, log_ref, mask_ref, score_ref, prob_ref, progress=None):
    def step(i, carry):
        if progress is not None:
            progress(i)
        pair, unit = i // UNITS, i % UNITS
        place, base = unit_place(unit, core)

        def branch(last):
            block = q_ref[base + place, pair_rows(pair), :]
            for half in range(2):
                q = head_rows(block, half)
                top = None
                for kb in range(last + 1):
                    for sub in range(BLK // SUB):
                        rows = slice(sub * SUB, (sub + 1) * SUB)
                        score = dot(k_ref[pair, base + kb, rows, :], q)
                        if kb == last:
                            score = score + mask_ref[rows, :]
                        score_ref[half, kb, rows, :] = score
                        peak = groups(score, jnp.maximum)
                        top = peak if top is None else jnp.maximum(top, peak)
                top = jnp.max(top, axis=0, keepdims=True)
                for kb in range(last + 1):
                    for sub in range(BLK // SUB):
                        rows = slice(sub * SUB, (sub + 1) * SUB)
                        weight = jnp.exp(score_ref[half, kb, rows, :] - top)
                        prob_ref[half, kb * BLK + sub * SUB : kb * BLK + (sub + 1) * SUB, :] = weight.astype(BF16)
                keys = (last + 1) * BLK
                out = dot(vt_ref[2 * pair + half, :, lanes(base * BLK, keys)], prob_ref[half, 0:keys, :])
                total = out[HD : HD + 1]
                o_ref[unit, pl.ds(pl.multiple_of(pair * 128 + half * HD, HD), HD), :] = (out[0:HD] / total).astype(BF16)
                log_ref[unit, pair, half : half + 1, :] = top + jnp.log(total)

        for last in range(OWN):
            pl.when(place == last)(partial(branch, last))
        return carry

    lax.fori_loop(0, 2 * UNITS, step, 0)


def attend_back(
    core, q_ref, k_ref, kt_ref, v_ref, go_ref, o_ref, log_ref, dq_ref, dk_ref, dv_ref, mask_ref, prob_ref, slope_ref, dk_acc, dv_acc
):
    dk_acc[...] = jnp.zeros_like(dk_acc)
    dv_acc[...] = jnp.zeros_like(dv_acc)

    def step(i, carry):
        pair, unit = i // UNITS, i % UNITS
        place, base = unit_place(unit, core)

        def branch(last):
            block = q_ref[base + place, pair_rows(pair), :]
            go_block = go_ref[unit, pair_rows(pair), :]
            o_block = o_ref[unit, pair_rows(pair), :]
            keys = (last + 1) * BLK
            for half in range(2):
                lo, hi = half * HD, (half + 1) * HD
                q = head_rows(block, half)
                go = head_rows(go_block, half)
                q_head = block[lo:hi]
                go_head = go_block[lo:hi]
                log_total = log_ref[unit, pair, half : half + 1, :]
                inner = jnp.sum(go_head.astype(F32) * o_block[lo:hi].astype(F32), axis=0, keepdims=True)
                for kb in range(last + 1):
                    for sub in range(BLK // SUB):
                        rows = slice(sub * SUB, (sub + 1) * SUB)
                        to = slice(kb * BLK + sub * SUB, kb * BLK + (sub + 1) * SUB)
                        score = dot(k_ref[pair, base + kb, rows, :], q)
                        if kb == last:
                            score = score + mask_ref[rows, :]
                        weight = jnp.exp(score - log_total)
                        slope = dot(v_ref[pair, base + kb, rows, :], go)
                        prob_ref[half, to, :] = weight.astype(BF16)
                        slope_ref[half, to, :] = (weight * (slope - inner)).astype(BF16)
                head = 2 * pair + half
                where = lanes(base * BLK, keys)
                dv_acc[head, :, where] += dot_nt(go_head, prob_ref[half, 0:keys, :])
                dk_acc[head, :, where] += dot_nt(q_head, slope_ref[half, 0:keys, :])
                dq = dot(kt_ref[head, :, where], slope_ref[half, 0:keys, :])
                dq_ref[unit, pl.ds(pl.multiple_of(pair * 128 + lo, HD), HD), :] = (dq * HD ** (-0.5)).astype(BF16)

        for last in range(OWN):
            pl.when(place == last)(partial(branch, last))
        return carry

    lax.fori_loop(0, 2 * UNITS, step, 0)
    for j in range(ALL):
        for ref, acc in ((dk_ref, dk_acc), (dv_ref, dv_acc)):
            ref[j] = acc[:, :, j * BLK : (j + 1) * BLK].reshape(D, BLK).astype(BF16)


def forward_parts(z, o, wot_ref, small_ref):
    r = z + dot(wot_ref[...], o)
    unit_values, inverse = standardize(r)
    m = (unit_values * param(small_ref, 2) + param(small_ref, 3)).astype(BF16)
    return r, unit_values, inverse, m


def squares_of(out):
    return groups(out * out, jnp.add)


def first_stage_body(
    n, pk_ref, pp_ref, x_ref, c_ref,
    xt_ref, a_ref, q_ref, kt_ref, k_ref, v_ref, o_ref, log_ref, r_ref, hid_ref, slope_ref, z_ref, a2_ref, sq_ref,
    wt_ref, wot_ref, wut_ref, wdt_ref, small_ref, w_ref, co_ref,
    vt_ref, mask_ref, score_ref, prob_ref, xo_ref, slot_ref, pslot_ref, chunk_ref,
    ss0, ss1, rs0, rs1, ps0, ps1, gs0, gs1, xs0, xs1, cs0, cs1,
):
    dp = lax.axis_index("dp")
    seq = lax.axis_index("seq")
    chip, core = seq // 2, seq % 2
    peers = peers_of(seq)

    def scatter(kind, k):
        to = (dp + k) % n
        return send(pk_ref.at[kind, to], slot_ref.at[kind, k], (ss0, ss1), (kind, k), {"dp": to})

    def small(k):
        return send(pp_ref, pslot_ref.at[k], (ps0, ps1), k, {"dp": (dp + k) % n})

    def gather(kind, k):
        return send(chunk_ref.at[kind], w_ref.at[kind, seq, dp], (rs0, rs1), (kind, k), {"dp": (dp + k) % n})

    def side(kind, which):
        part = peers[2] if which == 2 else seq
        to = peers[2] if which == 0 else peers[1]
        return send(w_ref.at[kind, part], w_ref.at[kind, part], (gs0, gs1), (kind, which), {"seq": to})

    def own(o):
        to = peers[o]
        return send(x_ref.at[3 * (to // 2) + to % 2], xo_ref.at[seq], (xs0, xs1), (o, 0), {"seq": to})

    def shared(o):
        if o == 3:
            there = xo_ref.at[OWN + peers[2]]
            return send(there, there, (xs0, xs1), (3, 1), {"seq": peers[1]})
        to = peers[o]
        return send(x_ref.at[3 * (to // 2) + 2], xo_ref.at[OWN + seq], (xs0, xs1), (o, 1), {"seq": to})

    def target(o):
        to = peers[o]
        return send(c_ref.at[3 * (to // 2) + to % 2], co_ref.at[seq], (cs0, cs1), o, {"seq": to})

    def target_shared(o):
        slot = 4 if o == 2 else 5
        return send(c_ref.at[2 if o == 3 else 5], co_ref.at[slot], (cs0, cs1), 4 + o, {"seq": peers[o]})

    def sum_up(kind):
        total = pk_ref[kind, dp].astype(F32)
        for k in range(1, n):
            scatter(kind, k).wait_recv()
            total = total + slot_ref[kind, k].astype(F32)
        chunk_ref[kind] = total.astype(BF16)
        w_ref[kind, seq, dp] = total.astype(BF16)

    offsets = range(1, n)
    greet(n, dp, [peers[1], peers[2], peers[3]], True)
    for k in offsets:
        scatter(0, k).start()
    for o in (2, 1):
        shared(o).start()
    for o in (2, 3, 1):
        own(o).start()
    for k in offsets:
        small(k).start()
    xo_ref[seq] = x_ref[3 * chip + core]
    xo_ref[OWN + seq] = x_ref[3 * chip + 2]
    co_ref[seq] = c_ref[3 * chip + core]
    pl.when(chip == 0)(lambda: co_ref.__setitem__(4, c_ref[2]))
    set_mask(mask_ref)
    vt_ref[:, HD:, :] = jnp.ones((HEADS, VROWS - HD, ALL * BLK), BF16)
    sum_up(0)
    for k in offsets:
        gather(0, k).start()
    for kind in (1, 2):
        for k in offsets:
            scatter(kind, k).start()
    total = pp_ref[...]
    for k in offsets:
        small(k).wait_recv()
        total = total + pslot_ref[k]
    for row in range(SMALL):
        for part in range(2):
            line = jnp.broadcast_to(total[2 * row + part : 2 * row + part + 1, :], (128, 128))
            small_ref[row * D + part * 128 : row * D + (part + 1) * 128, :] = line.T
    shared(2).wait_recv()
    shared(3).start()
    for o in (2, 3, 1):
        own(o).wait_recv()
    shared(1).wait_recv()
    for k in offsets:
        gather(0, k).wait_recv()
    side(0, 0).start()
    side(0, 1).start()
    for o in (2, 3, 1):
        target(o).start()
    pl.when(chip == 0)(lambda: target_shared(2).start())
    pl.when(chip == 1)(lambda: target_shared(3).start())
    pl.when(chip == 1)(lambda: target_shared(1).start())
    shared(3).wait_recv()

    def begin(j, carry):
        xt = xo_ref[j].T
        xt_ref[j] = xt
        unit_values, _ = standardize(xt.astype(F32))
        a_ref[j] = (unit_values * param(small_ref, 0) + param(small_ref, 1)).astype(BF16)
        return carry

    lax.fori_loop(0, ALL, begin, 0)
    side(0, 0).wait_recv()
    side(0, 2).start()
    side(0, 1).wait_recv()
    side(0, 2).wait_recv()
    for t in range(3):
        wt_ref[t * D : (t + 1) * D, :] = matrix(w_ref, 0, t).T

    def middle(j, carry):
        project(j, a_ref[j], wt_ref, q_ref, kt_ref, vt_ref, k_ref, v_ref)
        return carry

    lax.fori_loop(0, ALL, middle, 0)
    for kind in (1, 2):
        sum_up(kind)
        for k in offsets:
            gather(kind, k).start()

    def progress(i):
        @pl.when(i == 5)
        def _():
            for kind in (1, 2):
                for k in offsets:
                    gather(kind, k).wait_recv()
                side(kind, 0).start()
                side(kind, 1).start()

        @pl.when(i == 10)
        def _():
            for kind in (1, 2):
                side(kind, 0).wait_recv()
                side(kind, 2).start()

    attend(core, q_ref, k_ref, vt_ref, o_ref, log_ref, mask_ref, score_ref, prob_ref, progress)
    wot_ref[...] = matrix(w_ref, 0, 3).T
    for kind in (1, 2):
        side(kind, 1).wait_recv()
        side(kind, 2).wait_recv()
    for c in range(4):
        part = slice(c * D, (c + 1) * D)
        wut_ref[part, :] = matrix(w_ref, 1, c).T
        wdt_ref[:, part] = matrix(w_ref, 2, c).T

    def feed(u, carry):
        place, base = unit_place(u, core)
        x = xt_ref[base + place].astype(F32)
        r, _, _, m = forward_parts(x, o_ref[u], wot_ref, small_ref)
        r_ref[u] = r
        out = r + param(small_ref, 4)
        for c in range(FF // BLK):
            rows = slice(c * BLK, (c + 1) * BLK)
            e = dot(wut_ref[rows, :], m) + param(small_ref, 5 + c)
            hid, slope = gelu_parts(e)
            hid = hid.astype(BF16)
            hid_ref[u, rows, :] = hid
            slope_ref[u, rows, :] = slope.astype(BF16)
            out = out + dot(wdt_ref[:, rows], hid)
        sq_ref[u] = squares_of(out)
        z = out + x
        z_ref[u] = z
        unit_values, _ = standardize(z)
        a2_ref[u] = (unit_values * param(small_ref, 0) + param(small_ref, 1)).astype(BF16)
        return carry

    lax.fori_loop(0, UNITS, feed, 0)
    for o in (2, 3, 1):
        target(o).wait()
        own(o).wait_send()
        shared(o).wait_send()

    @pl.when(chip == 0)
    def _():
        target_shared(2).wait_send()
        target_shared(3).wait_recv()

    @pl.when(chip == 1)
    def _():
        target_shared(3).wait_send()
        target_shared(1).wait_send()
        target_shared(2).wait_recv()
        target_shared(1).wait_recv()

    for kind in range(3):
        for k in offsets:
            scatter(kind, k).wait_send()
            gather(kind, k).wait_send()
        for which in range(3):
            side(kind, which).wait_send()
    for k in offsets:
        small(k).wait_send()


def pair_of_sems(shape):
    return [pltpu.SemaphoreType.DMA(shape), pltpu.SemaphoreType.DMA(shape)]


VM = pl.BlockSpec(memory_space=pltpu.VMEM)


def shape_of(shape, dtype=BF16):
    return jax.ShapeDtypeStruct(shape, dtype)


KEYS = [
    shape_of((HEADS, HD, ALL * BLK)),
    shape_of((2, ALL, BLK, 128)),
    shape_of((2, ALL, BLK, 128)),
]
ATTEND_SCRATCH = [
    pltpu.VMEM((BLK, BLK), F32),
    pltpu.VMEM((2, OWN, BLK, BLK), F32),
    pltpu.VMEM((2, OWN * BLK, BLK), BF16),
]
BACK_SCRATCH = [
    pltpu.VMEM((BLK, BLK), F32),
    pltpu.VMEM((2, OWN * BLK, BLK), BF16),
    pltpu.VMEM((2, OWN * BLK, BLK), BF16),
    pltpu.VMEM((HEADS, HD, ALL * BLK), F32),
    pltpu.VMEM((HEADS, HD, ALL * BLK), F32),
]


def stage_call(body, name, args, outs, scratch, mib, flops, **comm):
    return pl.pallas_call(
        body,
        in_specs=[VM] * len(args),
        out_specs=[VM] * len(outs),
        out_shape=outs,
        scratch_shapes=scratch,
        compiler_params=pltpu.CompilerParams(vmem_limit_bytes=mib << 20, has_side_effects=bool(comm), **comm),
        cost_estimate=cost(flops, 1 << 20),
        name=name,
    )(*args)


def first_stage(n, pk, pp, x, c):
    rows = D // n
    tile, eight = (UNITS, BLK, BLK), (ALL, BLK, BLK)
    outs = [shape_of(eight), shape_of(eight), shape_of(eight)] + KEYS
    outs += [shape_of(tile), shape_of((UNITS, 2, 8, BLK), F32), shape_of(tile, F32)]
    outs += [shape_of((UNITS, FF, BLK)), shape_of((UNITS, FF, BLK)), shape_of(tile, F32), shape_of(tile)]
    outs += [shape_of((UNITS, 8, BLK), F32), shape_of((3 * D, D)), shape_of((D, D)), shape_of((FF, D))]
    outs += [shape_of((D, FF)), shape_of((SMALL * D, 128), F32), shape_of((3, 4, n, rows, D)), shape_of(tile)]
    scratch = [pltpu.VMEM((HEADS, VROWS, ALL * BLK), BF16)] + ATTEND_SCRATCH
    scratch += [
        pltpu.VMEM(eight, BF16),
        pltpu.VMEM((3, n, rows, D), BF16),
        pltpu.VMEM((n, 24, 128), F32),
        pltpu.VMEM((3, rows, D), BF16),
        *pair_of_sems((3, n)),
        *pair_of_sems((3, n)),
        *pair_of_sems((n,)),
        *pair_of_sems((3, 3)),
        *pair_of_sems((4, 2)),
        *pair_of_sems((8,)),
    ]
    return stage_call(
        partial(first_stage_body, n), "first_stage", [pk, pp, x, c], outs, scratch, FIRST_MIB, 8e9, collective_id=0
    )


def feed_back_tail(
    u, g, gy, r_unit, r_inv, m, o, small_ref, parts, w_ref, gr_ref, go_ref, gd_acc, gu_acc, go_acc, tail_acc
):
    tail_acc[2 * D : 3 * D, :] += fold(gy.astype(F32))
    gm = jnp.zeros((D, BLK), F32)
    for c in range(FF // BLK):
        rows = slice(c * BLK, (c + 1) * BLK)
        hid, slope = parts(c)
        gd_acc[rows, :] += dot_nt(hid, gy)
        ge = (dot(matrix(w_ref, 2, c), gy) * slope).astype(BF16)
        gu_acc[:, rows] += dot_nt(m, ge)
        tail_acc[3 * D + c * BLK : 3 * D + (c + 1) * BLK, :] += fold(ge.astype(F32))
        gm = gm + dot(matrix(w_ref, 1, c), ge)
    tail_acc[0:D, :] += fold(gm * r_unit)
    tail_acc[D : 2 * D, :] += fold(gm)
    gr = g + standardize_back(gm * param(small_ref, 2), r_unit, r_inv)
    gr_ref[u] = gr
    ga = gr.astype(BF16)
    go_acc[...] += dot_nt(o, ga)
    go_ref[u] = dot(matrix(w_ref, 0, 3), ga).astype(BF16)


TAIL = 3 * D + FF


def second_stage_body(
    a_ref, z_ref, cot_ref, w_ref, wt_ref, wot_ref, wut_ref, wdt_ref, small_ref,
    final_ref, sq_ref, gr_ref, gd_acc, gu_acc, go_acc, tail_acc, dq_ref, dk_ref, dv_ref,
    q_ref, kt_ref, k_ref, v_ref, vt_ref, o_ref, log_ref, go_ref, score_ref, hid_buf, slope_buf,
    mask_ref, prob_ref, ds_ref, dk_acc, dv_acc,
):
    core = lax.axis_index("seq") % 2
    set_mask(mask_ref)
    vt_ref[:, HD:, :] = jnp.ones((HEADS, VROWS - HD, ALL * BLK), BF16)
    for acc in (gd_acc, gu_acc, go_acc, tail_acc):
        acc[...] = jnp.zeros_like(acc)

    def begin(j, carry):
        project(j, a_ref[j], wt_ref, q_ref, kt_ref, vt_ref, k_ref, v_ref)
        return carry

    lax.fori_loop(0, ALL, begin, 0)
    attend(core, q_ref, k_ref, vt_ref, o_ref, log_ref, mask_ref, score_ref, prob_ref)

    def feed(u, carry):
        r, r_unit, r_inv, m = forward_parts(z_ref[u], o_ref[u], wot_ref, small_ref)
        out = r + param(small_ref, 4)
        for c in range(FF // BLK):
            rows = slice(c * BLK, (c + 1) * BLK)
            e = dot(wut_ref[rows, :], m) + param(small_ref, 5 + c)
            hid, slope = gelu_parts(e)
            hid = hid.astype(BF16)
            hid_buf[rows, :] = hid
            slope_buf[rows, :] = slope
            out = out + dot(wdt_ref[:, rows], hid)
        sq_ref[u] = squares_of(out)
        final_ref[u] = out.T.astype(BF16)
        gy = cot_ref[u].T
        feed_back_tail(
            u, gy.astype(F32), gy, r_unit, r_inv, m, o_ref[u], small_ref,
            lambda c: (hid_buf[c * BLK : (c + 1) * BLK, :], slope_buf[c * BLK : (c + 1) * BLK, :]),
            w_ref, gr_ref, go_ref, gd_acc, gu_acc, go_acc, tail_acc,
        )
        return carry

    lax.fori_loop(0, UNITS, feed, 0)
    attend_back(
        core, q_ref, k_ref, kt_ref, v_ref, go_ref, o_ref, log_ref, dq_ref, dk_ref, dv_ref, mask_ref, prob_ref, ds_ref, dk_acc, dv_acc
    )


def second_stage(a, z, cot, w, wt, wot, wut, wdt, small):
    tile, eight = (UNITS, BLK, BLK), (ALL, BLK, BLK)
    outs = [shape_of(tile), shape_of((UNITS, 8, BLK), F32), shape_of(tile, F32), shape_of((FF, D), F32)]
    outs += [shape_of((D, FF), F32), shape_of((D, D), F32), shape_of((TAIL, 128), F32), shape_of(tile)]
    outs += [shape_of(eight), shape_of(eight)]
    scratch = [pltpu.VMEM(eight, BF16)] + [pltpu.VMEM(s.shape, s.dtype) for s in KEYS]
    scratch += [pltpu.VMEM((HEADS, VROWS, ALL * BLK), BF16), pltpu.VMEM(tile, BF16)]
    scratch += [pltpu.VMEM((UNITS, 2, 8, BLK), F32), pltpu.VMEM(tile, BF16), ATTEND_SCRATCH[1]]
    scratch += [pltpu.VMEM((FF, BLK), BF16), pltpu.VMEM((FF, BLK), F32)] + BACK_SCRATCH
    return stage_call(
        second_stage_body, "second_stage", [a, z, cot, w, wt, wot, wut, wdt, small], outs, scratch, SECOND_MIB, 20e9
    )


def project_back(z, a, dq, dk, dv, gr, small_ref, w_ref, gqkv_acc, head_acc):
    grad = dot(matrix(w_ref, 0, 0), dq) + dot(matrix(w_ref, 0, 1), dk) + dot(matrix(w_ref, 0, 2), dv)
    gqkv_acc[0] += dot_nt(a, dq)
    gqkv_acc[1] += dot_nt(a, dk)
    gqkv_acc[2] += dot_nt(a, dv)
    unit_values, inverse = standardize(z)
    head_acc[0:D, :] += fold(grad * unit_values)
    head_acc[D : 2 * D, :] += fold(grad)
    return gr + standardize_back(grad * param(small_ref, 0), unit_values, inverse)


def third_stage_body(
    dq_in, dk_in, dv_in, a2_ref, z_ref, gr_in, hid_ref, slope_ref, r_ref, o_ref, log_ref, q_ref, kt_ref, k_ref, v_ref,
    small_ref, w_ref, gd_in, gu_in, go_in, tail_in,
    gz_ref, gr_ref, gd_acc, gu_acc, go_acc, tail_acc, gqkv_acc, head_acc, dq_ref, dk_ref, dv_ref,
    go_ref, mask_ref, prob_ref, ds_ref, dk_acc, dv_acc,
):
    core = lax.axis_index("seq") % 2
    set_mask(mask_ref)
    gqkv_acc[...] = jnp.zeros_like(gqkv_acc)
    head_acc[...] = jnp.zeros_like(head_acc)
    for acc, given in ((gd_acc, gd_in), (gu_acc, gu_in), (go_acc, go_in), (tail_acc, tail_in)):
        acc[...] = given[...]

    def feed(u, carry):
        place, base = unit_place(u, core)
        g = project_back(
            z_ref[u], a2_ref[base + place], dq_in[u], dk_in[u], dv_in[u], gr_in[u], small_ref, w_ref, gqkv_acc, head_acc
        )
        gz_ref[u] = g
        r_unit, r_inv = standardize(r_ref[u])
        m = (r_unit * param(small_ref, 2) + param(small_ref, 3)).astype(BF16)
        feed_back_tail(
            u, g, g.astype(BF16), r_unit, r_inv, m, o_ref[u], small_ref,
            lambda c: (hid_ref[u, c * BLK : (c + 1) * BLK, :], slope_ref[u, c * BLK : (c + 1) * BLK, :].astype(F32)),
            w_ref, gr_ref, go_ref, gd_acc, gu_acc, go_acc, tail_acc,
        )
        return carry

    lax.fori_loop(0, UNITS, feed, 0)
    attend_back(
        core, q_ref, k_ref, kt_ref, v_ref, go_ref, o_ref, log_ref, dq_ref, dk_ref, dv_ref, mask_ref, prob_ref, ds_ref, dk_acc, dv_acc
    )


def third_stage(*args):
    tile, eight = (UNITS, BLK, BLK), (ALL, BLK, BLK)
    outs = [shape_of(tile, F32), shape_of(tile, F32), shape_of((FF, D), F32), shape_of((D, FF), F32)]
    outs += [shape_of((D, D), F32), shape_of((TAIL, 128), F32), shape_of((3, D, D), F32), shape_of((2 * D, 128), F32)]
    outs += [shape_of(tile), shape_of(eight), shape_of(eight)]
    scratch = [pltpu.VMEM(tile, BF16)] + BACK_SCRATCH
    return stage_call(third_stage_body, "third_stage", args, outs, scratch, THIRD_MIB, 16e9)


def last_stage_body(
    n, dq_ref, dk_ref, dv_ref, a_ref, xt_ref, gr_ref, gz_ref, small_ref, w_ref, gqkv_in, head_in,
    gout_ref, gu_ref, gd_ref, tail_ref, sq1_ref, sq2_ref,
    grad_ref, g_ref, p_ref, gqkv_acc, head_acc,
):
    dp = lax.axis_index("dp")
    seq = lax.axis_index("seq")
    chip, core = seq // 2, seq % 2
    gqkv_acc[...] = gqkv_in[...]
    head_acc[...] = head_in[...]

    def end(u, carry):
        place, base = unit_place(u, core)
        g = project_back(
            xt_ref[base + place].astype(F32), a_ref[base + place], dq_ref[u], dk_ref[u], dv_ref[u], gr_ref[u],
            small_ref, w_ref, gqkv_acc, head_acc,
        )
        grad_ref[u] = (g + gz_ref[u]).T.astype(BF16)
        return carry

    lax.fori_loop(0, UNITS, end, 0)
    split = lambda values: values.astype(BF16).reshape(g_ref.shape[2:])
    for t in range(3):
        g_ref[0, t] = split(gqkv_acc[t])
    g_ref[0, 3] = split(gout_ref[...])
    for c in range(4):
        g_ref[1, c] = split(gu_ref[:, c * D : (c + 1) * D])
        g_ref[2, c] = split(gd_ref[c * D : (c + 1) * D, :])
    for row in range(SMALL):
        for side in range(2):
            ref, first = (head_acc, row) if row < 2 else (tail_ref, row - 2)
            first = first * D + side * 128
            p_ref[2 * row + side : 2 * row + side + 1, :] = jnp.sum(ref[first : first + 128, :].T, axis=0, keepdims=True)
    sequences = 6 * n
    place = lax.broadcasted_iota(jnp.int32, (6, 128), 0) * 128 + lax.broadcasted_iota(jnp.int32, (6, 128), 1)
    stats = jnp.zeros((6, 128), F32)
    for i, ref in enumerate((sq1_ref, sq2_ref)):
        lines = [jnp.sum(ref[u], axis=0, keepdims=True) for u in range(UNITS)]
        own = jnp.sum(lines[0] + lines[1] + lines[2] + lines[3], axis=1, keepdims=True)
        half = jnp.sum(lines[4] + lines[5], axis=1, keepdims=True)
        start = i * sequences + 6 * dp + 3 * chip
        stats = jnp.where(place == start + core, jnp.broadcast_to(own, (6, 128)), stats)
        stats = jnp.where(place == start + 2, jnp.broadcast_to(half, (6, 128)), stats)
    p_ref[18:24, :] = stats


def last_stage(n, *args):
    rows = D // n
    outs = [shape_of((UNITS, BLK, BLK)), shape_of((3, 4, n, rows, D)), shape_of((24, 128), F32)]
    scratch = [pltpu.VMEM((3, D, D), F32), pltpu.VMEM((2 * D, 128), F32)]
    return stage_call(partial(last_stage_body, n), "last_stage", args, outs, scratch, LAST_MIB, 3e9)


FIRST_MIB, SECOND_MIB, THIRD_MIB, LAST_MIB = 18, 24, 14, 8


def owner_scalars(owner_ref):
    sizes = [D * D] * 4 + [D * FF, FF * D, SMALL * D]
    starts = []
    for t in range(7):
        offset = jnp.int32(0)
        for u in range(t):
            offset = offset + jnp.where(owner_ref[u] == owner_ref[t], sizes[u], 0).astype(jnp.int32)
        starts.append(offset)
    return starts


def pack_body(owner_ref, row_ref, w_ref, p_ref):
    dp = lax.axis_index("dp")
    seq = lax.axis_index("seq")
    starts = owner_scalars(owner_ref)
    square = jnp.where(seq == 0, starts[0], jnp.where(seq == 1, starts[1], jnp.where(seq == 2, starts[2], starts[3])))
    plans = (
        (owner_ref[seq], square // 128, 2),
        (owner_ref[4], starts[4] // 128 + 2 * seq, FF // 128),
        (owner_ref[5], starts[5] // 128 + 2 * D * seq, 2),
    )
    for kind, (owner, base, stride) in enumerate(plans):
        keep = jnp.where(owner == dp, 1.0, 0.0).astype(F32)
        for side in range(2):
            values = row_ref[pl.ds(base + side, D, stride=stride), :]
            w_ref[kind, :, side * 128 : (side + 1) * 128] = (values * keep).astype(BF16)
    keep = jnp.where(owner_ref[6] == dp, 1.0, 0.0).astype(F32)
    values = row_ref[pl.ds(pl.multiple_of(starts[6] // 128, 8), 24), :] * keep
    rows = lax.broadcasted_iota(jnp.int32, (24, 128), 0)
    p_ref[...] = jnp.where(rows < 2 * SMALL, values, 0.0)


def pack(owner_list, row):
    return pl.pallas_call(
        pack_body,
        in_specs=[pl.BlockSpec(memory_space=pltpu.SMEM), pl.BlockSpec(memory_space=pltpu.VMEM)],
        out_specs=[pl.BlockSpec(memory_space=pltpu.VMEM)] * 2,
        out_shape=[jax.ShapeDtypeStruct((3, D, D), BF16), jax.ShapeDtypeStruct((24, 128), F32)],
        compiler_params=pltpu.CompilerParams(vmem_limit_bytes=20 << 20),
        cost_estimate=cost(1, 3 << 20),
        name="pack",
    )(owner_list, row)


def peers_of(seq):
    return {1: seq + 1 - 2 * (seq % 2), 2: (seq + 2) % 4, 3: 3 - seq}


def greet(n, dp, peers, wide_group):
    barrier = pltpu.get_barrier_semaphore()
    count = 0
    for peer in peers:
        pl.semaphore_signal(barrier, inc=1, device_id={"seq": peer}, device_id_type=MESH)
        count += 1
    if wide_group:
        for k in range(1, n):
            pl.semaphore_signal(barrier, inc=1, device_id={"dp": (dp + k) % n}, device_id_type=MESH)
            count += 1
    pl.semaphore_wait(barrier, count)


def send(source, target, sems, index, device):
    return pltpu.make_async_remote_copy(
        src_ref=source,
        dst_ref=target,
        send_sem=sems[0].at[index],
        recv_sem=sems[1].at[index],
        device_id=device,
        device_id_type=MESH,
    )


def spread(n, dp, seq, peers, kind, w_ref, chunk_ref, row_sems):
    copies = []
    for k in range(1, n):
        copies.append(
            send(chunk_ref.at[kind], w_ref.at[kind, seq, dp], row_sems, (kind, k), {"dp": (dp + k) % n})
        )
        copies[-1].start()
    return copies


def share(seq, peers, kind, w_ref, side_sems):
    copies = [
        send(w_ref.at[kind, seq], w_ref.at[kind, seq], side_sems, (kind, 0), {"seq": peers[2]}),
        send(w_ref.at[kind, seq], w_ref.at[kind, seq], side_sems, (kind, 1), {"seq": peers[1]}),
    ]
    for copy in copies:
        copy.start()
    return copies


def forward(seq, peers, kind, w_ref, side_sems):
    copy = send(w_ref.at[kind, peers[2]], w_ref.at[kind, peers[2]], side_sems, (kind, 2), {"seq": peers[1]})
    copy.start()
    return copy


def swap_inputs_body(a_ref, out_ref, s0, s1):
    seq = lax.axis_index("seq")
    core = seq % 2
    peers = peers_of(seq)
    greet(1, 0, [peers[1]], False)
    copies = [
        send(a_ref.at[4], out_ref.at[4 + core], (s0, s1), 0, {"seq": peers[1]}),
        send(a_ref.at[5], out_ref.at[7 - core], (s0, s1), 1, {"seq": peers[1]}),
    ]
    for copy in copies:
        copy.start()
    for j in range(OWN):
        out_ref[j] = a_ref[j]
    out_ref[4 + core] = a_ref[4]
    out_ref[7 - core] = a_ref[5]
    for copy in copies:
        copy.wait()


def swap_inputs(a):
    vmem = pl.BlockSpec(memory_space=pltpu.VMEM)
    return pl.pallas_call(
        swap_inputs_body,
        in_specs=[vmem],
        out_specs=vmem,
        out_shape=jax.ShapeDtypeStruct((ALL, BLK, BLK), BF16),
        scratch_shapes=pair_of_sems((2,)),
        compiler_params=pltpu.CompilerParams(collective_id=1, has_side_effects=True, vmem_limit_bytes=16 << 20),
        cost_estimate=cost(1, 2 << 20),
        name="swap_inputs",
    )(a)


def swap_grads_body(dk_ref, dv_ref, dk_out, dv_out, slot_ref, s0, s1):
    seq = lax.axis_index("seq")
    core = seq % 2
    peers = peers_of(seq)
    greet(1, 0, [peers[1]], False)
    copies = []
    for which, ref in enumerate((dk_ref, dv_ref)):
        for place, position in enumerate((5 - core, 6 + core)):
            copies.append(
                send(ref.at[position], slot_ref.at[which, place], (s0, s1), (which, place), {"seq": peers[1]})
            )
            copies[-1].start()
    for ref, out in ((dk_ref, dk_out), (dv_ref, dv_out)):
        for j in range(OWN):
            out[j] = ref[j]
    for copy in copies:
        copy.wait()
    for which, (ref, out) in enumerate(((dk_ref, dk_out), (dv_ref, dv_out))):
        for place, position in enumerate((4 + core, 7 - core)):
            out[4 + place] = (ref[position].astype(F32) + slot_ref[which, place].astype(F32)).astype(BF16)


def swap_grads(dk, dv):
    vmem = pl.BlockSpec(memory_space=pltpu.VMEM)
    out = jax.ShapeDtypeStruct((UNITS, BLK, BLK), BF16)
    return pl.pallas_call(
        swap_grads_body,
        in_specs=[vmem] * 2,
        out_specs=[vmem] * 2,
        out_shape=[out, out],
        scratch_shapes=[pltpu.VMEM((2, 2, BLK, BLK), BF16), *pair_of_sems((2, 2))],
        compiler_params=pltpu.CompilerParams(collective_id=2, has_side_effects=True, vmem_limit_bytes=16 << 20),
        cost_estimate=cost(1, 4 << 20),
        name="swap_grads",
    )(dk, dv)


def leave_body(
    n, g_ref, pp_ref, f_ref, i_ref, w_ref, p_ref, fo_ref, io_ref,
    half_ref, quarter_ref, out_ref, mine_ref, slot_ref, chunk_ref, pslot_ref, psum_ref,
    as0, as1, bs0, bs1, ss0, ss1, rs0, rs1, gs0, gs1, ps0, ps1, xs0, xs1,
):
    dp = lax.axis_index("dp")
    seq = lax.axis_index("seq")
    chip, core = seq // 2, seq % 2
    peers = peers_of(seq)
    greet(n, dp, [peers[1], peers[2], peers[3]], True)
    finish = []

    first = []
    for kind in range(3):
        copies = []
        for j, quarter in enumerate((peers[1], peers[3])):
            copies.append(
                send(g_ref.at[kind, quarter], half_ref.at[kind, j], (as0, as1), (kind, j), {"seq": peers[1]})
            )
            copies[-1].start()
        first.append(copies)
        finish += copies
    small = [send(pp_ref, pslot_ref.at[0], (ps0, ps1), 0, {"seq": peers[1]})]
    small[0].start()

    moves = []
    own = 3 * chip + core

    def move(which, source_ref, target_ref):
        for o in (2, 3, 1):
            copy = send(source_ref.at[peers[o]], target_ref.at[own], (xs0, xs1), (which, o), {"seq": peers[o]})
            copy.start()
            moves.append(copy)

        @pl.when(chip == 0)
        def _():
            send(source_ref.at[5], target_ref.at[2], (xs0, xs1), (which, 4 + 3), {"seq": peers[3]}).start()

        @pl.when(chip == 1)
        def _():
            send(source_ref.at[4], target_ref.at[5], (xs0, xs1), (which, 4 + 2), {"seq": peers[2]}).start()
            send(source_ref.at[5], target_ref.at[5], (xs0, xs1), (which, 4 + 1), {"seq": peers[1]}).start()

        target_ref[own] = source_ref[seq]

        @pl.when(chip == 0)
        def _():
            target_ref[2] = source_ref[4]

    def settle(which, source_ref, target_ref):
        @pl.when(chip == 0)
        def _():
            send(source_ref.at[5], target_ref.at[2], (xs0, xs1), (which, 4 + 3), {"seq": peers[3]}).wait_send()
            send(source_ref.at[4], target_ref.at[5], (xs0, xs1), (which, 4 + 2), {"seq": peers[2]}).wait_recv()

        @pl.when(chip == 1)
        def _():
            send(source_ref.at[4], target_ref.at[5], (xs0, xs1), (which, 4 + 2), {"seq": peers[2]}).wait_send()
            send(source_ref.at[5], target_ref.at[5], (xs0, xs1), (which, 4 + 1), {"seq": peers[1]}).wait_send()
            send(source_ref.at[5], target_ref.at[2], (xs0, xs1), (which, 4 + 3), {"seq": peers[3]}).wait_recv()
            send(source_ref.at[5], target_ref.at[5], (xs0, xs1), (which, 4 + 1), {"seq": peers[1]}).wait_recv()

    second = []
    for kind in range(3):
        for copy in first[kind]:
            copy.wait_recv()
        out_ref[kind] = (g_ref[kind, peers[2]].astype(F32) + half_ref[kind, 1].astype(F32)).astype(BF16)
        second.append(send(out_ref.at[kind], quarter_ref.at[kind], (bs0, bs1), kind, {"seq": peers[2]}))
        second[-1].start()
    finish += second
    small[0].wait_recv()
    psum_ref[0] = pp_ref[...] + pslot_ref[0]
    small.append(send(psum_ref.at[0], pslot_ref.at[1], (ps0, ps1), 1, {"seq": peers[2]}))
    small[1].start()
    move(0, f_ref, fo_ref)
    move(1, i_ref, io_ref)

    scatter = []
    for kind in range(3):
        second[kind].wait_recv()
        mine_ref[kind] = (
            g_ref[kind, seq].astype(F32) + half_ref[kind, 0].astype(F32) + quarter_ref[kind].astype(F32)
        ).astype(BF16)
        copies = []
        for k in range(1, n):
            to = (dp + k) % n
            copies.append(send(mine_ref.at[kind, to], slot_ref.at[kind, k], (ss0, ss1), (kind, k), {"dp": to}))
            copies[-1].start()
        scatter.append(copies)
        finish += copies
    small[1].wait_recv()
    psum_ref[1] = psum_ref[0] + pslot_ref[1]
    for k in range(1, n):
        copy = send(psum_ref.at[1], pslot_ref.at[1 + k], (ps0, ps1), 1 + k, {"dp": (dp + k) % n})
        copy.start()
        small.append(copy)
    gathers = []
    for kind in range(3):
        total = mine_ref[kind, dp].astype(F32)
        for k in range(1, n):
            scatter[kind][k - 1].wait_recv()
            total = total + slot_ref[kind, k].astype(F32)
        chunk_ref[kind] = total.astype(BF16)
        w_ref[kind, seq, dp] = total.astype(BF16)
        gathers.append(spread(n, dp, seq, peers, kind, w_ref, chunk_ref, (rs0, rs1)))
    sides = []
    for kind in range(3):
        for copy in gathers[kind]:
            copy.wait_recv()
        sides.append(share(seq, peers, kind, w_ref, (gs0, gs1)))
        finish += gathers[kind]
    total = psum_ref[1]
    for k in range(1, n):
        small[1 + k].wait_recv()
        total = total + pslot_ref[1 + k]
    p_ref[...] = total
    for kind in range(3):
        sides[kind][0].wait_recv()
        sides[kind].append(forward(seq, peers, kind, w_ref, (gs0, gs1)))
    for kind in range(3):
        sides[kind][1].wait_recv()
        sides[kind][2].wait_recv()
        finish += sides[kind]
    settle(0, f_ref, fo_ref)
    settle(1, i_ref, io_ref)
    for copy in moves:
        copy.wait()
    for copy in finish + small:
        copy.wait_send()


def leave(n, g, pp, f, i):
    rows = D // n
    vmem = pl.BlockSpec(memory_space=pltpu.VMEM)
    return pl.pallas_call(
        partial(leave_body, n),
        in_specs=[vmem] * 4,
        out_specs=[vmem] * 4,
        out_shape=[
            jax.ShapeDtypeStruct((3, 4, n, rows, D), BF16),
            jax.ShapeDtypeStruct((24, 128), F32),
            jax.ShapeDtypeStruct((UNITS, BLK, BLK), BF16),
            jax.ShapeDtypeStruct((UNITS, BLK, BLK), BF16),
        ],
        scratch_shapes=[
            pltpu.VMEM((3, 2, n, rows, D), BF16),
            pltpu.VMEM((3, n, rows, D), BF16),
            pltpu.VMEM((3, n, rows, D), BF16),
            pltpu.VMEM((3, n, rows, D), BF16),
            pltpu.VMEM((3, n, rows, D), BF16),
            pltpu.VMEM((3, rows, D), BF16),
            pltpu.VMEM((1 + n, 24, 128), F32),
            pltpu.VMEM((2, 24, 128), F32),
            *pair_of_sems((3, 2)),
            *pair_of_sems((3,)),
            *pair_of_sems((3, n)),
            *pair_of_sems((3, n)),
            *pair_of_sems((3, 3)),
            *pair_of_sems((1 + n,)),
            *pair_of_sems((2, 8)),
        ],
        compiler_params=pltpu.CompilerParams(collective_id=3, has_side_effects=True, vmem_limit_bytes=48 << 20),
        cost_estimate=cost(1, 20 << 20),
        name="leave",
    )(g, pp, f, i)


ROWS = D * D // 128


def adam_body(owner_ref, g_ref, p_ref, m_ref, v_ref, w_ref, m_out, v_out, w_out, grad_ref):
    dp = lax.axis_index("dp")
    block = pl.program_id(0)
    starts = owner_scalars(owner_ref)
    counts = [1, 1, 1, 1, 4, 4, 1]
    rate = jnp.float32(D ** (-0.5))
    decay = jnp.float32(0.1)
    limit = jnp.int32(0)
    for t in range(7):
        first = starts[t] // (D * D)
        here = (owner_ref[t] == dp) & (block >= first) & (block < first + counts[t])
        part = block - first
        limit = jnp.where(here, 2 * SMALL if t == 6 else ROWS, limit)
        if t == 5:
            rate = jnp.where(here, FF ** (-0.5), rate)
        if t == 6:
            rate = jnp.where(here, 0.5, rate)
            decay = jnp.where(here, 0.0, decay)

        @pl.when(here)
        def _(t=t, part=part):
            if t == 6:
                grad_ref[0:24, :] = p_ref[...]
            elif t == 4:
                for c in range(4):
                    piece = g_ref[4 + c, pl.ds(pl.multiple_of(part * 64, 64), 64), :].astype(F32)
                    for side in range(2):
                        grad_ref[pl.ds(2 * c + side, 64, stride=8), :] = piece[:, side * 128 : (side + 1) * 128]
            else:
                piece = g_ref[8 + part if t == 5 else t].astype(F32)
                for side in range(2):
                    grad_ref[pl.ds(side, D, stride=2), :] = piece[:, side * 128 : (side + 1) * 128]

    @pl.when(limit == 0)
    def _():
        for out in (m_out, v_out, w_out):
            out[...] = jnp.zeros_like(out)

    @pl.when(limit > 0)
    def _():
        correction = 1.0 - 0.5**STEP
        grad = grad_ref[...]
        valid = lax.broadcasted_iota(jnp.int32, (ROWS, 128), 0) < limit
        first_new = 0.5 * m_ref[...] + 0.5 * grad
        second_new = 0.5 * v_ref[...] + 0.5 * grad * grad
        old = w_ref[...]
        update = first_new / correction / (jnp.sqrt(second_new / correction) + adam_eps) + decay * old
        m_out[...] = jnp.where(valid, first_new, 0.0)
        v_out[...] = jnp.where(valid, second_new, 0.0)
        w_out[...] = jnp.where(valid, old - rate * update, 0.0)


def adam(owner_list, g, p, m, v, w):
    tile = pl.BlockSpec((ROWS, 128), lambda b, t: (b, 0))
    out = jax.ShapeDtypeStruct(m.shape, F32)
    spec = pltpu.PrefetchScalarGridSpec(
        num_scalar_prefetch=1,
        grid=(m.shape[0] // ROWS,),
        in_specs=[full(g.shape), full(p.shape), tile, tile, tile],
        out_specs=[tile, tile, tile],
        scratch_shapes=[pltpu.VMEM((ROWS, 128), F32)],
    )
    return pl.pallas_call(
        adam_body,
        grid_spec=spec,
        out_shape=[out, out, out],
        compiler_params=params_of(),
        cost_estimate=cost(20 * 524288, 14 << 20),
        name="adam",
    )(owner_list, g, p, m, v, w)


def per_device(inputs, cotangent, owner_list, master_rows, moment1_rows, moment2_rows):
    n = lax.axis_size("dp")
    rows = D // n
    flat = [r.reshape(-1, 128) for r in (master_rows, moment1_rows, moment2_rows)]
    pk, pp = pack(owner_list, flat[0])
    (xt, a1, q1, kt1, k1, v1, o1, log1, r1, hid, slope, z2, a2, sq1, wt, wot, wut, wdt, small, w, cot) = first_stage(
        n, pk.reshape(3, n, rows, D), pp, inputs, cotangent
    )
    a2 = swap_inputs(a2)
    final, sq2, gr, gd, gu, gout, tail, dq, dk, dv = second_stage(a2, z2, cot, w, wt, wot, wut, wdt, small)
    dk, dv = swap_grads(dk, dv)
    gz, gr, gd, gu, gout, tail, gqkv, head, dq, dk, dv = third_stage(
        dq, dk, dv, a2, z2, gr, hid, slope, r1, o1, log1, q1, kt1, k1, v1, small, w, gd, gu, gout, tail
    )
    dk, dv = swap_grads(dk, dv)
    grad, g, pp = last_stage(n, dq, dk, dv, a1, xt, gr, gz, small, w, gqkv, head, gout, gu, gd, tail, sq1, sq2)
    g, p, final, grad = leave(n, g, pp, final, grad)
    m_new, v_new, w_new = adam(owner_list, g.reshape(12, D, D), p, flat[1], flat[2], flat[0])
    sequences = inputs.shape[0] * n
    entries = inputs.shape[1] * lax.axis_size("seq") * D
    squares = p[18:].reshape(-1)[: 2 * sequences].reshape(2, sequences)
    stats = jnp.sqrt(squares / entries + stat_eps)
    back = lambda r: r.reshape(master_rows.shape)
    return (final.astype(F32), grad.astype(F32), stats, back(m_new), back(v_new), back(w_new))


def solution(mesh):
    placed = (P("dp", "seq", None), P("dp", "seq", None), P(), P("dp", None), P("dp", None), P("dp", None))
    return jax.shard_map(
        per_device,
        mesh=mesh,
        in_specs=placed,
        out_specs=(P("dp", "seq", None), P("dp", "seq", None), P(), P("dp", None), P("dp", None), P("dp", None)),
        check_vma=False,
    )
```

```python
import math
from functools import partial

import jax
import jax.numpy as jnp
from jax import lax
from jax.experimental import pallas as pl
from jax.experimental.pallas import tpu as pltpu
from jax.sharding import PartitionSpec as P

D = 256
HEADS = 4
HD = 64
FF = 1024
STEP = 3
SMALL = 9
BLK = 256
OWN = 4
UNITS = 6
ALL = 8
F32 = jnp.float32
BF16 = jnp.bfloat16
MESH = pl.DeviceIdType.MESH

norm_eps = 1e-05
stat_eps = 1e-06
adam_eps = 1e-08
masked_score = -1e30


def dot(left, right):
    return lax.dot_general(left, right, (((1,), (0,)), ((), ())), preferred_element_type=F32)


def dot_nt(left, right):
    return lax.dot_general(left, right, (((1,), (1,)), ((), ())), preferred_element_type=F32)


def wide(column):
    return jnp.concatenate([column, column], axis=1)


def fold(values):
    return values[:, :128] + values[:, 128:]


def standardize(values):
    average = jnp.mean(values, axis=0, keepdims=True)
    centered = values - average
    spread = jnp.mean(centered * centered, axis=0, keepdims=True)
    inverse = lax.rsqrt(spread + norm_eps)
    return centered * inverse, inverse


def standardize_back(grad, unit_values, inverse):
    average = jnp.mean(grad, axis=0, keepdims=True)
    inner = jnp.mean(grad * unit_values, axis=0, keepdims=True)
    return (grad - average - unit_values * inner) * inverse


def param(small_ref, row):
    return wide(small_ref[row * D : (row + 1) * D, :])


def gelu_parts(e):
    cdf = 0.5 * lax.erf(e * math.sqrt(0.5)) + 0.5
    hid = e * cdf
    slope = cdf + e * (jnp.exp(-0.5 * e * e) * (1.0 / math.sqrt(2.0 * math.pi)))
    return hid, slope


def full(shape):
    return pl.BlockSpec(shape, lambda *args: (0,) * len(shape), pipeline_mode=pl.Buffered(1))


def params_of(ndims=1, mib=56):
    return pltpu.CompilerParams(
        dimension_semantics=("arbitrary",) * ndims, vmem_limit_bytes=mib << 20
    )


def cost(flops, nbytes, trans=0):
    return pl.CostEstimate(flops=int(flops), bytes_accessed=int(nbytes), transcendentals=int(trans))


LOG2E = math.log2(math.e)
VROWS = HD + 16


def unit_place(unit, core):
    later = unit // OWN
    place = (1 - later) * unit + later * (core + (unit - OWN) * (3 - 2 * core))
    return place, later * OWN


def lanes(start, size):
    return pl.ds(pl.multiple_of(start, BLK), size)


def pair_rows(pair):
    return pl.ds(pl.multiple_of(pair * 128, 128), 128)


def matrix(w_ref, kind, part):
    n, rows = w_ref.shape[2:4]
    if rows % 16 == 0:
        return w_ref[kind, part].reshape(D, D)
    return jnp.concatenate([w_ref[kind, part, i] for i in range(n)], axis=0)


def peers_of(seq):
    return {1: seq + 1 - 2 * (seq % 2), 2: (seq + 2) % 4, 3: 3 - seq}


def greet(n, dp, peers, wide_group):
    barrier = pltpu.get_barrier_semaphore()
    count = 0
    for peer in peers:
        pl.semaphore_signal(barrier, inc=1, device_id={"seq": peer}, device_id_type=MESH)
        count += 1
    if wide_group:
        for k in range(1, n):
            pl.semaphore_signal(barrier, inc=1, device_id={"dp": (dp + k) % n}, device_id_type=MESH)
            count += 1
    pl.semaphore_wait(barrier, count)


def send(source, target, sems, index, device):
    return pltpu.make_async_remote_copy(
        src_ref=source,
        dst_ref=target,
        send_sem=sems[0].at[index],
        recv_sem=sems[1].at[index],
        device_id=device,
        device_id_type=MESH,
    )


def pair_of_sems(shape):
    return [pltpu.SemaphoreType.DMA(shape), pltpu.SemaphoreType.DMA(shape)]


def project(j, a, wt_ref, q_ref, kt_ref, vt_ref, k_ref, v_ref):
    where = lanes(j * BLK, BLK)
    q_ref[j] = (dot(wt_ref[0:D], a) * HD ** (-0.5)).astype(BF16)
    kt = dot(wt_ref[D : 2 * D], a).astype(BF16)
    vt = dot(wt_ref[2 * D : 3 * D], a).astype(BF16)
    for h in range(HEADS):
        kt_ref[h, :, where] = kt[h * HD : (h + 1) * HD]
        vt_ref[h, 0:HD, where] = vt[h * HD : (h + 1) * HD]
    k = kt.T
    v = vt.T
    for h in range(2):
        k_ref[h, j] = k[:, h * 128 : (h + 1) * 128]
        v_ref[h, j] = v[:, h * 128 : (h + 1) * 128]


def head_rows(values, half):
    rows = lax.broadcasted_iota(jnp.int32, values.shape, 0)
    keep = (rows < HD) if half == 0 else (rows >= HD)
    return jnp.where(keep, values, jnp.zeros_like(values))


def set_mask(mask_ref):
    keys = lax.broadcasted_iota(jnp.int32, (BLK, BLK), 0)
    queries = lax.broadcasted_iota(jnp.int32, (BLK, BLK), 1)
    mask_ref[...] = jnp.where(keys <= queries, 0.0, masked_score)


def groups(values, op):
    out = values[0:8]
    for i in range(1, values.shape[0] // 8):
        out = op(out, values[i * 8 : (i + 1) * 8])
    return out


SUB = 128


def ordered(i):
    return (i + OWN) % UNITS


def attend(core, q_ref, k_ref, vt_ref, o_ref, log_ref, mask_ref, score_ref, prob_ref, progress=None):
    def step(i, carry):
        if progress is not None:
            progress(i)
        pair, unit = i % 2, ordered(i // 2)
        place, base = unit_place(unit, core)

        def branch(last):
            block = q_ref[base + place, pair_rows(pair), :]
            for half in range(2):
                q = head_rows(block, half)
                top = None
                for kb in range(last + 1):
                    for sub in range(BLK // SUB):
                        rows = slice(sub * SUB, (sub + 1) * SUB)
                        score = dot(k_ref[pair, base + kb, rows, :], q)
                        if kb == last:
                            score = score + mask_ref[rows, :]
                        score_ref[half, kb, rows, :] = score
                        peak = groups(score, jnp.maximum)
                        top = peak if top is None else jnp.maximum(top, peak)
                top = jnp.max(top, axis=0, keepdims=True)
                for kb in range(last + 1):
                    for sub in range(BLK // SUB):
                        rows = slice(sub * SUB, (sub + 1) * SUB)
                        weight = jnp.exp(score_ref[half, kb, rows, :] - top)
                        prob_ref[half, kb * BLK + sub * SUB : kb * BLK + (sub + 1) * SUB, :] = weight.astype(BF16)
                keys = (last + 1) * BLK
                out = dot(vt_ref[2 * pair + half, :, lanes(base * BLK, keys)], prob_ref[half, 0:keys, :])
                total = out[HD : HD + 1]
                o_ref[unit, pl.ds(pl.multiple_of(pair * 128 + half * HD, HD), HD), :] = (out[0:HD] / total).astype(BF16)
                log_ref[unit, pair, half : half + 1, :] = top + jnp.log(total)

        for last in range(OWN):
            pl.when(place == last)(partial(branch, last))
        return carry

    lax.fori_loop(0, 2 * UNITS, step, 0)


def attend_back(
    core, q_ref, k_ref, kt_ref, v_ref, go_ref, o_ref, log_ref, dq_ref, dk_ref, dv_ref, mask_ref, prob_ref, slope_ref, dk_acc, dv_acc,
    part_ref, got_ref, ds0, ds1, peer, progress=None,
):
    dk_acc[...] = jnp.zeros_like(dk_acc)
    dv_acc[...] = jnp.zeros_like(dv_acc)

    pairs = ((0, dk_acc, dk_ref), (1, dv_acc, dv_ref))

    def piece(acc, j):
        return acc[:, :, j * BLK : (j + 1) * BLK].reshape(D, BLK)

    def swap(which, side):
        position = 1 - core if side == 0 else 2 + core
        return send(part_ref.at[which, position], got_ref.at[which, side], (ds0, ds1), (which, side), {"seq": peer})

    def step(i, carry):
        @pl.when(i == 4)
        def _():
            for which, acc, _ in pairs:
                for position in range(OWN):
                    part_ref[which, position] = piece(acc, OWN + position).astype(BF16)
            for which in range(2):
                for side in range(2):
                    swap(which, side).start()

        if progress is not None:
            progress(i)
        pair, unit = i % 2, ordered(i // 2)
        place, base = unit_place(unit, core)

        def branch(last):
            block = q_ref[base + place, pair_rows(pair), :]
            go_block = go_ref[unit, pair_rows(pair), :]
            o_block = o_ref[unit, pair_rows(pair), :]
            keys = (last + 1) * BLK
            for half in range(2):
                lo, hi = half * HD, (half + 1) * HD
                q = head_rows(block, half)
                go = head_rows(go_block, half)
                q_head = block[lo:hi]
                go_head = go_block[lo:hi]
                log_total = log_ref[unit, pair, half : half + 1, :]
                inner = jnp.sum(go_head.astype(F32) * o_block[lo:hi].astype(F32), axis=0, keepdims=True)
                for kb in range(last + 1):
                    for sub in range(BLK // SUB):
                        rows = slice(sub * SUB, (sub + 1) * SUB)
                        to = slice(kb * BLK + sub * SUB, kb * BLK + (sub + 1) * SUB)
                        score = dot(k_ref[pair, base + kb, rows, :], q)
                        if kb == last:
                            score = score + mask_ref[rows, :]
                        weight = jnp.exp(score - log_total)
                        slope = dot(v_ref[pair, base + kb, rows, :], go)
                        prob_ref[half, to, :] = weight.astype(BF16)
                        slope_ref[half, to, :] = (weight * (slope - inner)).astype(BF16)
                head = 2 * pair + half
                where = lanes(base * BLK, keys)
                dv_acc[head, :, where] += dot_nt(go_head, prob_ref[half, 0:keys, :])
                dk_acc[head, :, where] += dot_nt(q_head, slope_ref[half, 0:keys, :])
                dq = dot(kt_ref[head, :, where], slope_ref[half, 0:keys, :])
                dq_ref[unit, pl.ds(pl.multiple_of(pair * 128 + lo, HD), HD), :] = (dq * HD ** (-0.5)).astype(BF16)

        for last in range(OWN):
            pl.when(place == last)(partial(branch, last))
        return carry

    lax.fori_loop(0, 2 * UNITS, step, 0)
    for which, acc, ref in pairs:
        for j in range(OWN):
            ref[j] = piece(acc, j).astype(BF16)
    for which, acc, ref in pairs:
        for side, position in enumerate((core, 3 - core)):
            swap(which, side).wait()
            ref[OWN + side] = (part_ref[which, position].astype(F32) + got_ref[which, side].astype(F32)).astype(BF16)


def forward_parts(z, o, wot_ref, small_ref):
    r = z + dot(wot_ref[...], o)
    unit_values, inverse = standardize(r)
    m = (unit_values * param(small_ref, 2) + param(small_ref, 3)).astype(BF16)
    return r, unit_values, inverse, m


def squares_of(out):
    return groups(out * out, jnp.add)


def first_stage_body(
    n, pk_ref, pp_ref, x_ref, c_ref,
    xt_ref, a_ref, q_ref, kt_ref, k_ref, v_ref, o_ref, log_ref, r_ref, hid_ref, slope_ref, z_ref, a2_ref, sq_ref,
    wt_ref, wot_ref, wut_ref, wdt_ref, small_ref, w_ref, co_ref,
    vt_ref, mask_ref, score_ref, prob_ref, xo_ref, slot_ref, pslot_ref, chunk_ref,
    ss0, ss1, rs0, rs1, ps0, ps1, gs0, gs1, xs0, xs1, cs0, cs1, ns0, ns1, hid_buf, slope_buf, hs,
):
    dp = lax.axis_index("dp")
    seq = lax.axis_index("seq")
    chip, core = seq // 2, seq % 2
    peers = peers_of(seq)

    def scatter(kind, k):
        to = (dp + k) % n
        return send(pk_ref.at[kind, to], slot_ref.at[kind, k], (ss0, ss1), (kind, k), {"dp": to})

    def small(k):
        return send(pp_ref, pslot_ref.at[k], (ps0, ps1), k, {"dp": (dp + k) % n})

    def gather(kind, k):
        return send(chunk_ref.at[kind], w_ref.at[kind, seq, dp], (rs0, rs1), (kind, k), {"dp": (dp + k) % n})

    def side(kind, which):
        part = peers[2] if which == 2 else seq
        to = peers[2] if which == 0 else peers[1]
        return send(w_ref.at[kind, part], w_ref.at[kind, part], (gs0, gs1), (kind, which), {"seq": to})

    def own(o):
        to = peers[o]
        return send(x_ref.at[3 * (to // 2) + to % 2], xo_ref.at[seq], (xs0, xs1), (o, 0), {"seq": to})

    def shared(o):
        if o == 3:
            there = xo_ref.at[OWN + peers[2]]
            return send(there, there, (xs0, xs1), (3, 1), {"seq": peers[1]})
        to = peers[o]
        return send(x_ref.at[3 * (to // 2) + 2], xo_ref.at[OWN + seq], (xs0, xs1), (o, 1), {"seq": to})

    def target(o):
        to = peers[o]
        return send(c_ref.at[3 * (to // 2) + to % 2], co_ref.at[seq], (cs0, cs1), o, {"seq": to})

    def target_shared(o):
        slot = 4 if o == 2 else 5
        return send(c_ref.at[2 if o == 3 else 5], co_ref.at[slot], (cs0, cs1), 4 + o, {"seq": peers[o]})

    def sum_up(kind):
        total = pk_ref[kind, dp].astype(F32)
        for k in range(1, n):
            scatter(kind, k).wait_recv()
            total = total + slot_ref[kind, k].astype(F32)
        chunk_ref[kind] = total.astype(BF16)
        w_ref[kind, seq, dp] = total.astype(BF16)

    offsets = range(1, n)
    greet(n, dp, [peers[1], peers[2], peers[3]], True)
    for k in offsets:
        scatter(0, k).start()
    for o in (2, 1):
        shared(o).start()
    for o in (2, 3, 1):
        own(o).start()
    for k in offsets:
        small(k).start()
    xo_ref[seq] = x_ref[3 * chip + core]
    xo_ref[OWN + seq] = x_ref[3 * chip + 2]
    co_ref[seq] = c_ref[3 * chip + core]
    pl.when(chip == 0)(lambda: co_ref.__setitem__(4, c_ref[2]))
    set_mask(mask_ref)
    vt_ref[:, HD:, :] = jnp.ones((HEADS, VROWS - HD, ALL * BLK), BF16)
    sum_up(0)
    for k in offsets:
        gather(0, k).start()
    for kind in (1, 2):
        for k in offsets:
            scatter(kind, k).start()
    total = pp_ref[...]
    for k in offsets:
        small(k).wait_recv()
        total = total + pslot_ref[k]
    for row in range(SMALL):
        for part in range(2):
            line = jnp.broadcast_to(total[2 * row + part : 2 * row + part + 1, :], (128, 128))
            small_ref[row * D + part * 128 : row * D + (part + 1) * 128, :] = line.T
    shared(2).wait_recv()
    shared(3).start()
    for o in (2, 3, 1):
        own(o).wait_recv()
    shared(1).wait_recv()
    for k in offsets:
        gather(0, k).wait_recv()
    side(0, 0).start()
    side(0, 1).start()
    for o in (2, 3, 1):
        target(o).start()
    pl.when(chip == 0)(lambda: target_shared(2).start())
    pl.when(chip == 1)(lambda: target_shared(3).start())
    pl.when(chip == 1)(lambda: target_shared(1).start())
    shared(3).wait_recv()

    def begin(j, carry):
        xt = xo_ref[j].T
        xt_ref[j] = xt
        unit_values, _ = standardize(xt.astype(F32))
        a_ref[j] = (unit_values * param(small_ref, 0) + param(small_ref, 1)).astype(BF16)
        return carry

    lax.fori_loop(0, ALL, begin, 0)
    side(0, 0).wait_recv()
    side(0, 2).start()
    side(0, 1).wait_recv()
    side(0, 2).wait_recv()
    for t in range(3):
        wt_ref[t * D : (t + 1) * D, :] = matrix(w_ref, 0, t).T
    for kind in (1, 2):
        sum_up(kind)
        for k in offsets:
            gather(kind, k).start()

    def middle(j, carry):
        project(j, a_ref[j], wt_ref, q_ref, kt_ref, vt_ref, k_ref, v_ref)
        return carry

    lax.fori_loop(0, ALL, middle, 0)

    def progress(i):
        @pl.when(i == 3)
        def _():
            for kind in (1, 2):
                for k in offsets:
                    gather(kind, k).wait_recv()
                side(kind, 0).start()
                side(kind, 1).start()

        @pl.when(i == 10)
        def _():
            for kind in (1, 2):
                side(kind, 0).wait_recv()
                side(kind, 2).start()

    attend(core, q_ref, k_ref, vt_ref, o_ref, log_ref, mask_ref, score_ref, prob_ref, progress)
    wot_ref[...] = matrix(w_ref, 0, 3).T
    for kind in (1, 2):
        side(kind, 1).wait_recv()
        side(kind, 2).wait_recv()
    for c in range(4):
        part = slice(c * D, (c + 1) * D)
        wut_ref[part, :] = matrix(w_ref, 1, c).T
        wdt_ref[:, part] = matrix(w_ref, 2, c).T

    def normal(side):
        there = a2_ref.at[OWN + core if side == 0 else OWN + 3 - core]
        return send(there, there, (ns0, ns1), side, {"seq": peers[1]})

    def store(i):
        slot, u = i % 2, ordered(i)
        return (
            pltpu.make_async_copy(hid_buf.at[slot], hid_ref.at[u], hs.at[0, slot]),
            pltpu.make_async_copy(slope_buf.at[slot], slope_ref.at[u], hs.at[1, slot]),
        )

    def feed(i, carry):
        @pl.when(i == 2)
        def _():
            normal(0).start()
            normal(1).start()

        slot = i % 2

        @pl.when(i >= 2)
        def _():
            for copy in store(i - 2):
                copy.wait()

        u = ordered(i)
        place, base = unit_place(u, core)
        x = xt_ref[base + place].astype(F32)
        r, _, _, m = forward_parts(x, o_ref[u], wot_ref, small_ref)
        r_ref[u] = r
        out = r + param(small_ref, 4)
        for c in range(FF // BLK):
            rows = slice(c * BLK, (c + 1) * BLK)
            e = dot(wut_ref[rows, :], m) + param(small_ref, 5 + c)
            hid, slope = gelu_parts(e)
            hid = hid.astype(BF16)
            hid_buf[slot, rows, :] = hid
            slope_buf[slot, rows, :] = slope.astype(BF16)
            out = out + dot(wdt_ref[:, rows], hid)
        sq_ref[u] = squares_of(out)
        z = out + x
        z_ref[u] = z
        unit_values, _ = standardize(z)
        a2_ref[base + place] = (unit_values * param(small_ref, 0) + param(small_ref, 1)).astype(BF16)
        for copy in store(i):
            copy.start()
        return carry

    lax.fori_loop(0, UNITS, feed, 0)
    for i in (UNITS - 2, UNITS - 1):
        for copy in store(i):
            copy.wait()
    normal(0).wait()
    normal(1).wait()
    for o in (2, 3, 1):
        target(o).wait()
        own(o).wait_send()
        shared(o).wait_send()

    @pl.when(chip == 0)
    def _():
        target_shared(2).wait_send()
        target_shared(3).wait_recv()

    @pl.when(chip == 1)
    def _():
        target_shared(3).wait_send()
        target_shared(1).wait_send()
        target_shared(2).wait_recv()
        target_shared(1).wait_recv()

    for kind in range(3):
        for k in offsets:
            scatter(kind, k).wait_send()
            gather(kind, k).wait_send()
        for which in range(3):
            side(kind, which).wait_send()
    for k in offsets:
        small(k).wait_send()


VM = pl.BlockSpec(memory_space=pltpu.VMEM)
HB = pl.BlockSpec(memory_space=pltpu.HBM)


def shape_of(shape, dtype=BF16):
    return jax.ShapeDtypeStruct(shape, dtype)


KEYS = [
    shape_of((HEADS, HD, ALL * BLK)),
    shape_of((2, ALL, BLK, 128)),
    shape_of((2, ALL, BLK, 128)),
]
ATTEND_SCRATCH = [
    pltpu.VMEM((BLK, BLK), F32),
    pltpu.VMEM((2, OWN, BLK, BLK), F32),
    pltpu.VMEM((2, OWN * BLK, BLK), BF16),
]
BACK_SCRATCH = [
    pltpu.VMEM((BLK, BLK), F32),
    pltpu.VMEM((2, OWN * BLK, BLK), BF16),
    pltpu.VMEM((2, OWN * BLK, BLK), BF16),
    pltpu.VMEM((HEADS, HD, ALL * BLK), F32),
    pltpu.VMEM((HEADS, HD, ALL * BLK), F32),
    pltpu.VMEM((2, OWN, BLK, BLK), BF16),
    pltpu.VMEM((2, 2, BLK, BLK), BF16),
    *pair_of_sems((2, 2)),
]


def stage_call(body, name, args, outs, scratch, mib, flops, hbm_in=(), hbm_out=(), **comm):
    return pl.pallas_call(
        body,
        in_specs=[HB if i in hbm_in else VM for i in range(len(args))],
        out_specs=[HB if i in hbm_out else VM for i in range(len(outs))],
        out_shape=outs,
        scratch_shapes=scratch,
        compiler_params=pltpu.CompilerParams(vmem_limit_bytes=mib << 20, has_side_effects=bool(comm), **comm),
        cost_estimate=cost(flops, 1 << 20),
        name=name,
    )(*args)


def first_stage(n, pk, pp, x, c):
    rows = D // n
    tile, eight = (UNITS, BLK, BLK), (ALL, BLK, BLK)
    outs = [shape_of(eight), shape_of(eight), shape_of(eight)] + KEYS
    outs += [shape_of(tile), shape_of((UNITS, 2, 8, BLK), F32), shape_of(tile, F32)]
    outs += [shape_of((UNITS, FF, BLK)), shape_of((UNITS, FF, BLK)), shape_of(tile, F32), shape_of(eight)]
    outs += [shape_of((UNITS, 8, BLK), F32), shape_of((3 * D, D)), shape_of((D, D)), shape_of((FF, D))]
    outs += [shape_of((D, FF)), shape_of((SMALL * D, 128), F32), shape_of((3, 4, n, rows, D)), shape_of(tile)]
    scratch = [pltpu.VMEM((HEADS, VROWS, ALL * BLK), BF16)] + ATTEND_SCRATCH
    scratch += [
        pltpu.VMEM(eight, BF16),
        pltpu.VMEM((3, n, rows, D), BF16),
        pltpu.VMEM((n, 24, 128), F32),
        pltpu.VMEM((3, rows, D), BF16),
        *pair_of_sems((3, n)),
        *pair_of_sems((3, n)),
        *pair_of_sems((n,)),
        *pair_of_sems((3, 3)),
        *pair_of_sems((4, 2)),
        *pair_of_sems((8,)),
        *pair_of_sems((2,)),
        pltpu.VMEM((2, FF, BLK), BF16),
        pltpu.VMEM((2, FF, BLK), BF16),
        pltpu.SemaphoreType.DMA((2, 2)),
    ]
    return stage_call(
        partial(first_stage_body, n), "first_stage", [pk, pp, x, c], outs, scratch, FIRST_MIB, 8e9, hbm_out=(9, 10),
        collective_id=0,
    )


def feed_back_tail(
    u, g, gy, r_unit, r_inv, m, o, small_ref, parts, w_ref, gr_ref, go_ref, gd_acc, gu_acc, go_acc, tail_acc
):
    tail_acc[2 * D : 3 * D, :] += fold(gy.astype(F32))
    gm = jnp.zeros((D, BLK), F32)
    for c in range(FF // BLK):
        rows = slice(c * BLK, (c + 1) * BLK)
        hid, slope = parts(c)
        gd_acc[rows, :] += dot_nt(hid, gy)
        ge = (dot(matrix(w_ref, 2, c), gy) * slope).astype(BF16)
        gu_acc[:, rows] += dot_nt(m, ge)
        tail_acc[3 * D + c * BLK : 3 * D + (c + 1) * BLK, :] += fold(ge.astype(F32))
        gm = gm + dot(matrix(w_ref, 1, c), ge)
    tail_acc[0:D, :] += fold(gm * r_unit)
    tail_acc[D : 2 * D, :] += fold(gm)
    gr = g + standardize_back(gm * param(small_ref, 2), r_unit, r_inv)
    gr_ref[u] = gr
    ga = gr.astype(BF16)
    go_acc[...] += dot_nt(o, ga)
    go_ref[u] = dot(matrix(w_ref, 0, 3), ga).astype(BF16)


TAIL = 3 * D + FF


def second_stage_body(
    a_ref, z_ref, cot_ref, w_ref, wt_ref, wot_ref, wut_ref, wdt_ref, small_ref,
    final_ref, sq_ref, gr_ref, gd_acc, gu_acc, go_acc, tail_acc, dq_ref, dk_ref, dv_ref,
    q_ref, kt_ref, k_ref, v_ref, vt_ref, o_ref, log_ref, go_ref, score_ref, hid_buf, slope_buf,
    mask_ref, prob_ref, ds_ref, dk_acc, dv_acc, part_ref, got_ref, ds0, ds1,
):
    seq = lax.axis_index("seq")
    core = seq % 2
    peer = peers_of(seq)[1]
    greet(1, 0, [peer], False)
    set_mask(mask_ref)
    vt_ref[:, HD:, :] = jnp.ones((HEADS, VROWS - HD, ALL * BLK), BF16)
    for acc in (gd_acc, gu_acc, go_acc, tail_acc):
        acc[...] = jnp.zeros_like(acc)

    def begin(j, carry):
        project(j, a_ref[j], wt_ref, q_ref, kt_ref, vt_ref, k_ref, v_ref)
        return carry

    lax.fori_loop(0, ALL, begin, 0)
    attend(core, q_ref, k_ref, vt_ref, o_ref, log_ref, mask_ref, score_ref, prob_ref)

    def feed(u, carry):
        r, r_unit, r_inv, m = forward_parts(z_ref[u], o_ref[u], wot_ref, small_ref)
        out = r + param(small_ref, 4)
        for c in range(FF // BLK):
            rows = slice(c * BLK, (c + 1) * BLK)
            e = dot(wut_ref[rows, :], m) + param(small_ref, 5 + c)
            hid, slope = gelu_parts(e)
            hid = hid.astype(BF16)
            hid_buf[rows, :] = hid
            slope_buf[rows, :] = slope
            out = out + dot(wdt_ref[:, rows], hid)
        sq_ref[u] = squares_of(out)
        final_ref[u] = out.T.astype(BF16)
        gy = cot_ref[u].T
        feed_back_tail(
            u, gy.astype(F32), gy, r_unit, r_inv, m, o_ref[u], small_ref,
            lambda c: (hid_buf[c * BLK : (c + 1) * BLK, :], slope_buf[c * BLK : (c + 1) * BLK, :]),
            w_ref, gr_ref, go_ref, gd_acc, gu_acc, go_acc, tail_acc,
        )
        return carry

    lax.fori_loop(0, UNITS, feed, 0)
    attend_back(
        core, q_ref, k_ref, kt_ref, v_ref, go_ref, o_ref, log_ref, dq_ref, dk_ref, dv_ref, mask_ref, prob_ref, ds_ref, dk_acc, dv_acc,
        part_ref, got_ref, ds0, ds1, peer,
    )


def second_stage(a, z, cot, w, wt, wot, wut, wdt, small):
    tile, eight = (UNITS, BLK, BLK), (ALL, BLK, BLK)
    outs = [shape_of(tile), shape_of((UNITS, 8, BLK), F32), shape_of(tile, F32), shape_of((FF, D), F32)]
    outs += [shape_of((D, FF), F32), shape_of((D, D), F32), shape_of((TAIL, 128), F32), shape_of(tile)]
    outs += [shape_of(tile), shape_of(tile)]
    scratch = [pltpu.VMEM(eight, BF16)] + [pltpu.VMEM(s.shape, s.dtype) for s in KEYS]
    scratch += [pltpu.VMEM((HEADS, VROWS, ALL * BLK), BF16), pltpu.VMEM(tile, BF16)]
    scratch += [pltpu.VMEM((UNITS, 2, 8, BLK), F32), pltpu.VMEM(tile, BF16), ATTEND_SCRATCH[1]]
    scratch += [pltpu.VMEM((FF, BLK), BF16), pltpu.VMEM((FF, BLK), F32)] + BACK_SCRATCH
    return stage_call(
        second_stage_body, "second_stage", [a, z, cot, w, wt, wot, wut, wdt, small], outs, scratch, SECOND_MIB, 20e9,
        collective_id=1,
    )


def project_weights(a, dq, dk, dv, gqkv_acc):
    gqkv_acc[0] += dot_nt(a, dq)
    gqkv_acc[1] += dot_nt(a, dk)
    gqkv_acc[2] += dot_nt(a, dv)


def project_back(z, dq, dk, dv, gr, small_ref, w_ref, head_acc):
    grad = dot(matrix(w_ref, 0, 0), dq) + dot(matrix(w_ref, 0, 1), dk) + dot(matrix(w_ref, 0, 2), dv)
    unit_values, inverse = standardize(z)
    head_acc[0:D, :] += fold(grad * unit_values)
    head_acc[D : 2 * D, :] += fold(grad)
    return gr + standardize_back(grad * param(small_ref, 0), unit_values, inverse)


def third_stage_body(
    n, dq_in, dk_in, dv_in, a2_ref, z_ref, gr_in, hid_ref, slope_ref, r_ref, o_ref, log_ref, q_ref, kt_ref, k_ref, v_ref,
    small_ref, w_ref, gd_in, gu_in, go_in, tail_in, a_ref, xt_ref, sq1_ref, sq2_ref, f_ref,
    sum_ref, p_ref, fo_ref, io_ref,
    gz_ref, gr_ref, gd_acc, gu_acc, go_acc, tail_acc, gqkv_acc, head_acc, dq_ref, dk_ref, dv_ref, i_ref,
    g_ref, pp_ref, half_ref, quarter_ref, out_ref, mine_ref, slot_ref, chunk_ref, pslot_ref, psum_ref,
    as0, as1, bs0, bs1, ss0, ss1, rs0, rs1, gs0, gs1, ps0, ps1, xs0, xs1,
    go_ref, hid_buf, slope_buf, hs, mask_ref, prob_ref, ds_ref, dk_acc, dv_acc, part_ref, got_ref, ds0, ds1,
):
    dp = lax.axis_index("dp")
    seq = lax.axis_index("seq")
    chip, core = seq // 2, seq % 2
    peers = peers_of(seq)
    offsets = range(1, n)

    def half(kind, j):
        part = peers[1] if j == 0 else peers[3]
        return send(g_ref.at[kind, part], half_ref.at[kind, j], (as0, as1), (kind, j), {"seq": peers[1]})

    def cross(kind):
        return send(out_ref.at[kind], quarter_ref.at[kind], (bs0, bs1), kind, {"seq": peers[2]})

    def scatter(kind, k):
        to = (dp + k) % n
        return send(mine_ref.at[kind, to], slot_ref.at[kind, k], (ss0, ss1), (kind, k), {"dp": to})

    def gather(kind, k):
        return send(chunk_ref.at[kind], sum_ref.at[kind, seq, dp], (rs0, rs1), (kind, k), {"dp": (dp + k) % n})

    def side(kind, which):
        part = peers[2] if which == 2 else seq
        to = peers[2] if which == 0 else peers[1]
        return send(sum_ref.at[kind, part], sum_ref.at[kind, part], (gs0, gs1), (kind, which), {"seq": to})

    def small(k):
        if k == 0:
            return send(pp_ref, pslot_ref.at[0], (ps0, ps1), 0, {"seq": peers[1]})
        if k == 1:
            return send(psum_ref.at[0], pslot_ref.at[1], (ps0, ps1), 1, {"seq": peers[2]})
        return send(psum_ref.at[1], pslot_ref.at[k], (ps0, ps1), k, {"dp": (dp + k - 1) % n})

    def halves(kind):
        half(kind, 0).start()
        half(kind, 1).start()

    def crossing(kind):
        half(kind, 0).wait_recv()
        half(kind, 1).wait_recv()
        out_ref[kind] = (g_ref[kind, peers[2]].astype(F32) + half_ref[kind, 1].astype(F32)).astype(BF16)
        cross(kind).start()

    def scattering(kind):
        cross(kind).wait_recv()
        mine_ref[kind] = (
            g_ref[kind, seq].astype(F32) + half_ref[kind, 0].astype(F32) + quarter_ref[kind].astype(F32)
        ).astype(BF16)
        for k in offsets:
            scatter(kind, k).start()

    def gathering(kind):
        total = mine_ref[kind, dp].astype(F32)
        for k in offsets:
            scatter(kind, k).wait_recv()
            total = total + slot_ref[kind, k].astype(F32)
        chunk_ref[kind] = total.astype(BF16)
        sum_ref[kind, seq, dp] = total.astype(BF16)
        for k in offsets:
            gather(kind, k).start()

    def sharing(kind):
        for k in offsets:
            gather(kind, k).wait_recv()
        side(kind, 0).start()
        side(kind, 1).start()

    def passing(kind):
        side(kind, 0).wait_recv()
        side(kind, 2).start()

    def settled(kind):
        side(kind, 1).wait_recv()
        side(kind, 2).wait_recv()

    own = 3 * chip + core

    def move(which, o, source_ref, target_ref):
        return send(source_ref.at[peers[o]], target_ref.at[own], (xs0, xs1), (which, o), {"seq": peers[o]})

    def move_shared(which, o, source_ref, target_ref):
        source = source_ref.at[4 if o == 2 else 5]
        return send(source, target_ref.at[2 if o == 3 else 5], (xs0, xs1), (which, 4 + o), {"seq": peers[o]})

    def start_moves(which, source_ref, target_ref):
        pl.when(chip == 0)(lambda: move_shared(which, 3, source_ref, target_ref).start())
        pl.when(chip == 1)(lambda: move_shared(which, 2, source_ref, target_ref).start())
        pl.when(chip == 1)(lambda: move_shared(which, 1, source_ref, target_ref).start())
        for o in (2, 3, 1):
            move(which, o, source_ref, target_ref).start()
        target_ref[own] = source_ref[seq]
        pl.when(chip == 0)(lambda: target_ref.__setitem__(2, source_ref[4]))

    def finish_moves(which, source_ref, target_ref):
        @pl.when(chip == 0)
        def _():
            move_shared(which, 3, source_ref, target_ref).wait_send()
            move_shared(which, 2, source_ref, target_ref).wait_recv()

        @pl.when(chip == 1)
        def _():
            move_shared(which, 2, source_ref, target_ref).wait_send()
            move_shared(which, 1, source_ref, target_ref).wait()
            move_shared(which, 3, source_ref, target_ref).wait_recv()

        for o in (2, 3, 1):
            move(which, o, source_ref, target_ref).wait()

    def fetch(u):
        slot = u % 2
        return (
            pltpu.make_async_copy(hid_ref.at[u], hid_buf.at[slot], hs.at[0, slot]),
            pltpu.make_async_copy(slope_ref.at[u], slope_buf.at[slot], hs.at[1, slot]),
        )

    split = lambda values: values.astype(BF16).reshape(g_ref.shape[2:])
    for copy in fetch(0):
        copy.start()
    greet(n, dp, [peers[1], peers[2], peers[3]], True)
    start_moves(0, f_ref, fo_ref)
    set_mask(mask_ref)
    gqkv_acc[...] = jnp.zeros_like(gqkv_acc)
    head_acc[...] = jnp.zeros_like(head_acc)
    for acc, given in ((gd_acc, gd_in), (gu_acc, gu_in), (go_acc, go_in), (tail_acc, tail_in)):
        acc[...] = given[...]

    def feed(u, carry):
        @pl.when(u < UNITS - 1)
        def _():
            for copy in fetch(u + 1):
                copy.start()

        for copy in fetch(u):
            copy.wait()
        slot = u % 2
        place, base = unit_place(u, core)
        project_weights(a2_ref[base + place], dq_in[u], dk_in[u], dv_in[u], gqkv_acc)
        g = project_back(z_ref[u], dq_in[u], dk_in[u], dv_in[u], gr_in[u], small_ref, w_ref, head_acc)
        gz_ref[u] = g
        r_unit, r_inv = standardize(r_ref[u])
        m = (r_unit * param(small_ref, 2) + param(small_ref, 3)).astype(BF16)
        feed_back_tail(
            u, g, g.astype(BF16), r_unit, r_inv, m, o_ref[u], small_ref,
            lambda c: (
                hid_buf[slot, c * BLK : (c + 1) * BLK, :],
                slope_buf[slot, c * BLK : (c + 1) * BLK, :].astype(F32),
            ),
            w_ref, gr_ref, go_ref, gd_acc, gu_acc, go_acc, tail_acc,
        )
        return carry

    lax.fori_loop(0, UNITS, feed, 0)
    for c in range(4):
        g_ref[1, c] = split(gu_acc[:, c * D : (c + 1) * D])
        g_ref[2, c] = split(gd_acc[c * D : (c + 1) * D, :])
    halves(1)
    halves(2)

    def progress(i):
        @pl.when(i == 1)
        def _():
            crossing(1)
            crossing(2)

        @pl.when(i == 6)
        def _():
            scattering(1)
            scattering(2)

    attend_back(
        core, q_ref, k_ref, kt_ref, v_ref, go_ref, o_ref, log_ref, dq_ref, dk_ref, dv_ref, mask_ref, prob_ref, ds_ref, dk_acc, dv_acc,
        part_ref, got_ref, ds0, ds1, peers[1], progress,
    )
    gathering(1)
    gathering(2)

    def early(u, carry):
        place, base = unit_place(u, core)
        project_weights(a_ref[base + place], dq_ref[u], dk_ref[u], dv_ref[u], gqkv_acc)
        return carry

    lax.fori_loop(0, UNITS, early, 0)
    for t in range(3):
        g_ref[0, t] = split(gqkv_acc[t])
    g_ref[0, 3] = split(go_acc[...])
    halves(0)

    def end(u, carry):
        pl.when(u == 1)(lambda: crossing(0))
        place, base = unit_place(u, core)
        g = project_back(
            xt_ref[base + place].astype(F32), dq_ref[u], dk_ref[u], dv_ref[u], gr_ref[u], small_ref, w_ref, head_acc
        )
        i_ref[u] = (g + gz_ref[u]).T.astype(BF16)
        return carry

    lax.fori_loop(0, UNITS, end, 0)
    start_moves(1, i_ref, io_ref)
    for row in range(SMALL):
        for part in range(2):
            ref, first = (head_acc, row) if row < 2 else (tail_acc, row - 2)
            first = first * D + part * 128
            pp_ref[2 * row + part : 2 * row + part + 1, :] = jnp.sum(ref[first : first + 128, :].T, axis=0, keepdims=True)
    sequences = 6 * n
    place = lax.broadcasted_iota(jnp.int32, (6, 128), 0) * 128 + lax.broadcasted_iota(jnp.int32, (6, 128), 1)
    stats = jnp.zeros((6, 128), F32)
    for i, ref in enumerate((sq1_ref, sq2_ref)):
        lines = [jnp.sum(ref[u], axis=0, keepdims=True) for u in range(UNITS)]
        mine = jnp.sum(lines[0] + lines[1] + lines[2] + lines[3], axis=1, keepdims=True)
        shared = jnp.sum(lines[4] + lines[5], axis=1, keepdims=True)
        start = i * sequences + 6 * dp + 3 * chip
        stats = jnp.where(place == start + core, jnp.broadcast_to(mine, (6, 128)), stats)
        stats = jnp.where(place == start + 2, jnp.broadcast_to(shared, (6, 128)), stats)
    pp_ref[18:24, :] = stats
    small(0).start()
    scattering(0)
    small(0).wait_recv()
    psum_ref[0] = pp_ref[...] + pslot_ref[0]
    small(1).start()
    small(1).wait_recv()
    psum_ref[1] = psum_ref[0] + pslot_ref[1]
    for k in offsets:
        small(1 + k).start()
    sharing(1)
    sharing(2)
    gathering(0)
    passing(1)
    passing(2)
    total = psum_ref[1]
    for k in offsets:
        small(1 + k).wait_recv()
        total = total + pslot_ref[1 + k]
    p_ref[...] = total
    sharing(0)
    settled(1)
    settled(2)
    passing(0)
    settled(0)
    finish_moves(0, f_ref, fo_ref)
    finish_moves(1, i_ref, io_ref)
    for kind in range(3):
        half(kind, 0).wait_send()
        half(kind, 1).wait_send()
        cross(kind).wait_send()
        for k in offsets:
            scatter(kind, k).wait_send()
            gather(kind, k).wait_send()
        for which in range(3):
            side(kind, which).wait_send()
    for k in range(n + 1):
        small(k).wait_send()


def third_stage(n, *args):
    rows = D // n
    tile = (UNITS, BLK, BLK)
    quarter = (3, n, rows, D)
    outs = [shape_of((3, 4, n, rows, D)), shape_of((24, 128), F32), shape_of(tile), shape_of(tile)]
    scratch = [
        pltpu.VMEM(tile, F32),
        pltpu.VMEM(tile, F32),
        pltpu.VMEM((FF, D), F32),
        pltpu.VMEM((D, FF), F32),
        pltpu.VMEM((D, D), F32),
        pltpu.VMEM((TAIL, 128), F32),
        pltpu.VMEM((3, D, D), F32),
        pltpu.VMEM((2 * D, 128), F32),
        pltpu.VMEM(tile, BF16),
        pltpu.VMEM(tile, BF16),
        pltpu.VMEM(tile, BF16),
        pltpu.VMEM(tile, BF16),
        pltpu.VMEM((3, 4, n, rows, D), BF16),
        pltpu.VMEM((24, 128), F32),
        pltpu.VMEM((3, 2, n, rows, D), BF16),
        pltpu.VMEM(quarter, BF16),
        pltpu.VMEM(quarter, BF16),
        pltpu.VMEM(quarter, BF16),
        pltpu.VMEM(quarter, BF16),
        pltpu.VMEM((3, rows, D), BF16),
        pltpu.VMEM((1 + n, 24, 128), F32),
        pltpu.VMEM((2, 24, 128), F32),
        *pair_of_sems((3, 2)),
        *pair_of_sems((3,)),
        *pair_of_sems((3, n)),
        *pair_of_sems((3, n)),
        *pair_of_sems((3, 3)),
        *pair_of_sems((1 + n,)),
        *pair_of_sems((2, 8)),
        pltpu.VMEM(tile, BF16),
        pltpu.VMEM((2, FF, BLK), BF16),
        pltpu.VMEM((2, FF, BLK), BF16),
        pltpu.SemaphoreType.DMA((2, 2)),
        *BACK_SCRATCH,
    ]
    return stage_call(
        partial(third_stage_body, n), "third_stage", args, outs, scratch, THIRD_MIB, 20e9, hbm_in=(6, 7), collective_id=2
    )


FIRST_MIB, SECOND_MIB, THIRD_MIB, ADAM_MIB = 38, 22, 31, 58


def owner_scalars(owner_ref):
    sizes = [D * D] * 4 + [D * FF, FF * D, SMALL * D]
    starts = []
    for t in range(7):
        offset = jnp.int32(0)
        for u in range(t):
            offset = offset + jnp.where(owner_ref[u] == owner_ref[t], sizes[u], 0).astype(jnp.int32)
        starts.append(offset)
    return starts


def pack_body(owner_ref, row_ref, w_ref, p_ref):
    dp = lax.axis_index("dp")
    seq = lax.axis_index("seq")
    starts = owner_scalars(owner_ref)
    square = jnp.where(seq == 0, starts[0], jnp.where(seq == 1, starts[1], jnp.where(seq == 2, starts[2], starts[3])))
    plans = (
        (owner_ref[seq], square // 128, 2),
        (owner_ref[4], starts[4] // 128 + 2 * seq, FF // 128),
        (owner_ref[5], starts[5] // 128 + 2 * D * seq, 2),
    )
    for kind, (owner, base, stride) in enumerate(plans):
        keep = jnp.where(owner == dp, 1.0, 0.0).astype(F32)
        for side in range(2):
            values = row_ref[pl.ds(base + side, D, stride=stride), :]
            w_ref[kind, :, side * 128 : (side + 1) * 128] = (values * keep).astype(BF16)
    keep = jnp.where(owner_ref[6] == dp, 1.0, 0.0).astype(F32)
    values = row_ref[pl.ds(pl.multiple_of(starts[6] // 128, 8), 24), :] * keep
    rows = lax.broadcasted_iota(jnp.int32, (24, 128), 0)
    p_ref[...] = jnp.where(rows < 2 * SMALL, values, 0.0)


def pack(owner_list, row):
    return pl.pallas_call(
        pack_body,
        in_specs=[pl.BlockSpec(memory_space=pltpu.SMEM), pl.BlockSpec(memory_space=pltpu.VMEM)],
        out_specs=[pl.BlockSpec(memory_space=pltpu.VMEM)] * 2,
        out_shape=[jax.ShapeDtypeStruct((3, D, D), BF16), jax.ShapeDtypeStruct((24, 128), F32)],
        compiler_params=pltpu.CompilerParams(vmem_limit_bytes=20 << 20),
        cost_estimate=cost(1, 3 << 20),
        name="pack",
    )(owner_list, row)


ROWS = D * D // 128


def adam_body(owner_ref, g_ref, p_ref, f_ref, i_ref, m_ref, v_ref, w_ref, m_out, v_out, w_out, f_out, i_out, grad_ref):
    dp = lax.axis_index("dp")
    block = pl.program_id(0)
    starts = owner_scalars(owner_ref)
    counts = [1, 1, 1, 1, 4, 4, 1]
    rate = jnp.float32(D ** (-0.5))
    decay = jnp.float32(0.1)
    limit = jnp.int32(0)
    f_out[...] = f_ref[...].astype(F32)
    i_out[...] = i_ref[...].astype(F32)
    for t in range(7):
        first = starts[t] // (D * D)
        here = (owner_ref[t] == dp) & (block >= first) & (block < first + counts[t])
        part = block - first
        limit = jnp.where(here, 2 * SMALL if t == 6 else ROWS, limit)
        if t == 5:
            rate = jnp.where(here, FF ** (-0.5), rate)
        if t == 6:
            rate = jnp.where(here, 0.5, rate)
            decay = jnp.where(here, 0.0, decay)

        @pl.when(here)
        def _(t=t, part=part):
            if t == 6:
                grad_ref[0:24, :] = p_ref[...]
            elif t == 4:
                for c in range(4):
                    piece = g_ref[4 + c, pl.ds(pl.multiple_of(part * 64, 64), 64), :].astype(F32)
                    for side in range(2):
                        grad_ref[pl.ds(2 * c + side, 64, stride=8), :] = piece[:, side * 128 : (side + 1) * 128]
            else:
                for r in range(4):
                    piece = g_ref[8 + part if t == 5 else t, r * 64 : (r + 1) * 64, :].astype(F32)
                    for side in range(2):
                        grad_ref[pl.ds(r * 128 + side, 64, stride=2), :] = piece[:, side * 128 : (side + 1) * 128]

    @pl.when(limit == 0)
    def _():
        for out in (m_out, v_out, w_out):
            out[...] = jnp.zeros_like(out)

    @pl.when(limit > 0)
    def _():
        scale = 1.0 / (1.0 - 0.5**STEP)
        for r in range(0, ROWS, PIECE):
            rows = slice(r, r + PIECE)
            grad = grad_ref[rows, :]
            valid = lax.broadcasted_iota(jnp.int32, (PIECE, 128), 0) + r < limit
            first_new = 0.5 * m_ref[rows, :] + 0.5 * grad
            second_new = 0.5 * v_ref[rows, :] + 0.5 * grad * grad
            old = w_ref[rows, :]
            update = first_new * scale / (jnp.sqrt(second_new * scale) + adam_eps) + decay * old
            m_out[rows, :] = jnp.where(valid, first_new, 0.0)
            v_out[rows, :] = jnp.where(valid, second_new, 0.0)
            w_out[rows, :] = jnp.where(valid, old - rate * update, 0.0)


PIECE = 64


def adam(owner_list, g, p, f, i, m, v, w):
    blocks = m.shape[0] // ROWS
    tile = pl.BlockSpec((ROWS, 128), lambda b, t: (b, 0))
    states = pl.BlockSpec((f.shape[0] // blocks, D), lambda b, t: (b, 0))
    out = jax.ShapeDtypeStruct(m.shape, F32)
    state = jax.ShapeDtypeStruct(f.shape, F32)
    whole = pl.BlockSpec(memory_space=pltpu.VMEM)
    spec = pltpu.PrefetchScalarGridSpec(
        num_scalar_prefetch=1,
        grid=(blocks,),
        in_specs=[whole, whole, states, states, tile, tile, tile],
        out_specs=[tile, tile, tile, states, states],
        scratch_shapes=[pltpu.VMEM((ROWS, 128), F32)],
    )
    return pl.pallas_call(
        adam_body,
        grid_spec=spec,
        out_shape=[out, out, out, state, state],
        compiler_params=params_of(mib=ADAM_MIB),
        cost_estimate=cost(20 * 524288, 14 << 20),
        name="adam",
    )(owner_list, g, p, f, i, m, v, w)


def per_device(inputs, cotangent, owner_list, master_rows, moment1_rows, moment2_rows):
    n = lax.axis_size("dp")
    rows = D // n
    flat = [r.reshape(-1, 128) for r in (master_rows, moment1_rows, moment2_rows)]
    pk, pp = pack(owner_list, flat[0])
    (xt, a1, q1, kt1, k1, v1, o1, log1, r1, hid, slope, z2, a2, sq1, wt, wot, wut, wdt, small, w, cot) = first_stage(
        n, pk.reshape(3, n, rows, D), pp, inputs, cotangent
    )
    final, sq2, gr, gd, gu, gout, tail, dq, dk, dv = second_stage(a2, z2, cot, w, wt, wot, wut, wdt, small)
    g, p, final, grad = third_stage(
        n, dq, dk, dv, a2, z2, gr, hid, slope, r1, o1, log1, q1, kt1, k1, v1, small, w, gd, gu, gout, tail,
        a1, xt, sq1, sq2, final,
    )
    states = [r.reshape(-1, D) for r in (final, grad)]
    m_new, v_new, w_new, final, grad = adam(owner_list, g.reshape(12, D, D), p, *states, flat[1], flat[2], flat[0])
    sequences = inputs.shape[0] * n
    entries = inputs.shape[1] * lax.axis_size("seq") * D
    squares = p[18:].reshape(-1)[: 2 * sequences].reshape(2, sequences)
    stats = jnp.sqrt(squares / entries + stat_eps)
    back = lambda r: r.reshape(master_rows.shape)
    return (final.reshape(inputs.shape), grad.reshape(inputs.shape), stats, back(m_new), back(v_new), back(w_new))


def solution(mesh):
    placed = (P("dp", "seq", None), P("dp", "seq", None), P(), P("dp", None), P("dp", None), P("dp", None))
    return jax.shard_map(
        per_device,
        mesh=mesh,
        in_specs=placed,
        out_specs=(P("dp", "seq", None), P("dp", "seq", None), P(), P("dp", None), P("dp", None), P("dp", None)),
        check_vma=False,
    )
```

```python
import math
from functools import partial

import jax
import jax.numpy as jnp
from jax import lax
from jax.experimental import pallas as pl
from jax.experimental.pallas import tpu as pltpu
from jax.sharding import PartitionSpec as P

D = 256
HEADS = 4
HD = 64
FF = 1024
STEP = 3
SMALL = 9
BLK = 256
OWN = 4
UNITS = 6
ALL = 8
F32 = jnp.float32
BF16 = jnp.bfloat16
MESH = pl.DeviceIdType.MESH

norm_eps = 1e-05
stat_eps = 1e-06
adam_eps = 1e-08
masked_score = -1e30


def dot(left, right):
    return lax.dot_general(left, right, (((1,), (0,)), ((), ())), preferred_element_type=F32)


def dot_nt(left, right):
    return lax.dot_general(left, right, (((1,), (1,)), ((), ())), preferred_element_type=F32)


def wide(column):
    return jnp.concatenate([column, column], axis=1)


def fold(values):
    return values[:, :128] + values[:, 128:]


def standardize(values):
    average = jnp.mean(values, axis=0, keepdims=True)
    centered = values - average
    spread = jnp.mean(centered * centered, axis=0, keepdims=True)
    inverse = lax.rsqrt(spread + norm_eps)
    return centered * inverse, inverse


def standardize_back(grad, unit_values, inverse):
    average = jnp.mean(grad, axis=0, keepdims=True)
    inner = jnp.mean(grad * unit_values, axis=0, keepdims=True)
    return (grad - average - unit_values * inner) * inverse


def param(small_ref, row):
    return wide(small_ref[row * D : (row + 1) * D, :])


def gelu_parts(e):
    cdf = 0.5 * lax.erf(e * math.sqrt(0.5)) + 0.5
    hid = e * cdf
    slope = cdf + e * (jnp.exp(-0.5 * e * e) * (1.0 / math.sqrt(2.0 * math.pi)))
    return hid, slope


def full(shape):
    return pl.BlockSpec(shape, lambda *args: (0,) * len(shape), pipeline_mode=pl.Buffered(1))


def params_of(ndims=1, mib=56):
    return pltpu.CompilerParams(
        dimension_semantics=("arbitrary",) * ndims, vmem_limit_bytes=mib << 20
    )


def cost(flops, nbytes, trans=0):
    return pl.CostEstimate(flops=int(flops), bytes_accessed=int(nbytes), transcendentals=int(trans))


LOG2E = math.log2(math.e)
VROWS = HD + 16


def unit_place(unit, core):
    later = unit // OWN
    place = (1 - later) * unit + later * (core + (unit - OWN) * (3 - 2 * core))
    return place, later * OWN


def lanes(start, size):
    return pl.ds(pl.multiple_of(start, BLK), size)


def pair_rows(pair):
    return pl.ds(pl.multiple_of(pair * 128, 128), 128)


def matrix(w_ref, kind, part):
    n, rows = w_ref.shape[2:4]
    if rows % 16 == 0:
        return w_ref[kind, part].reshape(D, D)
    return jnp.concatenate([w_ref[kind, part, i] for i in range(n)], axis=0)


def peers_of(seq):
    return {1: seq + 1 - 2 * (seq % 2), 2: (seq + 2) % 4, 3: 3 - seq}


def greet(n, dp, peers, wide_group):
    barrier = pltpu.get_barrier_semaphore()
    count = 0
    for peer in peers:
        pl.semaphore_signal(barrier, inc=1, device_id={"seq": peer}, device_id_type=MESH)
        count += 1
    if wide_group:
        for k in range(1, n):
            pl.semaphore_signal(barrier, inc=1, device_id={"dp": (dp + k) % n}, device_id_type=MESH)
            count += 1
    pl.semaphore_wait(barrier, count)


def send(source, target, sems, index, device):
    return pltpu.make_async_remote_copy(
        src_ref=source,
        dst_ref=target,
        send_sem=sems[0].at[index],
        recv_sem=sems[1].at[index],
        device_id=device,
        device_id_type=MESH,
    )


def pair_of_sems(shape):
    return [pltpu.SemaphoreType.DMA(shape), pltpu.SemaphoreType.DMA(shape)]


def project(j, a, wt_ref, q_ref, kt_ref, vt_ref, k_ref, v_ref):
    where = lanes(j * BLK, BLK)
    q_ref[j] = (dot(wt_ref[0:D], a) * HD ** (-0.5)).astype(BF16)
    kt = dot(wt_ref[D : 2 * D], a).astype(BF16)
    vt = dot(wt_ref[2 * D : 3 * D], a).astype(BF16)
    for h in range(HEADS):
        kt_ref[h, :, where] = kt[h * HD : (h + 1) * HD]
        vt_ref[h, 0:HD, where] = vt[h * HD : (h + 1) * HD]
    k = kt.T
    v = vt.T
    for h in range(2):
        k_ref[h, j] = k[:, h * 128 : (h + 1) * 128]
        v_ref[h, j] = v[:, h * 128 : (h + 1) * 128]


def head_rows(values, half):
    rows = lax.broadcasted_iota(jnp.int32, values.shape, 0)
    keep = (rows < HD) if half == 0 else (rows >= HD)
    return jnp.where(keep, values, jnp.zeros_like(values))


def set_mask(mask_ref):
    keys = lax.broadcasted_iota(jnp.int32, (BLK, BLK), 0)
    queries = lax.broadcasted_iota(jnp.int32, (BLK, BLK), 1)
    mask_ref[...] = jnp.where(keys <= queries, 0.0, masked_score)


def groups(values, op):
    out = values[0:8]
    for i in range(1, values.shape[0] // 8):
        out = op(out, values[i * 8 : (i + 1) * 8])
    return out


SUB = 128
BSUB = 256


def ordered(i):
    return (i + OWN) % UNITS


def attend(core, q_ref, k_ref, vt_ref, o_ref, log_ref, mask_ref, score_ref, prob_ref, progress=None):
    def step(i, carry):
        if progress is not None:
            progress(i)
        unit = ordered(i)
        place, base = unit_place(unit, core)

        def branch(last):
            keys = (last + 1) * BLK
            chunks = [(kb, sub) for kb in range(last + 1) for sub in range(BLK // SUB)]
            queries = [head_rows(q_ref[base + place, (h // 2) * 128 : (h // 2 + 1) * 128, :], h % 2) for h in range(HEADS)]
            tops = [None] * HEADS
            outs = [None] * HEADS

            def scores(h, kb, sub):
                rows = slice(sub * SUB, (sub + 1) * SUB)
                score = dot(k_ref[h // 2, base + kb, rows, :], queries[h])
                if kb == last:
                    score = score + mask_ref[rows, :]
                score_ref[h % 2, kb, rows, :] = score
                peak = groups(score, jnp.maximum)
                tops[h] = peak if tops[h] is None else jnp.maximum(tops[h], peak)

            def weights(h, kb, sub):
                rows = slice(sub * SUB, (sub + 1) * SUB)
                weight = jnp.exp(score_ref[h % 2, kb, rows, :] - tops[h])
                prob_ref[h % 2, kb * BLK + sub * SUB : kb * BLK + (sub + 1) * SUB, :] = weight.astype(BF16)

            def mixed(h, kb):
                part = dot(vt_ref[h, :, lanes((base + kb) * BLK, BLK)], prob_ref[h % 2, kb * BLK : (kb + 1) * BLK, :])
                outs[h] = part if outs[h] is None else outs[h] + part

            for t in range(HEADS + 2):
                if 0 <= t - 1 < HEADS:
                    tops[t - 1] = jnp.max(tops[t - 1], axis=0, keepdims=True)
                for kb, sub in chunks:
                    if t < HEADS:
                        scores(t, kb, sub)
                    if 0 <= t - 1 < HEADS:
                        weights(t - 1, kb, sub)
                    if 0 <= t - 2 < HEADS and sub == 0:
                        mixed(t - 2, kb)
                if 0 <= t - 2 < HEADS:
                    h = t - 2
                    total = outs[h][HD : HD + 1]
                    o_ref[unit, h * HD : (h + 1) * HD, :] = (outs[h][0:HD] / total).astype(BF16)
                    log_ref[unit, h // 2, h % 2 : h % 2 + 1, :] = tops[h] + jnp.log(total)

        for last in range(OWN):
            pl.when(place == last)(partial(branch, last))
        return carry

    lax.fori_loop(0, UNITS, step, 0)


def attend_back(
    core, q_ref, k_ref, kt_ref, v_ref, go_ref, o_ref, log_ref, dq_ref, dk_ref, dv_ref, mask_ref, prob_ref, slope_ref, dk_acc, dv_acc,
    part_ref, got_ref, ds0, ds1, peer, progress=None,
):
    dk_acc[...] = jnp.zeros_like(dk_acc)
    dv_acc[...] = jnp.zeros_like(dv_acc)
    pairs = ((0, dk_acc, dk_ref), (1, dv_acc, dv_ref))

    def piece(acc, j):
        return acc[:, :, j * BLK : (j + 1) * BLK].reshape(D, BLK)

    def swap(which, side):
        position = 1 - core if side == 0 else 2 + core
        return send(part_ref.at[which, position], got_ref.at[which, side], (ds0, ds1), (which, side), {"seq": peer})

    def step(i, carry):
        @pl.when(i == 2)
        def _():
            for which, acc, _ in pairs:
                for position in range(OWN):
                    part_ref[which, position] = piece(acc, OWN + position).astype(BF16)
            for which in range(2):
                for side in range(2):
                    swap(which, side).start()

        if progress is not None:
            progress(i)
        unit = ordered(i)
        place, base = unit_place(unit, core)

        def branch(last):
            chunks = [(kb, sub) for kb in range(last + 1) for sub in range(BLK // BSUB)]
            heads = []
            for h in range(HEADS):
                pair = slice((h // 2) * 128, (h // 2 + 1) * 128)
                block = q_ref[base + place, pair, :]
                go_block = go_ref[unit, pair, :]
                mine = slice((h % 2) * HD, (h % 2 + 1) * HD)
                inner = jnp.sum(
                    go_block[mine].astype(F32) * o_ref[unit, h * HD : (h + 1) * HD, :].astype(F32), axis=0, keepdims=True
                )
                heads.append(
                    (head_rows(block, h % 2), head_rows(go_block, h % 2), log_ref[unit, h // 2, h % 2 : h % 2 + 1, :], inner)
                )
            dqs = [None] * HEADS
            ready = {}

            def products(h, kb, sub):
                rows = slice(sub * BSUB, (sub + 1) * BSUB)
                q, go, _, _ = heads[h]
                ready[h, kb, sub] = (
                    dot(k_ref[h // 2, base + kb, rows, :], q),
                    dot(v_ref[h // 2, base + kb, rows, :], go),
                )

            def elements(h, kb, sub):
                rows = slice(sub * BSUB, (sub + 1) * BSUB)
                to = slice(kb * BLK + sub * BSUB, kb * BLK + (sub + 1) * BSUB)
                _, _, log_total, inner = heads[h]
                score, slope = ready.pop((h, kb, sub))
                if kb == last:
                    score = score + mask_ref[rows, :]
                weight = jnp.exp(score - log_total)
                prob_ref[h % 2, to, :] = weight.astype(BF16)
                slope_ref[h % 2, to, :] = (weight * (slope - inner)).astype(BF16)

            def gradients(h, kb, which):
                rows = slice(kb * BLK, (kb + 1) * BLK)
                where = lanes((base + kb) * BLK, BLK)
                head = slice(h * HD, (h + 1) * HD)
                if which == 0:
                    dv_acc[h, :, where] += dot_nt(go_ref[unit, head, :], prob_ref[h % 2, rows, :])
                elif which == 1:
                    dk_acc[h, :, where] += dot_nt(q_ref[base + place, head, :], slope_ref[h % 2, rows, :])
                else:
                    part = dot(kt_ref[h, :, where], slope_ref[h % 2, rows, :])
                    dqs[h] = part if dqs[h] is None else dqs[h] + part

            work = [(h, kb, sub) for h in range(HEADS) for kb, sub in chunks]
            per = BLK // BSUB
            products(*work[0])
            for at, (h, kb, sub) in enumerate(work):
                if at + 1 < len(work):
                    products(*work[at + 1])
                elements(h, kb, sub)
                if h > 0 and sub == 0:
                    for which in range(3):
                        gradients(h - 1, kb, which)
                if h > 0 and kb == last and sub == per - 1:
                    dq_ref[unit, (h - 1) * HD : h * HD, :] = (dqs[h - 1] * HD ** (-0.5)).astype(BF16)
            for kb in range(last + 1):
                for which in range(3):
                    gradients(HEADS - 1, kb, which)
            dq_ref[unit, (HEADS - 1) * HD :, :] = (dqs[HEADS - 1] * HD ** (-0.5)).astype(BF16)

        for last in range(OWN):
            pl.when(place == last)(partial(branch, last))
        return carry

    lax.fori_loop(0, UNITS, step, 0)
    for which, acc, ref in pairs:
        for j in range(OWN):
            ref[j] = piece(acc, j).astype(BF16)
    for which, acc, ref in pairs:
        for side, position in enumerate((core, 3 - core)):
            swap(which, side).wait()
            ref[OWN + side] = (part_ref[which, position].astype(F32) + got_ref[which, side].astype(F32)).astype(BF16)


def forward_parts(z, o, wot_ref, small_ref):
    r = z + dot(wot_ref[...], o)
    unit_values, inverse = standardize(r)
    m = (unit_values * param(small_ref, 2) + param(small_ref, 3)).astype(BF16)
    return r, unit_values, inverse, m


def squares_of(out):
    return groups(out * out, jnp.add)


def first_stage_body(
    n, pk_ref, pp_ref, x_ref, c_ref,
    xt_ref, a_ref, q_ref, kt_ref, k_ref, v_ref, o_ref, log_ref, r_ref, hid_ref, slope_ref, z_ref, a2_ref, sq_ref,
    wt_ref, wot_ref, wut_ref, wdt_ref, small_ref, w_ref, co_ref,
    vt_ref, mask_ref, score_ref, prob_ref, xo_ref, slot_ref, pslot_ref, chunk_ref,
    ss0, ss1, rs0, rs1, ps0, ps1, gs0, gs1, xs0, xs1, cs0, cs1, ns0, ns1, hid_buf, slope_buf, hs,
):
    dp = lax.axis_index("dp")
    seq = lax.axis_index("seq")
    chip, core = seq // 2, seq % 2
    peers = peers_of(seq)

    def scatter(kind, k):
        to = (dp + k) % n
        return send(pk_ref.at[kind, to], slot_ref.at[kind, k], (ss0, ss1), (kind, k), {"dp": to})

    def small(k):
        return send(pp_ref, pslot_ref.at[k], (ps0, ps1), k, {"dp": (dp + k) % n})

    def gather(kind, k):
        return send(chunk_ref.at[kind], w_ref.at[kind, seq, dp], (rs0, rs1), (kind, k), {"dp": (dp + k) % n})

    def side(kind, which):
        part = peers[2] if which == 2 else seq
        to = peers[2] if which == 0 else peers[1]
        return send(w_ref.at[kind, part], w_ref.at[kind, part], (gs0, gs1), (kind, which), {"seq": to})

    def own(o):
        to = peers[o]
        return send(x_ref.at[3 * (to // 2) + to % 2], xo_ref.at[seq], (xs0, xs1), (o, 0), {"seq": to})

    def shared(o):
        if o == 3:
            there = xo_ref.at[OWN + peers[2]]
            return send(there, there, (xs0, xs1), (3, 1), {"seq": peers[1]})
        to = peers[o]
        return send(x_ref.at[3 * (to // 2) + 2], xo_ref.at[OWN + seq], (xs0, xs1), (o, 1), {"seq": to})

    def target(o):
        to = peers[o]
        return send(c_ref.at[3 * (to // 2) + to % 2], co_ref.at[seq], (cs0, cs1), o, {"seq": to})

    def target_shared(o):
        slot = 4 if o == 2 else 5
        return send(c_ref.at[2 if o == 3 else 5], co_ref.at[slot], (cs0, cs1), 4 + o, {"seq": peers[o]})

    def sum_up(kind):
        total = pk_ref[kind, dp].astype(F32)
        for k in range(1, n):
            scatter(kind, k).wait_recv()
            total = total + slot_ref[kind, k].astype(F32)
        chunk_ref[kind] = total.astype(BF16)
        w_ref[kind, seq, dp] = total.astype(BF16)

    offsets = range(1, n)
    greet(n, dp, [peers[1], peers[2], peers[3]], True)
    for k in offsets:
        scatter(0, k).start()
    for o in (2, 1):
        shared(o).start()
    for o in (2, 3, 1):
        own(o).start()
    for k in offsets:
        small(k).start()
    xo_ref[seq] = x_ref[3 * chip + core]
    xo_ref[OWN + seq] = x_ref[3 * chip + 2]
    co_ref[seq] = c_ref[3 * chip + core]
    pl.when(chip == 0)(lambda: co_ref.__setitem__(4, c_ref[2]))
    set_mask(mask_ref)
    vt_ref[:, HD:, :] = jnp.ones((HEADS, VROWS - HD, ALL * BLK), BF16)
    sum_up(0)
    for k in offsets:
        gather(0, k).start()
    for kind in (1, 2):
        for k in offsets:
            scatter(kind, k).start()
    total = pp_ref[...]
    for k in offsets:
        small(k).wait_recv()
        total = total + pslot_ref[k]
    for row in range(SMALL):
        for part in range(2):
            line = jnp.broadcast_to(total[2 * row + part : 2 * row + part + 1, :], (128, 128))
            small_ref[row * D + part * 128 : row * D + (part + 1) * 128, :] = line.T
    shared(2).wait_recv()
    shared(3).start()
    for o in (2, 3, 1):
        own(o).wait_recv()
    shared(1).wait_recv()
    for k in offsets:
        gather(0, k).wait_recv()
    side(0, 0).start()
    side(0, 1).start()
    for o in (2, 3, 1):
        target(o).start()
    pl.when(chip == 0)(lambda: target_shared(2).start())
    pl.when(chip == 1)(lambda: target_shared(3).start())
    pl.when(chip == 1)(lambda: target_shared(1).start())
    shared(3).wait_recv()

    def begin(j, carry):
        xt = xo_ref[j].T
        xt_ref[j] = xt
        unit_values, _ = standardize(xt.astype(F32))
        a_ref[j] = (unit_values * param(small_ref, 0) + param(small_ref, 1)).astype(BF16)
        return carry

    lax.fori_loop(0, ALL, begin, 0)
    side(0, 0).wait_recv()
    side(0, 2).start()
    side(0, 1).wait_recv()
    side(0, 2).wait_recv()
    for t in range(3):
        wt_ref[t * D : (t + 1) * D, :] = matrix(w_ref, 0, t).T
    for kind in (1, 2):
        sum_up(kind)
        for k in offsets:
            gather(kind, k).start()

    def middle(j, carry):
        project(j, a_ref[j], wt_ref, q_ref, kt_ref, vt_ref, k_ref, v_ref)
        return carry

    lax.fori_loop(0, ALL, middle, 0)

    def progress(i):
        @pl.when(i == 2)
        def _():
            for kind in (1, 2):
                for k in offsets:
                    gather(kind, k).wait_recv()
                side(kind, 0).start()
                side(kind, 1).start()

        @pl.when(i == 5)
        def _():
            for kind in (1, 2):
                side(kind, 0).wait_recv()
                side(kind, 2).start()

    attend(core, q_ref, k_ref, vt_ref, o_ref, log_ref, mask_ref, score_ref, prob_ref, progress)
    wot_ref[...] = matrix(w_ref, 0, 3).T
    for kind in (1, 2):
        side(kind, 1).wait_recv()
        side(kind, 2).wait_recv()
    for c in range(4):
        part = slice(c * D, (c + 1) * D)
        wut_ref[part, :] = matrix(w_ref, 1, c).T
        wdt_ref[:, part] = matrix(w_ref, 2, c).T

    def normal(side):
        there = a2_ref.at[OWN + core if side == 0 else OWN + 3 - core]
        return send(there, there, (ns0, ns1), side, {"seq": peers[1]})

    def store(i):
        slot, u = i % 2, ordered(i)
        return (
            pltpu.make_async_copy(hid_buf.at[slot], hid_ref.at[u], hs.at[0, slot]),
            pltpu.make_async_copy(slope_buf.at[slot], slope_ref.at[u], hs.at[1, slot]),
        )

    def feed(i, carry):
        @pl.when(i == 2)
        def _():
            normal(0).start()
            normal(1).start()

        slot = i % 2

        @pl.when(i >= 2)
        def _():
            for copy in store(i - 2):
                copy.wait()

        u = ordered(i)
        place, base = unit_place(u, core)
        x = xt_ref[base + place].astype(F32)
        r, _, _, m = forward_parts(x, o_ref[u], wot_ref, small_ref)
        r_ref[u] = r
        out = r + param(small_ref, 4)
        for c in range(FF // BLK):
            rows = slice(c * BLK, (c + 1) * BLK)
            e = dot(wut_ref[rows, :], m) + param(small_ref, 5 + c)
            hid, slope = gelu_parts(e)
            hid = hid.astype(BF16)
            hid_buf[slot, rows, :] = hid
            slope_buf[slot, rows, :] = slope.astype(BF16)
            out = out + dot(wdt_ref[:, rows], hid)
        sq_ref[u] = squares_of(out)
        z = out + x
        z_ref[u] = z
        unit_values, _ = standardize(z)
        a2_ref[base + place] = (unit_values * param(small_ref, 0) + param(small_ref, 1)).astype(BF16)
        for copy in store(i):
            copy.start()
        return carry

    lax.fori_loop(0, UNITS, feed, 0)
    for i in (UNITS - 2, UNITS - 1):
        for copy in store(i):
            copy.wait()
    normal(0).wait()
    normal(1).wait()
    for o in (2, 3, 1):
        target(o).wait()
        own(o).wait_send()
        shared(o).wait_send()

    @pl.when(chip == 0)
    def _():
        target_shared(2).wait_send()
        target_shared(3).wait_recv()

    @pl.when(chip == 1)
    def _():
        target_shared(3).wait_send()
        target_shared(1).wait_send()
        target_shared(2).wait_recv()
        target_shared(1).wait_recv()

    for kind in range(3):
        for k in offsets:
            scatter(kind, k).wait_send()
            gather(kind, k).wait_send()
        for which in range(3):
            side(kind, which).wait_send()
    for k in offsets:
        small(k).wait_send()


VM = pl.BlockSpec(memory_space=pltpu.VMEM)
HB = pl.BlockSpec(memory_space=pltpu.HBM)


def shape_of(shape, dtype=BF16):
    return jax.ShapeDtypeStruct(shape, dtype)


KEYS = [
    shape_of((HEADS, HD, ALL * BLK)),
    shape_of((2, ALL, BLK, 128)),
    shape_of((2, ALL, BLK, 128)),
]
ATTEND_SCRATCH = [
    pltpu.VMEM((BLK, BLK), F32),
    pltpu.VMEM((2, OWN, BLK, BLK), F32),
    pltpu.VMEM((2, OWN * BLK, BLK), BF16),
]
BACK_SCRATCH = [
    pltpu.VMEM((BLK, BLK), F32),
    pltpu.VMEM((2, OWN * BLK, BLK), BF16),
    pltpu.VMEM((2, OWN * BLK, BLK), BF16),
    pltpu.VMEM((HEADS, HD, ALL * BLK), F32),
    pltpu.VMEM((HEADS, HD, ALL * BLK), F32),
    pltpu.VMEM((2, OWN, BLK, BLK), BF16),
    pltpu.VMEM((2, 2, BLK, BLK), BF16),
    *pair_of_sems((2, 2)),
]


def stage_call(body, name, args, outs, scratch, mib, flops, hbm_in=(), hbm_out=(), **comm):
    return pl.pallas_call(
        body,
        in_specs=[HB if i in hbm_in else VM for i in range(len(args))],
        out_specs=[HB if i in hbm_out else VM for i in range(len(outs))],
        out_shape=outs,
        scratch_shapes=scratch,
        compiler_params=pltpu.CompilerParams(vmem_limit_bytes=mib << 20, has_side_effects=bool(comm), **comm),
        cost_estimate=cost(flops, 1 << 20),
        name=name,
    )(*args)


def first_stage(n, pk, pp, x, c):
    rows = D // n
    tile, eight = (UNITS, BLK, BLK), (ALL, BLK, BLK)
    outs = [shape_of(eight), shape_of(eight), shape_of(eight)] + KEYS
    outs += [shape_of(tile), shape_of((UNITS, 2, 8, BLK), F32), shape_of(tile, F32)]
    outs += [shape_of((UNITS, FF, BLK)), shape_of((UNITS, FF, BLK)), shape_of(tile, F32), shape_of(eight)]
    outs += [shape_of((UNITS, 8, BLK), F32), shape_of((3 * D, D)), shape_of((D, D)), shape_of((FF, D))]
    outs += [shape_of((D, FF)), shape_of((SMALL * D, 128), F32), shape_of((3, 4, n, rows, D)), shape_of(tile)]
    scratch = [pltpu.VMEM((HEADS, VROWS, ALL * BLK), BF16)] + ATTEND_SCRATCH
    scratch += [
        pltpu.VMEM(eight, BF16),
        pltpu.VMEM((3, n, rows, D), BF16),
        pltpu.VMEM((n, 24, 128), F32),
        pltpu.VMEM((3, rows, D), BF16),
        *pair_of_sems((3, n)),
        *pair_of_sems((3, n)),
        *pair_of_sems((n,)),
        *pair_of_sems((3, 3)),
        *pair_of_sems((4, 2)),
        *pair_of_sems((8,)),
        *pair_of_sems((2,)),
        pltpu.VMEM((2, FF, BLK), BF16),
        pltpu.VMEM((2, FF, BLK), BF16),
        pltpu.SemaphoreType.DMA((2, 2)),
    ]
    return stage_call(
        partial(first_stage_body, n), "first_stage", [pk, pp, x, c], outs, scratch, FIRST_MIB, 8e9, hbm_out=(9, 10),
        collective_id=0,
    )


def feed_back_tail(
    u, g, gy, r_unit, r_inv, m, o, small_ref, parts, w_ref, gr_ref, go_ref, gd_acc, gu_acc, go_acc, tail_acc
):
    tail_acc[2 * D : 3 * D, :] += fold(gy.astype(F32))
    gm = jnp.zeros((D, BLK), F32)
    for c in range(FF // BLK):
        rows = slice(c * BLK, (c + 1) * BLK)
        hid, slope = parts(c)
        gd_acc[rows, :] += dot_nt(hid, gy)
        ge = (dot(matrix(w_ref, 2, c), gy) * slope).astype(BF16)
        gu_acc[:, rows] += dot_nt(m, ge)
        tail_acc[3 * D + c * BLK : 3 * D + (c + 1) * BLK, :] += fold(ge.astype(F32))
        gm = gm + dot(matrix(w_ref, 1, c), ge)
    tail_acc[0:D, :] += fold(gm * r_unit)
    tail_acc[D : 2 * D, :] += fold(gm)
    gr = g + standardize_back(gm * param(small_ref, 2), r_unit, r_inv)
    gr_ref[u] = gr
    ga = gr.astype(BF16)
    go_acc[...] += dot_nt(o, ga)
    go_ref[u] = dot(matrix(w_ref, 0, 3), ga).astype(BF16)


TAIL = 3 * D + FF


def second_stage_body(
    a_ref, z_ref, cot_ref, w_ref, wt_ref, wot_ref, wut_ref, wdt_ref, small_ref,
    final_ref, sq_ref, gr_ref, gd_acc, gu_acc, go_acc, tail_acc, dq_ref, dk_ref, dv_ref,
    q_ref, kt_ref, k_ref, v_ref, vt_ref, o_ref, log_ref, go_ref, score_ref, hid_buf, slope_buf,
    mask_ref, prob_ref, ds_ref, dk_acc, dv_acc, part_ref, got_ref, ds0, ds1,
):
    seq = lax.axis_index("seq")
    core = seq % 2
    peer = peers_of(seq)[1]
    greet(1, 0, [peer], False)
    set_mask(mask_ref)
    vt_ref[:, HD:, :] = jnp.ones((HEADS, VROWS - HD, ALL * BLK), BF16)
    for acc in (gd_acc, gu_acc, go_acc, tail_acc):
        acc[...] = jnp.zeros_like(acc)

    def begin(j, carry):
        project(j, a_ref[j], wt_ref, q_ref, kt_ref, vt_ref, k_ref, v_ref)
        return carry

    lax.fori_loop(0, ALL, begin, 0)
    attend(core, q_ref, k_ref, vt_ref, o_ref, log_ref, mask_ref, score_ref, prob_ref)

    def feed(u, carry):
        r, r_unit, r_inv, m = forward_parts(z_ref[u], o_ref[u], wot_ref, small_ref)
        out = r + param(small_ref, 4)
        for c in range(FF // BLK):
            rows = slice(c * BLK, (c + 1) * BLK)
            e = dot(wut_ref[rows, :], m) + param(small_ref, 5 + c)
            hid, slope = gelu_parts(e)
            hid = hid.astype(BF16)
            hid_buf[rows, :] = hid
            slope_buf[rows, :] = slope
            out = out + dot(wdt_ref[:, rows], hid)
        sq_ref[u] = squares_of(out)
        final_ref[u] = out.T.astype(BF16)
        gy = cot_ref[u].T
        feed_back_tail(
            u, gy.astype(F32), gy, r_unit, r_inv, m, o_ref[u], small_ref,
            lambda c: (hid_buf[c * BLK : (c + 1) * BLK, :], slope_buf[c * BLK : (c + 1) * BLK, :]),
            w_ref, gr_ref, go_ref, gd_acc, gu_acc, go_acc, tail_acc,
        )
        return carry

    lax.fori_loop(0, UNITS, feed, 0)
    attend_back(
        core, q_ref, k_ref, kt_ref, v_ref, go_ref, o_ref, log_ref, dq_ref, dk_ref, dv_ref, mask_ref, prob_ref, ds_ref, dk_acc, dv_acc,
        part_ref, got_ref, ds0, ds1, peer,
    )


def second_stage(a, z, cot, w, wt, wot, wut, wdt, small):
    tile, eight = (UNITS, BLK, BLK), (ALL, BLK, BLK)
    outs = [shape_of(tile), shape_of((UNITS, 8, BLK), F32), shape_of(tile, F32), shape_of((FF, D), F32)]
    outs += [shape_of((D, FF), F32), shape_of((D, D), F32), shape_of((TAIL, 128), F32), shape_of(tile)]
    outs += [shape_of(tile), shape_of(tile)]
    scratch = [pltpu.VMEM(eight, BF16)] + [pltpu.VMEM(s.shape, s.dtype) for s in KEYS]
    scratch += [pltpu.VMEM((HEADS, VROWS, ALL * BLK), BF16), pltpu.VMEM(tile, BF16)]
    scratch += [pltpu.VMEM((UNITS, 2, 8, BLK), F32), pltpu.VMEM(tile, BF16), ATTEND_SCRATCH[1]]
    scratch += [pltpu.VMEM((FF, BLK), BF16), pltpu.VMEM((FF, BLK), F32)] + BACK_SCRATCH
    return stage_call(
        second_stage_body, "second_stage", [a, z, cot, w, wt, wot, wut, wdt, small], outs, scratch, SECOND_MIB, 20e9,
        collective_id=1,
    )


def project_weights(a, dq, dk, dv, gqkv_acc):
    gqkv_acc[0] += dot_nt(a, dq)
    gqkv_acc[1] += dot_nt(a, dk)
    gqkv_acc[2] += dot_nt(a, dv)


def project_back(z, dq, dk, dv, gr, small_ref, w_ref, head_acc):
    grad = dot(matrix(w_ref, 0, 0), dq) + dot(matrix(w_ref, 0, 1), dk) + dot(matrix(w_ref, 0, 2), dv)
    unit_values, inverse = standardize(z)
    head_acc[0:D, :] += fold(grad * unit_values)
    head_acc[D : 2 * D, :] += fold(grad)
    return gr + standardize_back(grad * param(small_ref, 0), unit_values, inverse)


def third_stage_body(
    n, dq_in, dk_in, dv_in, a2_ref, z_ref, gr_in, hid_ref, slope_ref, r_ref, o_ref, log_ref, q_ref, kt_ref, k_ref, v_ref,
    small_ref, w_ref, gd_in, gu_in, go_in, tail_in, a_ref, xt_ref, sq1_ref, sq2_ref, f_ref,
    sum_ref, p_ref, fo_ref, io_ref,
    gz_ref, gr_ref, gd_acc, gu_acc, go_acc, tail_acc, gqkv_acc, head_acc, dq_ref, dk_ref, dv_ref, i_ref,
    g_ref, pp_ref, half_ref, quarter_ref, out_ref, mine_ref, slot_ref, chunk_ref, pslot_ref, psum_ref,
    as0, as1, bs0, bs1, ss0, ss1, rs0, rs1, gs0, gs1, ps0, ps1, xs0, xs1,
    go_ref, hid_buf, slope_buf, hs, mask_ref, prob_ref, ds_ref, dk_acc, dv_acc, part_ref, got_ref, ds0, ds1,
):
    dp = lax.axis_index("dp")
    seq = lax.axis_index("seq")
    chip, core = seq // 2, seq % 2
    peers = peers_of(seq)
    offsets = range(1, n)

    def half(kind, j):
        part = peers[1] if j == 0 else peers[3]
        return send(g_ref.at[kind, part], half_ref.at[kind, j], (as0, as1), (kind, j), {"seq": peers[1]})

    def cross(kind):
        return send(out_ref.at[kind], quarter_ref.at[kind], (bs0, bs1), kind, {"seq": peers[2]})

    def scatter(kind, k):
        to = (dp + k) % n
        return send(mine_ref.at[kind, to], slot_ref.at[kind, k], (ss0, ss1), (kind, k), {"dp": to})

    def gather(kind, k):
        return send(chunk_ref.at[kind], sum_ref.at[kind, seq, dp], (rs0, rs1), (kind, k), {"dp": (dp + k) % n})

    def side(kind, which):
        part = peers[2] if which == 2 else seq
        to = peers[2] if which == 0 else peers[1]
        return send(sum_ref.at[kind, part], sum_ref.at[kind, part], (gs0, gs1), (kind, which), {"seq": to})

    def small(k):
        if k == 0:
            return send(pp_ref, pslot_ref.at[0], (ps0, ps1), 0, {"seq": peers[1]})
        if k == 1:
            return send(psum_ref.at[0], pslot_ref.at[1], (ps0, ps1), 1, {"seq": peers[2]})
        return send(psum_ref.at[1], pslot_ref.at[k], (ps0, ps1), k, {"dp": (dp + k - 1) % n})

    def halves(kind):
        half(kind, 0).start()
        half(kind, 1).start()

    def crossing(kind):
        half(kind, 0).wait_recv()
        half(kind, 1).wait_recv()
        out_ref[kind] = (g_ref[kind, peers[2]].astype(F32) + half_ref[kind, 1].astype(F32)).astype(BF16)
        cross(kind).start()

    def scattering(kind):
        cross(kind).wait_recv()
        mine_ref[kind] = (
            g_ref[kind, seq].astype(F32) + half_ref[kind, 0].astype(F32) + quarter_ref[kind].astype(F32)
        ).astype(BF16)
        for k in offsets:
            scatter(kind, k).start()

    def gathering(kind):
        total = mine_ref[kind, dp].astype(F32)
        for k in offsets:
            scatter(kind, k).wait_recv()
            total = total + slot_ref[kind, k].astype(F32)
        chunk_ref[kind] = total.astype(BF16)
        sum_ref[kind, seq, dp] = total.astype(BF16)
        for k in offsets:
            gather(kind, k).start()

    def sharing(kind):
        for k in offsets:
            gather(kind, k).wait_recv()
        side(kind, 0).start()
        side(kind, 1).start()

    def passing(kind):
        side(kind, 0).wait_recv()
        side(kind, 2).start()

    def settled(kind):
        side(kind, 1).wait_recv()
        side(kind, 2).wait_recv()

    own = 3 * chip + core

    def move(which, o, source_ref, target_ref):
        return send(source_ref.at[peers[o]], target_ref.at[own], (xs0, xs1), (which, o), {"seq": peers[o]})

    def move_shared(which, o, source_ref, target_ref):
        source = source_ref.at[4 if o == 2 else 5]
        return send(source, target_ref.at[2 if o == 3 else 5], (xs0, xs1), (which, 4 + o), {"seq": peers[o]})

    def start_moves(which, source_ref, target_ref):
        pl.when(chip == 0)(lambda: move_shared(which, 3, source_ref, target_ref).start())
        pl.when(chip == 1)(lambda: move_shared(which, 2, source_ref, target_ref).start())
        pl.when(chip == 1)(lambda: move_shared(which, 1, source_ref, target_ref).start())
        for o in (2, 3, 1):
            move(which, o, source_ref, target_ref).start()
        target_ref[own] = source_ref[seq]
        pl.when(chip == 0)(lambda: target_ref.__setitem__(2, source_ref[4]))

    def finish_moves(which, source_ref, target_ref):
        @pl.when(chip == 0)
        def _():
            move_shared(which, 3, source_ref, target_ref).wait_send()
            move_shared(which, 2, source_ref, target_ref).wait_recv()

        @pl.when(chip == 1)
        def _():
            move_shared(which, 2, source_ref, target_ref).wait_send()
            move_shared(which, 1, source_ref, target_ref).wait()
            move_shared(which, 3, source_ref, target_ref).wait_recv()

        for o in (2, 3, 1):
            move(which, o, source_ref, target_ref).wait()

    def fetch(u):
        slot = u % 2
        return (
            pltpu.make_async_copy(hid_ref.at[u], hid_buf.at[slot], hs.at[0, slot]),
            pltpu.make_async_copy(slope_ref.at[u], slope_buf.at[slot], hs.at[1, slot]),
        )

    split = lambda values: values.astype(BF16).reshape(g_ref.shape[2:])
    for copy in fetch(0):
        copy.start()
    greet(n, dp, [peers[1], peers[2], peers[3]], True)
    start_moves(0, f_ref, fo_ref)
    set_mask(mask_ref)
    gqkv_acc[...] = jnp.zeros_like(gqkv_acc)
    head_acc[...] = jnp.zeros_like(head_acc)
    for acc, given in ((gd_acc, gd_in), (gu_acc, gu_in), (go_acc, go_in), (tail_acc, tail_in)):
        acc[...] = given[...]

    def feed(u, carry):
        @pl.when(u < UNITS - 1)
        def _():
            for copy in fetch(u + 1):
                copy.start()

        for copy in fetch(u):
            copy.wait()
        slot = u % 2
        place, base = unit_place(u, core)
        project_weights(a2_ref[base + place], dq_in[u], dk_in[u], dv_in[u], gqkv_acc)
        g = project_back(z_ref[u], dq_in[u], dk_in[u], dv_in[u], gr_in[u], small_ref, w_ref, head_acc)
        gz_ref[u] = g
        r_unit, r_inv = standardize(r_ref[u])
        m = (r_unit * param(small_ref, 2) + param(small_ref, 3)).astype(BF16)
        feed_back_tail(
            u, g, g.astype(BF16), r_unit, r_inv, m, o_ref[u], small_ref,
            lambda c: (
                hid_buf[slot, c * BLK : (c + 1) * BLK, :],
                slope_buf[slot, c * BLK : (c + 1) * BLK, :].astype(F32),
            ),
            w_ref, gr_ref, go_ref, gd_acc, gu_acc, go_acc, tail_acc,
        )
        return carry

    lax.fori_loop(0, UNITS, feed, 0)
    for c in range(4):
        g_ref[1, c] = split(gu_acc[:, c * D : (c + 1) * D])
        g_ref[2, c] = split(gd_acc[c * D : (c + 1) * D, :])
    halves(1)
    halves(2)

    def progress(i):
        @pl.when(i == 1)
        def _():
            crossing(1)
            crossing(2)

        pl.when(i == 4)(lambda: scattering(1))
        pl.when(i == 5)(lambda: scattering(2))

    attend_back(
        core, q_ref, k_ref, kt_ref, v_ref, go_ref, o_ref, log_ref, dq_ref, dk_ref, dv_ref, mask_ref, prob_ref, ds_ref, dk_acc, dv_acc,
        part_ref, got_ref, ds0, ds1, peers[1], progress,
    )
    gathering(1)
    gathering(2)

    def early(u, carry):
        place, base = unit_place(u, core)
        project_weights(a_ref[base + place], dq_ref[u], dk_ref[u], dv_ref[u], gqkv_acc)
        return carry

    lax.fori_loop(0, UNITS, early, 0)
    for t in range(3):
        g_ref[0, t] = split(gqkv_acc[t])
    g_ref[0, 3] = split(go_acc[...])
    halves(0)

    def end(u, carry):
        pl.when(u == 1)(lambda: crossing(0))
        pl.when(u == 4)(lambda: sharing(1))
        place, base = unit_place(u, core)
        g = project_back(
            xt_ref[base + place].astype(F32), dq_ref[u], dk_ref[u], dv_ref[u], gr_ref[u], small_ref, w_ref, head_acc
        )
        i_ref[u] = (g + gz_ref[u]).T.astype(BF16)
        return carry

    lax.fori_loop(0, UNITS, end, 0)
    start_moves(1, i_ref, io_ref)
    for row in range(SMALL):
        for part in range(2):
            ref, first = (head_acc, row) if row < 2 else (tail_acc, row - 2)
            first = first * D + part * 128
            pp_ref[2 * row + part : 2 * row + part + 1, :] = jnp.sum(ref[first : first + 128, :].T, axis=0, keepdims=True)
    sequences = 6 * n
    place = lax.broadcasted_iota(jnp.int32, (6, 128), 0) * 128 + lax.broadcasted_iota(jnp.int32, (6, 128), 1)
    stats = jnp.zeros((6, 128), F32)
    for i, ref in enumerate((sq1_ref, sq2_ref)):
        lines = [jnp.sum(ref[u], axis=0, keepdims=True) for u in range(UNITS)]
        mine = jnp.sum(lines[0] + lines[1] + lines[2] + lines[3], axis=1, keepdims=True)
        shared = jnp.sum(lines[4] + lines[5], axis=1, keepdims=True)
        start = i * sequences + 6 * dp + 3 * chip
        stats = jnp.where(place == start + core, jnp.broadcast_to(mine, (6, 128)), stats)
        stats = jnp.where(place == start + 2, jnp.broadcast_to(shared, (6, 128)), stats)
    pp_ref[18:24, :] = stats
    small(0).start()
    scattering(0)
    small(0).wait_recv()
    psum_ref[0] = pp_ref[...] + pslot_ref[0]
    small(1).start()
    small(1).wait_recv()
    psum_ref[1] = psum_ref[0] + pslot_ref[1]
    for k in offsets:
        small(1 + k).start()
    sharing(2)
    gathering(0)
    passing(1)
    passing(2)
    total = psum_ref[1]
    for k in offsets:
        small(1 + k).wait_recv()
        total = total + pslot_ref[1 + k]
    p_ref[...] = total
    sharing(0)
    settled(1)
    settled(2)
    passing(0)
    settled(0)
    finish_moves(0, f_ref, fo_ref)
    finish_moves(1, i_ref, io_ref)
    for kind in range(3):
        half(kind, 0).wait_send()
        half(kind, 1).wait_send()
        cross(kind).wait_send()
        for k in offsets:
            scatter(kind, k).wait_send()
            gather(kind, k).wait_send()
        for which in range(3):
            side(kind, which).wait_send()
    for k in range(n + 1):
        small(k).wait_send()


def third_stage(n, *args):
    rows = D // n
    tile = (UNITS, BLK, BLK)
    quarter = (3, n, rows, D)
    outs = [shape_of((3, 4, n, rows, D)), shape_of((24, 128), F32), shape_of(tile), shape_of(tile)]
    scratch = [
        pltpu.VMEM(tile, F32),
        pltpu.VMEM(tile, F32),
        pltpu.VMEM((FF, D), F32),
        pltpu.VMEM((D, FF), F32),
        pltpu.VMEM((D, D), F32),
        pltpu.VMEM((TAIL, 128), F32),
        pltpu.VMEM((3, D, D), F32),
        pltpu.VMEM((2 * D, 128), F32),
        pltpu.VMEM(tile, BF16),
        pltpu.VMEM(tile, BF16),
        pltpu.VMEM(tile, BF16),
        pltpu.VMEM(tile, BF16),
        pltpu.VMEM((3, 4, n, rows, D), BF16),
        pltpu.VMEM((24, 128), F32),
        pltpu.VMEM((3, 2, n, rows, D), BF16),
        pltpu.VMEM(quarter, BF16),
        pltpu.VMEM(quarter, BF16),
        pltpu.VMEM(quarter, BF16),
        pltpu.VMEM(quarter, BF16),
        pltpu.VMEM((3, rows, D), BF16),
        pltpu.VMEM((1 + n, 24, 128), F32),
        pltpu.VMEM((2, 24, 128), F32),
        *pair_of_sems((3, 2)),
        *pair_of_sems((3,)),
        *pair_of_sems((3, n)),
        *pair_of_sems((3, n)),
        *pair_of_sems((3, 3)),
        *pair_of_sems((1 + n,)),
        *pair_of_sems((2, 8)),
        pltpu.VMEM(tile, BF16),
        pltpu.VMEM((2, FF, BLK), BF16),
        pltpu.VMEM((2, FF, BLK), BF16),
        pltpu.SemaphoreType.DMA((2, 2)),
        *BACK_SCRATCH,
    ]
    return stage_call(
        partial(third_stage_body, n), "third_stage", args, outs, scratch, THIRD_MIB, 20e9, hbm_in=(6, 7), collective_id=2
    )


FIRST_MIB, SECOND_MIB, THIRD_MIB, ADAM_MIB = 38, 22, 31, 58


def owner_scalars(owner_ref):
    sizes = [D * D] * 4 + [D * FF, FF * D, SMALL * D]
    starts = []
    for t in range(7):
        offset = jnp.int32(0)
        for u in range(t):
            offset = offset + jnp.where(owner_ref[u] == owner_ref[t], sizes[u], 0).astype(jnp.int32)
        starts.append(offset)
    return starts


def pack_body(owner_ref, row_ref, w_ref, p_ref):
    dp = lax.axis_index("dp")
    seq = lax.axis_index("seq")
    starts = owner_scalars(owner_ref)
    square = jnp.where(seq == 0, starts[0], jnp.where(seq == 1, starts[1], jnp.where(seq == 2, starts[2], starts[3])))
    plans = (
        (owner_ref[seq], square // 128, 2),
        (owner_ref[4], starts[4] // 128 + 2 * seq, FF // 128),
        (owner_ref[5], starts[5] // 128 + 2 * D * seq, 2),
    )
    for kind, (owner, base, stride) in enumerate(plans):
        keep = jnp.where(owner == dp, 1.0, 0.0).astype(F32)
        for side in range(2):
            values = row_ref[pl.ds(base + side, D, stride=stride), :]
            w_ref[kind, :, side * 128 : (side + 1) * 128] = (values * keep).astype(BF16)
    keep = jnp.where(owner_ref[6] == dp, 1.0, 0.0).astype(F32)
    values = row_ref[pl.ds(pl.multiple_of(starts[6] // 128, 8), 24), :] * keep
    rows = lax.broadcasted_iota(jnp.int32, (24, 128), 0)
    p_ref[...] = jnp.where(rows < 2 * SMALL, values, 0.0)


def pack(owner_list, row):
    return pl.pallas_call(
        pack_body,
        in_specs=[pl.BlockSpec(memory_space=pltpu.SMEM), pl.BlockSpec(memory_space=pltpu.VMEM)],
        out_specs=[pl.BlockSpec(memory_space=pltpu.VMEM)] * 2,
        out_shape=[jax.ShapeDtypeStruct((3, D, D), BF16), jax.ShapeDtypeStruct((24, 128), F32)],
        compiler_params=pltpu.CompilerParams(vmem_limit_bytes=20 << 20),
        cost_estimate=cost(1, 3 << 20),
        name="pack",
    )(owner_list, row)


ROWS = D * D // 128


def adam_body(owner_ref, g_ref, p_ref, f_ref, i_ref, m_ref, v_ref, w_ref, m_out, v_out, w_out, f_out, i_out, grad_ref):
    dp = lax.axis_index("dp")
    block = pl.program_id(0)
    starts = owner_scalars(owner_ref)
    counts = [1, 1, 1, 1, 4, 4, 1]
    rate = jnp.float32(D ** (-0.5))
    decay = jnp.float32(0.1)
    limit = jnp.int32(0)
    f_out[...] = f_ref[...].astype(F32)
    i_out[...] = i_ref[...].astype(F32)
    for t in range(7):
        first = starts[t] // (D * D)
        here = (owner_ref[t] == dp) & (block >= first) & (block < first + counts[t])
        part = block - first
        limit = jnp.where(here, 2 * SMALL if t == 6 else ROWS, limit)
        if t == 5:
            rate = jnp.where(here, FF ** (-0.5), rate)
        if t == 6:
            rate = jnp.where(here, 0.5, rate)
            decay = jnp.where(here, 0.0, decay)

        @pl.when(here)
        def _(t=t, part=part):
            if t == 6:
                grad_ref[0:24, :] = p_ref[...]
            elif t == 4:
                for c in range(4):
                    piece = g_ref[4 + c, pl.ds(pl.multiple_of(part * 64, 64), 64), :].astype(F32)
                    for side in range(2):
                        grad_ref[pl.ds(2 * c + side, 64, stride=8), :] = piece[:, side * 128 : (side + 1) * 128]
            else:
                for r in range(4):
                    piece = g_ref[8 + part if t == 5 else t, r * 64 : (r + 1) * 64, :].astype(F32)
                    for side in range(2):
                        grad_ref[pl.ds(r * 128 + side, 64, stride=2), :] = piece[:, side * 128 : (side + 1) * 128]

    @pl.when(limit == 0)
    def _():
        for out in (m_out, v_out, w_out):
            out[...] = jnp.zeros_like(out)

    @pl.when(limit > 0)
    def _():
        scale = 1.0 / (1.0 - 0.5**STEP)
        for r in range(0, ROWS, PIECE):
            rows = slice(r, r + PIECE)
            grad = grad_ref[rows, :]
            valid = lax.broadcasted_iota(jnp.int32, (PIECE, 128), 0) + r < limit
            first_new = 0.5 * m_ref[rows, :] + 0.5 * grad
            second_new = 0.5 * v_ref[rows, :] + 0.5 * grad * grad
            old = w_ref[rows, :]
            update = first_new * scale / (jnp.sqrt(second_new * scale) + adam_eps) + decay * old
            m_out[rows, :] = jnp.where(valid, first_new, 0.0)
            v_out[rows, :] = jnp.where(valid, second_new, 0.0)
            w_out[rows, :] = jnp.where(valid, old - rate * update, 0.0)


PIECE = 64


def adam(owner_list, g, p, f, i, m, v, w):
    blocks = m.shape[0] // ROWS
    tile = pl.BlockSpec((ROWS, 128), lambda b, t: (b, 0))
    states = pl.BlockSpec((f.shape[0] // blocks, D), lambda b, t: (b, 0))
    out = jax.ShapeDtypeStruct(m.shape, F32)
    state = jax.ShapeDtypeStruct(f.shape, F32)
    whole = pl.BlockSpec(memory_space=pltpu.VMEM)
    spec = pltpu.PrefetchScalarGridSpec(
        num_scalar_prefetch=1,
        grid=(blocks,),
        in_specs=[whole, whole, states, states, tile, tile, tile],
        out_specs=[tile, tile, tile, states, states],
        scratch_shapes=[pltpu.VMEM((ROWS, 128), F32)],
    )
    return pl.pallas_call(
        adam_body,
        grid_spec=spec,
        out_shape=[out, out, out, state, state],
        compiler_params=params_of(mib=ADAM_MIB),
        cost_estimate=cost(20 * 524288, 14 << 20),
        name="adam",
    )(owner_list, g, p, f, i, m, v, w)


def per_device(inputs, cotangent, owner_list, master_rows, moment1_rows, moment2_rows):
    n = lax.axis_size("dp")
    rows = D // n
    flat = [r.reshape(-1, 128) for r in (master_rows, moment1_rows, moment2_rows)]
    pk, pp = pack(owner_list, flat[0])
    (xt, a1, q1, kt1, k1, v1, o1, log1, r1, hid, slope, z2, a2, sq1, wt, wot, wut, wdt, small, w, cot) = first_stage(
        n, pk.reshape(3, n, rows, D), pp, inputs, cotangent
    )
    final, sq2, gr, gd, gu, gout, tail, dq, dk, dv = second_stage(a2, z2, cot, w, wt, wot, wut, wdt, small)
    g, p, final, grad = third_stage(
        n, dq, dk, dv, a2, z2, gr, hid, slope, r1, o1, log1, q1, kt1, k1, v1, small, w, gd, gu, gout, tail,
        a1, xt, sq1, sq2, final,
    )
    states = [r.reshape(-1, D) for r in (final, grad)]
    m_new, v_new, w_new, final, grad = adam(owner_list, g.reshape(12, D, D), p, *states, flat[1], flat[2], flat[0])
    sequences = inputs.shape[0] * n
    entries = inputs.shape[1] * lax.axis_size("seq") * D
    squares = p[18:].reshape(-1)[: 2 * sequences].reshape(2, sequences)
    stats = jnp.sqrt(squares / entries + stat_eps)
    back = lambda r: r.reshape(master_rows.shape)
    return (final.reshape(inputs.shape), grad.reshape(inputs.shape), stats, back(m_new), back(v_new), back(w_new))


def solution(mesh):
    placed = (P("dp", "seq", None), P("dp", "seq", None), P(), P("dp", None), P("dp", None), P("dp", None))
    return jax.shard_map(
        per_device,
        mesh=mesh,
        in_specs=placed,
        out_specs=(P("dp", "seq", None), P("dp", "seq", None), P(), P("dp", None), P("dp", None), P("dp", None)),
        check_vma=False,
    )
```

```python
import math
from functools import partial

import jax
import jax.numpy as jnp
from jax import lax
from jax.experimental import pallas as pl
from jax.experimental.pallas import tpu as pltpu
from jax.sharding import PartitionSpec as P

D = 256
HEADS = 4
HD = 64
FF = 1024
STEP = 3
SMALL = 9
BLK = 256
OWN = 4
UNITS = 6
ALL = 8
F32 = jnp.float32
BF16 = jnp.bfloat16
MESH = pl.DeviceIdType.MESH

norm_eps = 1e-05
stat_eps = 1e-06
adam_eps = 1e-08
masked_score = -1e30


def dot(left, right):
    return lax.dot_general(left, right, (((1,), (0,)), ((), ())), preferred_element_type=F32)


def dot_nt(left, right):
    return lax.dot_general(left, right, (((1,), (1,)), ((), ())), preferred_element_type=F32)


def wide(column):
    return jnp.concatenate([column, column], axis=1)


def fold(values):
    return values[:, :128] + values[:, 128:]


def standardize(values):
    average = jnp.mean(values, axis=0, keepdims=True)
    centered = values - average
    spread = jnp.mean(centered * centered, axis=0, keepdims=True)
    inverse = lax.rsqrt(spread + norm_eps)
    return centered * inverse, inverse


def standardize_back(grad, unit_values, inverse):
    average = jnp.mean(grad, axis=0, keepdims=True)
    inner = jnp.mean(grad * unit_values, axis=0, keepdims=True)
    return (grad - average - unit_values * inner) * inverse


def param(small_ref, row):
    return wide(small_ref[row * D : (row + 1) * D, :])


def gelu_parts(e):
    cdf = 0.5 * lax.erf(e * math.sqrt(0.5)) + 0.5
    hid = e * cdf
    slope = cdf + e * (jnp.exp(-0.5 * e * e) * (1.0 / math.sqrt(2.0 * math.pi)))
    return hid, slope


def full(shape):
    return pl.BlockSpec(shape, lambda *args: (0,) * len(shape), pipeline_mode=pl.Buffered(1))


def params_of(ndims=1, mib=56):
    return pltpu.CompilerParams(
        dimension_semantics=("arbitrary",) * ndims, vmem_limit_bytes=mib << 20
    )


def cost(flops, nbytes, trans=0):
    return pl.CostEstimate(flops=int(flops), bytes_accessed=int(nbytes), transcendentals=int(trans))


LOG2E = math.log2(math.e)
VROWS = HD + 16


def unit_place(unit, core):
    later = unit // OWN
    place = (1 - later) * unit + later * (core + (unit - OWN) * (3 - 2 * core))
    return place, later * OWN


def lanes(start, size):
    return pl.ds(pl.multiple_of(start, BLK), size)


def pair_rows(pair):
    return pl.ds(pl.multiple_of(pair * 128, 128), 128)


def matrix(w_ref, kind, part):
    n, rows = w_ref.shape[2:4]
    if rows % 16 == 0:
        return w_ref[kind, part].reshape(D, D)
    return jnp.concatenate([w_ref[kind, part, i] for i in range(n)], axis=0)


def peers_of(seq):
    return {1: seq + 1 - 2 * (seq % 2), 2: (seq + 2) % 4, 3: 3 - seq}


def greet(n, dp, peers, wide_group):
    barrier = pltpu.get_barrier_semaphore()
    count = 0
    for peer in peers:
        pl.semaphore_signal(barrier, inc=1, device_id={"seq": peer}, device_id_type=MESH)
        count += 1
    if wide_group:
        for k in range(1, n):
            pl.semaphore_signal(barrier, inc=1, device_id={"dp": (dp + k) % n}, device_id_type=MESH)
            count += 1
    pl.semaphore_wait(barrier, count)


def send(source, target, sems, index, device):
    return pltpu.make_async_remote_copy(
        src_ref=source,
        dst_ref=target,
        send_sem=sems[0].at[index],
        recv_sem=sems[1].at[index],
        device_id=device,
        device_id_type=MESH,
    )


def pair_of_sems(shape):
    return [pltpu.SemaphoreType.DMA(shape), pltpu.SemaphoreType.DMA(shape)]


def project(j, a, wt_ref, q_ref, kt_ref, vt_ref, k_ref, v_ref):
    where = lanes(j * BLK, BLK)
    q_ref[j] = (dot(wt_ref[0:D], a) * HD ** (-0.5)).astype(BF16)
    kt = dot(wt_ref[D : 2 * D], a).astype(BF16)
    vt = dot(wt_ref[2 * D : 3 * D], a).astype(BF16)
    for h in range(HEADS):
        kt_ref[h, :, where] = kt[h * HD : (h + 1) * HD]
        vt_ref[h, 0:HD, where] = vt[h * HD : (h + 1) * HD]
    k = kt.T
    v = vt.T
    for h in range(2):
        k_ref[h, j] = k[:, h * 128 : (h + 1) * 128]
        v_ref[h, j] = v[:, h * 128 : (h + 1) * 128]


def head_rows(values, half):
    rows = lax.broadcasted_iota(jnp.int32, values.shape, 0)
    keep = (rows < HD) if half == 0 else (rows >= HD)
    return jnp.where(keep, values, jnp.zeros_like(values))


def set_mask(mask_ref):
    keys = lax.broadcasted_iota(jnp.int32, (BLK, BLK), 0)
    queries = lax.broadcasted_iota(jnp.int32, (BLK, BLK), 1)
    mask_ref[...] = jnp.where(keys <= queries, 0.0, masked_score)


def groups(values, op):
    out = values[0:8]
    for i in range(1, values.shape[0] // 8):
        out = op(out, values[i * 8 : (i + 1) * 8])
    return out


SUB = 128
BSUB = 256


def ordered(i):
    return (i + OWN) % UNITS


def attend(core, q_ref, k_ref, vt_ref, o_ref, log_ref, mask_ref, score_ref, prob_ref, progress=None):
    def step(i, carry):
        if progress is not None:
            progress(i)
        unit = ordered(i)
        place, base = unit_place(unit, core)

        def branch(last):
            keys = (last + 1) * BLK
            chunks = [(kb, sub) for kb in range(last + 1) for sub in range(BLK // SUB)]
            queries = [head_rows(q_ref[base + place, (h // 2) * 128 : (h // 2 + 1) * 128, :], h % 2) for h in range(HEADS)]
            tops = [None] * HEADS
            outs = [None] * HEADS

            def scores(h, kb, sub):
                rows = slice(sub * SUB, (sub + 1) * SUB)
                score = dot(k_ref[h // 2, base + kb, rows, :], queries[h])
                if kb == last:
                    score = score + mask_ref[rows, :]
                score_ref[h % 2, kb, rows, :] = score
                peak = groups(score, jnp.maximum)
                tops[h] = peak if tops[h] is None else jnp.maximum(tops[h], peak)

            def weights(h, kb, sub):
                rows = slice(sub * SUB, (sub + 1) * SUB)
                weight = jnp.exp(score_ref[h % 2, kb, rows, :] - tops[h])
                prob_ref[h % 2, kb * BLK + sub * SUB : kb * BLK + (sub + 1) * SUB, :] = weight.astype(BF16)

            def mixed(h, kb):
                part = dot(vt_ref[h, :, lanes((base + kb) * BLK, BLK)], prob_ref[h % 2, kb * BLK : (kb + 1) * BLK, :])
                outs[h] = part if outs[h] is None else outs[h] + part

            for t in range(HEADS + 2):
                if 0 <= t - 1 < HEADS:
                    tops[t - 1] = jnp.max(tops[t - 1], axis=0, keepdims=True)
                for kb, sub in chunks:
                    if t < HEADS:
                        scores(t, kb, sub)
                    if 0 <= t - 1 < HEADS:
                        weights(t - 1, kb, sub)
                    if 0 <= t - 2 < HEADS and sub == 0:
                        mixed(t - 2, kb)
                if 0 <= t - 2 < HEADS:
                    h = t - 2
                    total = outs[h][HD : HD + 1]
                    o_ref[unit, h * HD : (h + 1) * HD, :] = (outs[h][0:HD] / total).astype(BF16)
                    log_ref[unit, h // 2, h % 2 : h % 2 + 1, :] = tops[h] + jnp.log(total)

        for last in range(OWN):
            pl.when(place == last)(partial(branch, last))
        return carry

    lax.fori_loop(0, UNITS, step, 0)


def attend_back(
    core, q_ref, k_ref, kt_ref, v_ref, go_ref, o_ref, log_ref, dq_ref, dk_ref, dv_ref, mask_ref, prob_ref, slope_ref, dk_acc, dv_acc,
    part_ref, got_ref, ds0, ds1, peer, progress=None,
):
    dk_acc[...] = jnp.zeros_like(dk_acc)
    dv_acc[...] = jnp.zeros_like(dv_acc)
    pairs = ((0, dk_acc, dk_ref), (1, dv_acc, dv_ref))

    def piece(acc, j):
        return acc[:, :, j * BLK : (j + 1) * BLK].reshape(D, BLK)

    def swap(which, side):
        position = 1 - core if side == 0 else 2 + core
        return send(part_ref.at[which, position], got_ref.at[which, side], (ds0, ds1), (which, side), {"seq": peer})

    def step(i, carry):
        @pl.when(i == 2)
        def _():
            for which, acc, _ in pairs:
                for position in range(OWN):
                    part_ref[which, position] = piece(acc, OWN + position).astype(BF16)
            for which in range(2):
                for side in range(2):
                    swap(which, side).start()

        if progress is not None:
            progress(i)
        unit = ordered(i)
        place, base = unit_place(unit, core)

        def branch(last):
            chunks = [(kb, sub) for kb in range(last + 1) for sub in range(BLK // BSUB)]
            heads = []
            for h in range(HEADS):
                pair = slice((h // 2) * 128, (h // 2 + 1) * 128)
                block = q_ref[base + place, pair, :]
                go_block = go_ref[unit, pair, :]
                mine = slice((h % 2) * HD, (h % 2 + 1) * HD)
                inner = jnp.sum(
                    go_block[mine].astype(F32) * o_ref[unit, h * HD : (h + 1) * HD, :].astype(F32), axis=0, keepdims=True
                )
                heads.append(
                    (head_rows(block, h % 2), head_rows(go_block, h % 2), log_ref[unit, h // 2, h % 2 : h % 2 + 1, :], inner)
                )
            dqs = [None] * HEADS
            ready = {}

            def products(h, kb, sub):
                rows = slice(sub * BSUB, (sub + 1) * BSUB)
                q, go, _, _ = heads[h]
                ready[h, kb, sub] = (
                    dot(k_ref[h // 2, base + kb, rows, :], q),
                    dot(v_ref[h // 2, base + kb, rows, :], go),
                )

            def elements(h, kb, sub):
                rows = slice(sub * BSUB, (sub + 1) * BSUB)
                to = slice(kb * BLK + sub * BSUB, kb * BLK + (sub + 1) * BSUB)
                _, _, log_total, inner = heads[h]
                score, slope = ready.pop((h, kb, sub))
                if kb == last:
                    score = score + mask_ref[rows, :]
                weight = jnp.exp(score - log_total)
                prob_ref[h % 2, to, :] = weight.astype(BF16)
                slope_ref[h % 2, to, :] = (weight * (slope - inner)).astype(BF16)

            def gradients(h, kb, which):
                rows = slice(kb * BLK, (kb + 1) * BLK)
                where = lanes((base + kb) * BLK, BLK)
                head = slice(h * HD, (h + 1) * HD)
                if which == 0:
                    dv_acc[h, :, where] += dot_nt(go_ref[unit, head, :], prob_ref[h % 2, rows, :])
                elif which == 1:
                    dk_acc[h, :, where] += dot_nt(q_ref[base + place, head, :], slope_ref[h % 2, rows, :])
                else:
                    part = dot(kt_ref[h, :, where], slope_ref[h % 2, rows, :])
                    dqs[h] = part if dqs[h] is None else dqs[h] + part

            work = [(h, kb, sub) for h in range(HEADS) for kb, sub in chunks]
            per = BLK // BSUB
            products(*work[0])
            for at, (h, kb, sub) in enumerate(work):
                if at + 1 < len(work):
                    products(*work[at + 1])
                elements(h, kb, sub)
                if h > 0 and sub == 0:
                    for which in range(3):
                        gradients(h - 1, kb, which)
                if h > 0 and kb == last and sub == per - 1:
                    dq_ref[unit, (h - 1) * HD : h * HD, :] = (dqs[h - 1] * HD ** (-0.5)).astype(BF16)
            for kb in range(last + 1):
                for which in range(3):
                    gradients(HEADS - 1, kb, which)
            dq_ref[unit, (HEADS - 1) * HD :, :] = (dqs[HEADS - 1] * HD ** (-0.5)).astype(BF16)

        for last in range(OWN):
            pl.when(place == last)(partial(branch, last))
        return carry

    lax.fori_loop(0, UNITS, step, 0)
    for which, acc, ref in pairs:
        for j in range(OWN):
            ref[j] = piece(acc, j).astype(BF16)
    for which, acc, ref in pairs:
        for side, position in enumerate((core, 3 - core)):
            swap(which, side).wait()
            ref[OWN + side] = (part_ref[which, position].astype(F32) + got_ref[which, side].astype(F32)).astype(BF16)


def forward_parts(z, o, wot_ref, small_ref):
    r = z + dot(wot_ref[...], o)
    unit_values, inverse = standardize(r)
    m = (unit_values * param(small_ref, 2) + param(small_ref, 3)).astype(BF16)
    return r, unit_values, inverse, m


def squares_of(out):
    return groups(out * out, jnp.add)


def first_stage_body(
    n, pk_ref, pp_ref, x_ref, c_ref,
    xt_ref, a_ref, q_ref, kt_ref, k_ref, v_ref, o_ref, log_ref, r_ref, hid_ref, slope_ref, z_ref, a2_ref, sq_ref,
    wt_ref, wot_ref, wut_ref, wdt_ref, small_ref, w_ref, co_ref,
    vt_ref, mask_ref, score_ref, prob_ref, xo_ref, slot_ref, pslot_ref, chunk_ref,
    ss0, ss1, rs0, rs1, ps0, ps1, gs0, gs1, xs0, xs1, cs0, cs1, ns0, ns1, hid_buf, slope_buf, hs, ls,
):
    dp = lax.axis_index("dp")
    seq = lax.axis_index("seq")
    chip, core = seq // 2, seq % 2
    peers = peers_of(seq)

    def scatter(kind, k):
        to = (dp + k) % n
        return send(pk_ref.at[kind, to], slot_ref.at[kind, k], (ss0, ss1), (kind, k), {"dp": to})

    def small(k):
        return send(pp_ref, pslot_ref.at[k], (ps0, ps1), k, {"dp": (dp + k) % n})

    def gather(kind, k):
        return send(chunk_ref.at[kind], w_ref.at[kind, seq, dp], (rs0, rs1), (kind, k), {"dp": (dp + k) % n})

    def side(kind, which):
        part = peers[2] if which == 2 else seq
        to = peers[2] if which == 0 else peers[1]
        return send(w_ref.at[kind, part], w_ref.at[kind, part], (gs0, gs1), (kind, which), {"seq": to})

    def own(o):
        to = peers[o]
        return send(x_ref.at[3 * (to // 2) + to % 2], xo_ref.at[seq], (xs0, xs1), (o, 0), {"seq": to})

    def shared(o):
        if o == 3:
            there = xo_ref.at[OWN + peers[2]]
            return send(there, there, (xs0, xs1), (3, 1), {"seq": peers[1]})
        to = peers[o]
        return send(x_ref.at[3 * (to // 2) + 2], xo_ref.at[OWN + seq], (xs0, xs1), (o, 1), {"seq": to})

    def target(o):
        to = peers[o]
        return send(c_ref.at[3 * (to // 2) + to % 2], co_ref.at[seq], (cs0, cs1), o, {"seq": to})

    def target_shared(o):
        slot = 4 if o == 2 else 5
        return send(c_ref.at[2 if o == 3 else 5], co_ref.at[slot], (cs0, cs1), 4 + o, {"seq": peers[o]})

    def sum_up(kind):
        total = pk_ref[kind, dp].astype(F32)
        for k in range(1, n):
            scatter(kind, k).wait_recv()
            total = total + slot_ref[kind, k].astype(F32)
        chunk_ref[kind] = total.astype(BF16)
        w_ref[kind, seq, dp] = total.astype(BF16)

    def kept():
        return pltpu.make_async_copy(c_ref.at[2], co_ref.at[4], ls.at[3])

    locals_ = (
        pltpu.make_async_copy(x_ref.at[3 * chip + core], xo_ref.at[seq], ls.at[0]),
        pltpu.make_async_copy(x_ref.at[3 * chip + 2], xo_ref.at[OWN + seq], ls.at[1]),
        pltpu.make_async_copy(c_ref.at[3 * chip + core], co_ref.at[seq], ls.at[2]),
    )
    offsets = range(1, n)

    def summed(kind):
        sum_up(kind)
        for k in offsets:
            gather(kind, k).start()

    def sharing(kind):
        for k in offsets:
            gather(kind, k).wait_recv()
        side(kind, 0).start()
        side(kind, 1).start()

    def passing(kind):
        side(kind, 0).wait_recv()
        side(kind, 2).start()

    def targets():
        for o in (2, 3, 1):
            target(o).start()
        pl.when(chip == 0)(lambda: target_shared(2).start())
        pl.when(chip == 1)(lambda: target_shared(3).start())
        pl.when(chip == 1)(lambda: target_shared(1).start())

    greet(n, dp, [peers[1], peers[2], peers[3]], True)
    for k in offsets:
        scatter(0, k).start()
    for o in (2, 1):
        shared(o).start()
    for o in (2, 3, 1):
        own(o).start()
    for k in offsets:
        small(k).start()
    for copy in locals_:
        copy.start()
    pl.when(chip == 0)(lambda: kept().start())
    set_mask(mask_ref)
    vt_ref[:, HD:, :] = jnp.ones((HEADS, VROWS - HD, ALL * BLK), BF16)
    sum_up(0)
    for k in offsets:
        gather(0, k).start()
    for kind in (1, 2):
        for k in offsets:
            scatter(kind, k).start()
    total = pp_ref[...]
    for k in offsets:
        small(k).wait_recv()
        total = total + pslot_ref[k]
    for row in range(SMALL):
        for part in range(2):
            line = jnp.broadcast_to(total[2 * row + part : 2 * row + part + 1, :], (128, 128))
            small_ref[row * D + part * 128 : row * D + (part + 1) * 128, :] = line.T
    shared(2).wait_recv()
    shared(3).start()
    for o in (2, 3, 1):
        own(o).wait_recv()
    shared(1).wait_recv()
    for k in offsets:
        gather(0, k).wait_recv()
    side(0, 0).start()
    side(0, 1).start()
    shared(3).wait_recv()
    for copy in locals_:
        copy.wait()
    pl.when(chip == 0)(lambda: kept().wait())

    def begin(j, carry):
        xt = xo_ref[j].T
        xt_ref[j] = xt
        unit_values, _ = standardize(xt.astype(F32))
        a_ref[j] = (unit_values * param(small_ref, 0) + param(small_ref, 1)).astype(BF16)
        return carry

    lax.fori_loop(0, ALL, begin, 0)
    summed(1)
    side(0, 0).wait_recv()
    side(0, 2).start()
    side(0, 1).wait_recv()
    side(0, 2).wait_recv()
    for t in range(3):
        wt_ref[t * D : (t + 1) * D, :] = matrix(w_ref, 0, t).T
    summed(2)

    def middle(j, carry):
        pl.when(j == 5)(lambda: sharing(1))
        project(j, a_ref[j], wt_ref, q_ref, kt_ref, vt_ref, k_ref, v_ref)
        return carry

    lax.fori_loop(0, ALL, middle, 0)

    def progress(i):
        pl.when(i == 2)(lambda: sharing(2))
        pl.when(i == 3)(targets)
        pl.when(i == 4)(lambda: passing(1))
        pl.when(i == 5)(lambda: passing(2))

    attend(core, q_ref, k_ref, vt_ref, o_ref, log_ref, mask_ref, score_ref, prob_ref, progress)
    wot_ref[...] = matrix(w_ref, 0, 3).T
    for kind in (1, 2):
        side(kind, 1).wait_recv()
        side(kind, 2).wait_recv()
    for c in range(4):
        part = slice(c * D, (c + 1) * D)
        wut_ref[part, :] = matrix(w_ref, 1, c).T
        wdt_ref[:, part] = matrix(w_ref, 2, c).T

    def normal(side):
        there = a2_ref.at[OWN + core if side == 0 else OWN + 3 - core]
        return send(there, there, (ns0, ns1), side, {"seq": peers[1]})

    def store(i):
        slot, u = i % 2, ordered(i)
        return (
            pltpu.make_async_copy(hid_buf.at[slot], hid_ref.at[u], hs.at[0, slot]),
            pltpu.make_async_copy(slope_buf.at[slot], slope_ref.at[u], hs.at[1, slot]),
        )

    def feed(i, carry):
        @pl.when(i == 2)
        def _():
            normal(0).start()
            normal(1).start()

        slot = i % 2

        @pl.when(i >= 2)
        def _():
            for copy in store(i - 2):
                copy.wait()

        u = ordered(i)
        place, base = unit_place(u, core)
        x = xt_ref[base + place].astype(F32)
        r, _, _, m = forward_parts(x, o_ref[u], wot_ref, small_ref)
        r_ref[u] = r
        out = r + param(small_ref, 4)
        for c in range(FF // BLK):
            rows = slice(c * BLK, (c + 1) * BLK)
            e = dot(wut_ref[rows, :], m) + param(small_ref, 5 + c)
            hid, slope = gelu_parts(e)
            hid = hid.astype(BF16)
            hid_buf[slot, rows, :] = hid
            slope_buf[slot, rows, :] = slope.astype(BF16)
            out = out + dot(wdt_ref[:, rows], hid)
        sq_ref[u] = squares_of(out)
        z = out + x
        z_ref[u] = z
        unit_values, _ = standardize(z)
        a2_ref[base + place] = (unit_values * param(small_ref, 0) + param(small_ref, 1)).astype(BF16)
        for copy in store(i):
            copy.start()
        return carry

    lax.fori_loop(0, UNITS, feed, 0)
    for i in (UNITS - 2, UNITS - 1):
        for copy in store(i):
            copy.wait()
    normal(0).wait()
    normal(1).wait()
    for o in (2, 3, 1):
        target(o).wait()
        own(o).wait_send()
        shared(o).wait_send()

    @pl.when(chip == 0)
    def _():
        target_shared(2).wait_send()
        target_shared(3).wait_recv()

    @pl.when(chip == 1)
    def _():
        target_shared(3).wait_send()
        target_shared(1).wait_send()
        target_shared(2).wait_recv()
        target_shared(1).wait_recv()

    for kind in range(3):
        for k in offsets:
            scatter(kind, k).wait_send()
            gather(kind, k).wait_send()
        for which in range(3):
            side(kind, which).wait_send()
    for k in offsets:
        small(k).wait_send()


VM = pl.BlockSpec(memory_space=pltpu.VMEM)
HB = pl.BlockSpec(memory_space=pltpu.HBM)


def shape_of(shape, dtype=BF16):
    return jax.ShapeDtypeStruct(shape, dtype)


KEYS = [
    shape_of((HEADS, HD, ALL * BLK)),
    shape_of((2, ALL, BLK, 128)),
    shape_of((2, ALL, BLK, 128)),
]
ATTEND_SCRATCH = [
    pltpu.VMEM((BLK, BLK), F32),
    pltpu.VMEM((2, OWN, BLK, BLK), F32),
    pltpu.VMEM((2, OWN * BLK, BLK), BF16),
]
BACK_SCRATCH = [
    pltpu.VMEM((BLK, BLK), F32),
    pltpu.VMEM((2, OWN * BLK, BLK), BF16),
    pltpu.VMEM((2, OWN * BLK, BLK), BF16),
    pltpu.VMEM((HEADS, HD, ALL * BLK), F32),
    pltpu.VMEM((HEADS, HD, ALL * BLK), F32),
    pltpu.VMEM((2, OWN, BLK, BLK), BF16),
    pltpu.VMEM((2, 2, BLK, BLK), BF16),
    *pair_of_sems((2, 2)),
]


def stage_call(body, name, args, outs, scratch, mib, flops, hbm_in=(), hbm_out=(), **comm):
    return pl.pallas_call(
        body,
        in_specs=[HB if i in hbm_in else VM for i in range(len(args))],
        out_specs=[HB if i in hbm_out else VM for i in range(len(outs))],
        out_shape=outs,
        scratch_shapes=scratch,
        compiler_params=pltpu.CompilerParams(vmem_limit_bytes=mib << 20, has_side_effects=bool(comm), **comm),
        cost_estimate=cost(flops, 1 << 20),
        name=name,
    )(*args)


def first_stage(n, pk, pp, x, c):
    rows = D // n
    tile, eight = (UNITS, BLK, BLK), (ALL, BLK, BLK)
    outs = [shape_of(eight), shape_of(eight), shape_of(eight)] + KEYS
    outs += [shape_of(tile), shape_of((UNITS, 2, 8, BLK), F32), shape_of(tile, F32)]
    outs += [shape_of((UNITS, FF, BLK)), shape_of((UNITS, FF, BLK)), shape_of(tile, F32), shape_of(eight)]
    outs += [shape_of((UNITS, 8, BLK), F32), shape_of((3 * D, D)), shape_of((D, D)), shape_of((FF, D))]
    outs += [shape_of((D, FF)), shape_of((SMALL * D, 128), F32), shape_of((3, 4, n, rows, D)), shape_of(tile)]
    scratch = [pltpu.VMEM((HEADS, VROWS, ALL * BLK), BF16)] + ATTEND_SCRATCH
    scratch += [
        pltpu.VMEM(eight, BF16),
        pltpu.VMEM((3, n, rows, D), BF16),
        pltpu.VMEM((n, 24, 128), F32),
        pltpu.VMEM((3, rows, D), BF16),
        *pair_of_sems((3, n)),
        *pair_of_sems((3, n)),
        *pair_of_sems((n,)),
        *pair_of_sems((3, 3)),
        *pair_of_sems((4, 2)),
        *pair_of_sems((8,)),
        *pair_of_sems((2,)),
        pltpu.VMEM((2, FF, BLK), BF16),
        pltpu.VMEM((2, FF, BLK), BF16),
        pltpu.SemaphoreType.DMA((2, 2)),
        pltpu.SemaphoreType.DMA((4,)),
    ]
    return stage_call(
        partial(first_stage_body, n), "first_stage", [pk, pp, x, c], outs, scratch, FIRST_MIB, 8e9, hbm_in=(2, 3), hbm_out=(9, 10),
        collective_id=0,
    )


def feed_back_tail(
    u, g, gy, r_unit, r_inv, m, o, small_ref, parts, w_ref, gr_ref, go_ref, gd_acc, gu_acc, go_acc, tail_acc
):
    tail_acc[2 * D : 3 * D, :] += fold(gy.astype(F32))
    gm = jnp.zeros((D, BLK), F32)
    for c in range(FF // BLK):
        rows = slice(c * BLK, (c + 1) * BLK)
        hid, slope = parts(c)
        gd_acc[rows, :] += dot_nt(hid, gy)
        ge = (dot(matrix(w_ref, 2, c), gy) * slope).astype(BF16)
        gu_acc[:, rows] += dot_nt(m, ge)
        tail_acc[3 * D + c * BLK : 3 * D + (c + 1) * BLK, :] += fold(ge.astype(F32))
        gm = gm + dot(matrix(w_ref, 1, c), ge)
    tail_acc[0:D, :] += fold(gm * r_unit)
    tail_acc[D : 2 * D, :] += fold(gm)
    gr = g + standardize_back(gm * param(small_ref, 2), r_unit, r_inv)
    gr_ref[u] = gr
    ga = gr.astype(BF16)
    go_acc[...] += dot_nt(o, ga)
    go_ref[u] = dot(matrix(w_ref, 0, 3), ga).astype(BF16)


TAIL = 3 * D + FF


def second_stage_body(
    a_ref, z_ref, cot_ref, w_ref, wt_ref, wot_ref, wut_ref, wdt_ref, small_ref,
    final_ref, sq_ref, gr_ref, gd_acc, gu_acc, go_acc, tail_acc, dq_ref, dk_ref, dv_ref,
    q_ref, kt_ref, k_ref, v_ref, vt_ref, o_ref, log_ref, go_ref, score_ref, hid_buf, slope_buf,
    mask_ref, prob_ref, ds_ref, dk_acc, dv_acc, part_ref, got_ref, ds0, ds1,
):
    seq = lax.axis_index("seq")
    core = seq % 2
    peer = peers_of(seq)[1]
    greet(1, 0, [peer], False)
    set_mask(mask_ref)
    vt_ref[:, HD:, :] = jnp.ones((HEADS, VROWS - HD, ALL * BLK), BF16)
    for acc in (gd_acc, gu_acc, go_acc, tail_acc):
        acc[...] = jnp.zeros_like(acc)

    def begin(j, carry):
        project(j, a_ref[j], wt_ref, q_ref, kt_ref, vt_ref, k_ref, v_ref)
        return carry

    lax.fori_loop(0, ALL, begin, 0)
    attend(core, q_ref, k_ref, vt_ref, o_ref, log_ref, mask_ref, score_ref, prob_ref)

    def feed(u, carry):
        r, r_unit, r_inv, m = forward_parts(z_ref[u], o_ref[u], wot_ref, small_ref)
        out = r + param(small_ref, 4)
        for c in range(FF // BLK):
            rows = slice(c * BLK, (c + 1) * BLK)
            e = dot(wut_ref[rows, :], m) + param(small_ref, 5 + c)
            hid, slope = gelu_parts(e)
            hid = hid.astype(BF16)
            hid_buf[rows, :] = hid
            slope_buf[rows, :] = slope
            out = out + dot(wdt_ref[:, rows], hid)
        sq_ref[u] = squares_of(out)
        final_ref[u] = out.T.astype(BF16)
        gy = cot_ref[u].T
        feed_back_tail(
            u, gy.astype(F32), gy, r_unit, r_inv, m, o_ref[u], small_ref,
            lambda c: (hid_buf[c * BLK : (c + 1) * BLK, :], slope_buf[c * BLK : (c + 1) * BLK, :]),
            w_ref, gr_ref, go_ref, gd_acc, gu_acc, go_acc, tail_acc,
        )
        return carry

    lax.fori_loop(0, UNITS, feed, 0)
    attend_back(
        core, q_ref, k_ref, kt_ref, v_ref, go_ref, o_ref, log_ref, dq_ref, dk_ref, dv_ref, mask_ref, prob_ref, ds_ref, dk_acc, dv_acc,
        part_ref, got_ref, ds0, ds1, peer,
    )


def second_stage(a, z, cot, w, wt, wot, wut, wdt, small):
    tile, eight = (UNITS, BLK, BLK), (ALL, BLK, BLK)
    outs = [shape_of(tile), shape_of((UNITS, 8, BLK), F32), shape_of(tile, F32), shape_of((FF, D), F32)]
    outs += [shape_of((D, FF), F32), shape_of((D, D), F32), shape_of((TAIL, 128), F32), shape_of(tile)]
    outs += [shape_of(tile), shape_of(tile)]
    scratch = [pltpu.VMEM(eight, BF16)] + [pltpu.VMEM(s.shape, s.dtype) for s in KEYS]
    scratch += [pltpu.VMEM((HEADS, VROWS, ALL * BLK), BF16), pltpu.VMEM(tile, BF16)]
    scratch += [pltpu.VMEM((UNITS, 2, 8, BLK), F32), pltpu.VMEM(tile, BF16), ATTEND_SCRATCH[1]]
    scratch += [pltpu.VMEM((FF, BLK), BF16), pltpu.VMEM((FF, BLK), F32)] + BACK_SCRATCH
    return stage_call(
        second_stage_body, "second_stage", [a, z, cot, w, wt, wot, wut, wdt, small], outs, scratch, SECOND_MIB, 20e9,
        collective_id=1,
    )


def project_weights(a, dq, dk, dv, gqkv_acc):
    gqkv_acc[0] += dot_nt(a, dq)
    gqkv_acc[1] += dot_nt(a, dk)
    gqkv_acc[2] += dot_nt(a, dv)


def project_back(z, dq, dk, dv, gr, small_ref, w_ref, head_acc):
    grad = dot(matrix(w_ref, 0, 0), dq) + dot(matrix(w_ref, 0, 1), dk) + dot(matrix(w_ref, 0, 2), dv)
    unit_values, inverse = standardize(z)
    head_acc[0:D, :] += fold(grad * unit_values)
    head_acc[D : 2 * D, :] += fold(grad)
    return gr + standardize_back(grad * param(small_ref, 0), unit_values, inverse)


def third_stage_body(
    n, dq_in, dk_in, dv_in, a2_ref, z_ref, gr_in, hid_ref, slope_ref, r_ref, o_ref, log_ref, q_ref, kt_ref, k_ref, v_ref,
    small_ref, w_ref, gd_in, gu_in, go_in, tail_in, a_ref, xt_ref, sq1_ref, sq2_ref, f_ref,
    sum_ref, p_ref, fo_ref, io_ref,
    gz_ref, gr_ref, gd_acc, gu_acc, go_acc, tail_acc, gqkv_acc, head_acc, dq_ref, dk_ref, dv_ref, i_ref,
    g_ref, pp_ref, half_ref, quarter_ref, out_ref, mine_ref, slot_ref, chunk_ref, pslot_ref, psum_ref,
    as0, as1, bs0, bs1, ss0, ss1, rs0, rs1, gs0, gs1, ps0, ps1, xs0, xs1, us0, us1, vs0, vs1,
    go_ref, hid_buf, slope_buf, hs, mask_ref, prob_ref, ds_ref, dk_acc, dv_acc, part_ref, got_ref, ds0, ds1,
):
    dp = lax.axis_index("dp")
    seq = lax.axis_index("seq")
    chip, core = seq // 2, seq % 2
    peers = peers_of(seq)
    offsets = range(1, n)

    def half(kind, j):
        part = peers[1] if j == 0 else peers[3]
        return send(g_ref.at[kind, part], half_ref.at[kind, j], (as0, as1), (kind, j), {"seq": peers[1]})

    def cross(kind):
        return send(out_ref.at[kind], quarter_ref.at[kind], (bs0, bs1), kind, {"seq": peers[2]})

    def scatter(kind, k):
        to = (dp + k) % n
        return send(mine_ref.at[kind, to], slot_ref.at[kind, k], (ss0, ss1), (kind, k), {"dp": to})

    def gather(kind, k):
        return send(chunk_ref.at[kind], sum_ref.at[kind, seq, dp], (rs0, rs1), (kind, k), {"dp": (dp + k) % n})

    def side(kind, which):
        part = peers[2] if which == 2 else seq
        to = peers[2] if which == 0 else peers[1]
        return send(sum_ref.at[kind, part], sum_ref.at[kind, part], (gs0, gs1), (kind, which), {"seq": to})

    def chunk(kind):
        return send(chunk_ref.at[kind], sum_ref.at[kind, seq, dp], (us0, us1), kind, {"seq": peers[2]})

    def again(kind, k):
        there = sum_ref.at[kind, peers[2], dp]
        return send(there, there, (vs0, vs1), (kind, k), {"dp": (dp + k) % n})

    def small(k):
        if k == 0:
            return send(pp_ref, pslot_ref.at[0], (ps0, ps1), 0, {"seq": peers[1]})
        if k == 1:
            return send(psum_ref.at[0], pslot_ref.at[1], (ps0, ps1), 1, {"seq": peers[2]})
        return send(psum_ref.at[1], pslot_ref.at[k], (ps0, ps1), k, {"dp": (dp + k - 1) % n})

    def halves(kind):
        half(kind, 0).start()
        half(kind, 1).start()

    def crossing(kind):
        half(kind, 0).wait_recv()
        half(kind, 1).wait_recv()
        out_ref[kind] = (g_ref[kind, peers[2]].astype(F32) + half_ref[kind, 1].astype(F32)).astype(BF16)
        cross(kind).start()

    def scattering(kind):
        cross(kind).wait_recv()
        mine_ref[kind] = (
            g_ref[kind, seq].astype(F32) + half_ref[kind, 0].astype(F32) + quarter_ref[kind].astype(F32)
        ).astype(BF16)
        for k in offsets:
            scatter(kind, k).start()

    def gathering(kind):
        total = mine_ref[kind, dp].astype(F32)
        for k in offsets:
            scatter(kind, k).wait_recv()
            total = total + slot_ref[kind, k].astype(F32)
        chunk_ref[kind] = total.astype(BF16)
        sum_ref[kind, seq, dp] = total.astype(BF16)
        if kind in DOUBLE:
            chunk(kind).start()
        for k in offsets:
            gather(kind, k).start()

    def doubling(kind):
        if kind in DOUBLE:
            chunk(kind).wait_recv()
            for k in offsets:
                again(kind, k).start()

    def sharing(kind):
        for k in offsets:
            gather(kind, k).wait_recv()
        if kind not in DOUBLE:
            side(kind, 0).start()
        side(kind, 1).start()

    def passing(kind):
        if kind in DOUBLE:
            for k in offsets:
                again(kind, k).wait_recv()
        else:
            side(kind, 0).wait_recv()
        side(kind, 2).start()

    def settled(kind):
        side(kind, 1).wait_recv()
        side(kind, 2).wait_recv()

    own = 3 * chip + core

    def move(which, o, source_ref, target_ref):
        return send(source_ref.at[peers[o]], target_ref.at[own], (xs0, xs1), (which, o), {"seq": peers[o]})

    def move_shared(which, o, source_ref, target_ref):
        source = source_ref.at[4 if o == 2 else 5]
        return send(source, target_ref.at[2 if o == 3 else 5], (xs0, xs1), (which, 4 + o), {"seq": peers[o]})

    def start_moves(which, source_ref, target_ref):
        pl.when(chip == 0)(lambda: move_shared(which, 3, source_ref, target_ref).start())
        pl.when(chip == 1)(lambda: move_shared(which, 2, source_ref, target_ref).start())
        pl.when(chip == 1)(lambda: move_shared(which, 1, source_ref, target_ref).start())
        move(which, 1, source_ref, target_ref).start()
        target_ref[own] = source_ref[seq]
        pl.when(chip == 0)(lambda: target_ref.__setitem__(2, source_ref[4]))

    def more_moves(which, source_ref, target_ref):
        for o in (2, 3):
            move(which, o, source_ref, target_ref).start()

    def finish_moves(which, source_ref, target_ref):
        @pl.when(chip == 0)
        def _():
            move_shared(which, 3, source_ref, target_ref).wait_send()
            move_shared(which, 2, source_ref, target_ref).wait_recv()

        @pl.when(chip == 1)
        def _():
            move_shared(which, 2, source_ref, target_ref).wait_send()
            move_shared(which, 1, source_ref, target_ref).wait()
            move_shared(which, 3, source_ref, target_ref).wait_recv()

        for o in (2, 3, 1):
            move(which, o, source_ref, target_ref).wait()

    def fetch(u):
        slot = u % 2
        return (
            pltpu.make_async_copy(hid_ref.at[u], hid_buf.at[slot], hs.at[0, slot]),
            pltpu.make_async_copy(slope_ref.at[u], slope_buf.at[slot], hs.at[1, slot]),
        )

    split = lambda values: values.astype(BF16).reshape(g_ref.shape[2:])
    for copy in fetch(0):
        copy.start()
    greet(n, dp, [peers[1], peers[2], peers[3]], True)
    start_moves(0, f_ref, fo_ref)
    more_moves(0, f_ref, fo_ref)
    set_mask(mask_ref)
    gqkv_acc[...] = jnp.zeros_like(gqkv_acc)
    head_acc[...] = jnp.zeros_like(head_acc)
    for acc, given in ((gd_acc, gd_in), (gu_acc, gu_in), (go_acc, go_in), (tail_acc, tail_in)):
        acc[...] = given[...]

    def feed(u, carry):
        @pl.when(u < UNITS - 1)
        def _():
            for copy in fetch(u + 1):
                copy.start()

        for copy in fetch(u):
            copy.wait()
        slot = u % 2
        place, base = unit_place(u, core)
        project_weights(a2_ref[base + place], dq_in[u], dk_in[u], dv_in[u], gqkv_acc)
        g = project_back(z_ref[u], dq_in[u], dk_in[u], dv_in[u], gr_in[u], small_ref, w_ref, head_acc)
        gz_ref[u] = g
        r_unit, r_inv = standardize(r_ref[u])
        m = (r_unit * param(small_ref, 2) + param(small_ref, 3)).astype(BF16)
        feed_back_tail(
            u, g, g.astype(BF16), r_unit, r_inv, m, o_ref[u], small_ref,
            lambda c: (
                hid_buf[slot, c * BLK : (c + 1) * BLK, :],
                slope_buf[slot, c * BLK : (c + 1) * BLK, :].astype(F32),
            ),
            w_ref, gr_ref, go_ref, gd_acc, gu_acc, go_acc, tail_acc,
        )
        return carry

    lax.fori_loop(0, UNITS, feed, 0)
    for c in range(4):
        g_ref[1, c] = split(gu_acc[:, c * D : (c + 1) * D])
        g_ref[2, c] = split(gd_acc[c * D : (c + 1) * D, :])
    halves(1)
    halves(2)

    def progress(i):
        @pl.when(i == 1)
        def _():
            crossing(1)
            crossing(2)

        pl.when(i == 4)(lambda: scattering(1))
        pl.when(i == 5)(lambda: scattering(2))

    attend_back(
        core, q_ref, k_ref, kt_ref, v_ref, go_ref, o_ref, log_ref, dq_ref, dk_ref, dv_ref, mask_ref, prob_ref, ds_ref, dk_acc, dv_acc,
        part_ref, got_ref, ds0, ds1, peers[1], progress,
    )
    gathering(1)
    gathering(2)

    def early(u, carry):
        place, base = unit_place(u, core)
        project_weights(a_ref[base + place], dq_ref[u], dk_ref[u], dv_ref[u], gqkv_acc)
        return carry

    lax.fori_loop(0, UNITS, early, 0)
    for t in range(3):
        g_ref[0, t] = split(gqkv_acc[t])
    g_ref[0, 3] = split(go_acc[...])
    halves(0)

    def end(u, carry):
        pl.when(u == 1)(lambda: crossing(0))
        pl.when(u == 3)(lambda: doubling(2))
        pl.when(u == 4)(lambda: sharing(1))
        place, base = unit_place(u, core)
        g = project_back(
            xt_ref[base + place].astype(F32), dq_ref[u], dk_ref[u], dv_ref[u], gr_ref[u], small_ref, w_ref, head_acc
        )
        i_ref[u] = (g + gz_ref[u]).T.astype(BF16)
        return carry

    lax.fori_loop(0, UNITS, end, 0)
    start_moves(1, i_ref, io_ref)
    for row in range(SMALL):
        for part in range(2):
            ref, first = (head_acc, row) if row < 2 else (tail_acc, row - 2)
            first = first * D + part * 128
            pp_ref[2 * row + part : 2 * row + part + 1, :] = jnp.sum(ref[first : first + 128, :].T, axis=0, keepdims=True)
    sequences = 6 * n
    place = lax.broadcasted_iota(jnp.int32, (6, 128), 0) * 128 + lax.broadcasted_iota(jnp.int32, (6, 128), 1)
    stats = jnp.zeros((6, 128), F32)
    for i, ref in enumerate((sq1_ref, sq2_ref)):
        lines = [jnp.sum(ref[u], axis=0, keepdims=True) for u in range(UNITS)]
        mine = jnp.sum(lines[0] + lines[1] + lines[2] + lines[3], axis=1, keepdims=True)
        shared = jnp.sum(lines[4] + lines[5], axis=1, keepdims=True)
        start = i * sequences + 6 * dp + 3 * chip
        stats = jnp.where(place == start + core, jnp.broadcast_to(mine, (6, 128)), stats)
        stats = jnp.where(place == start + 2, jnp.broadcast_to(shared, (6, 128)), stats)
    pp_ref[18:24, :] = stats
    small(0).start()
    scattering(0)
    small(0).wait_recv()
    psum_ref[0] = pp_ref[...] + pslot_ref[0]
    small(1).start()
    small(1).wait_recv()
    psum_ref[1] = psum_ref[0] + pslot_ref[1]
    for k in offsets:
        small(1 + k).start()
    sharing(2)
    gathering(0)
    more_moves(1, i_ref, io_ref)
    doubling(0)
    passing(1)
    passing(2)
    total = psum_ref[1]
    for k in offsets:
        small(1 + k).wait_recv()
        total = total + pslot_ref[1 + k]
    p_ref[...] = total
    sharing(0)
    settled(1)
    settled(2)
    passing(0)
    settled(0)
    finish_moves(0, f_ref, fo_ref)
    finish_moves(1, i_ref, io_ref)
    for kind in range(3):
        half(kind, 0).wait_send()
        half(kind, 1).wait_send()
        cross(kind).wait_send()
        for k in offsets:
            scatter(kind, k).wait_send()
            gather(kind, k).wait_send()
        if kind in DOUBLE:
            chunk(kind).wait_send()
            for k in offsets:
                again(kind, k).wait_send()
        for which in (1, 2) if kind in DOUBLE else range(3):
            side(kind, which).wait_send()
    for k in range(n + 1):
        small(k).wait_send()


DOUBLE = (0, 2)


def third_stage(n, *args):
    rows = D // n
    tile = (UNITS, BLK, BLK)
    quarter = (3, n, rows, D)
    outs = [shape_of((3, 4, n, rows, D)), shape_of((24, 128), F32), shape_of(tile), shape_of(tile)]
    scratch = [
        pltpu.VMEM(tile, F32),
        pltpu.VMEM(tile, F32),
        pltpu.VMEM((FF, D), F32),
        pltpu.VMEM((D, FF), F32),
        pltpu.VMEM((D, D), F32),
        pltpu.VMEM((TAIL, 128), F32),
        pltpu.VMEM((3, D, D), F32),
        pltpu.VMEM((2 * D, 128), F32),
        pltpu.VMEM(tile, BF16),
        pltpu.VMEM(tile, BF16),
        pltpu.VMEM(tile, BF16),
        pltpu.VMEM(tile, BF16),
        pltpu.VMEM((3, 4, n, rows, D), BF16),
        pltpu.VMEM((24, 128), F32),
        pltpu.VMEM((3, 2, n, rows, D), BF16),
        pltpu.VMEM(quarter, BF16),
        pltpu.VMEM(quarter, BF16),
        pltpu.VMEM(quarter, BF16),
        pltpu.VMEM(quarter, BF16),
        pltpu.VMEM((3, rows, D), BF16),
        pltpu.VMEM((1 + n, 24, 128), F32),
        pltpu.VMEM((2, 24, 128), F32),
        *pair_of_sems((3, 2)),
        *pair_of_sems((3,)),
        *pair_of_sems((3, n)),
        *pair_of_sems((3, n)),
        *pair_of_sems((3, 3)),
        *pair_of_sems((1 + n,)),
        *pair_of_sems((2, 8)),
        *pair_of_sems((3,)),
        *pair_of_sems((3, n)),
        pltpu.VMEM(tile, BF16),
        pltpu.VMEM((2, FF, BLK), BF16),
        pltpu.VMEM((2, FF, BLK), BF16),
        pltpu.SemaphoreType.DMA((2, 2)),
        *BACK_SCRATCH,
    ]
    return stage_call(
        partial(third_stage_body, n), "third_stage", args, outs, scratch, THIRD_MIB, 20e9, hbm_in=(6, 7), collective_id=2
    )


FIRST_MIB, SECOND_MIB, THIRD_MIB, ADAM_MIB = 38, 22, 31, 58


def owner_scalars(owner_ref):
    sizes = [D * D] * 4 + [D * FF, FF * D, SMALL * D]
    starts = []
    for t in range(7):
        offset = jnp.int32(0)
        for u in range(t):
            offset = offset + jnp.where(owner_ref[u] == owner_ref[t], sizes[u], 0).astype(jnp.int32)
        starts.append(offset)
    return starts


def pack_body(owner_ref, row_ref, w_ref, p_ref):
    dp = lax.axis_index("dp")
    seq = lax.axis_index("seq")
    starts = owner_scalars(owner_ref)
    square = jnp.where(seq == 0, starts[0], jnp.where(seq == 1, starts[1], jnp.where(seq == 2, starts[2], starts[3])))
    plans = (
        (owner_ref[seq], square // 128, 2),
        (owner_ref[4], starts[4] // 128 + 2 * seq, FF // 128),
        (owner_ref[5], starts[5] // 128 + 2 * D * seq, 2),
    )
    for kind, (owner, base, stride) in enumerate(plans):
        keep = jnp.where(owner == dp, 1.0, 0.0).astype(F32)
        for side in range(2):
            values = row_ref[pl.ds(base + side, D, stride=stride), :]
            w_ref[kind, :, side * 128 : (side + 1) * 128] = (values * keep).astype(BF16)
    keep = jnp.where(owner_ref[6] == dp, 1.0, 0.0).astype(F32)
    values = row_ref[pl.ds(pl.multiple_of(starts[6] // 128, 8), 24), :] * keep
    rows = lax.broadcasted_iota(jnp.int32, (24, 128), 0)
    p_ref[...] = jnp.where(rows < 2 * SMALL, values, 0.0)


def pack(owner_list, row):
    return pl.pallas_call(
        pack_body,
        in_specs=[pl.BlockSpec(memory_space=pltpu.SMEM), pl.BlockSpec(memory_space=pltpu.VMEM)],
        out_specs=[pl.BlockSpec(memory_space=pltpu.VMEM)] * 2,
        out_shape=[jax.ShapeDtypeStruct((3, D, D), BF16), jax.ShapeDtypeStruct((24, 128), F32)],
        compiler_params=pltpu.CompilerParams(vmem_limit_bytes=20 << 20),
        cost_estimate=cost(1, 3 << 20),
        name="pack",
    )(owner_list, row)


ROWS = D * D // 128


def adam_body(owner_ref, g_ref, p_ref, f_ref, i_ref, m_ref, v_ref, w_ref, m_out, v_out, w_out, f_out, i_out, grad_ref):
    dp = lax.axis_index("dp")
    block = pl.program_id(0)
    starts = owner_scalars(owner_ref)
    counts = [1, 1, 1, 1, 4, 4, 1]
    rate = jnp.float32(D ** (-0.5))
    decay = jnp.float32(0.1)
    limit = jnp.int32(0)
    f_out[...] = f_ref[...].astype(F32)
    i_out[...] = i_ref[...].astype(F32)
    for t in range(7):
        first = starts[t] // (D * D)
        here = (owner_ref[t] == dp) & (block >= first) & (block < first + counts[t])
        part = block - first
        limit = jnp.where(here, 2 * SMALL if t == 6 else ROWS, limit)
        if t == 5:
            rate = jnp.where(here, FF ** (-0.5), rate)
        if t == 6:
            rate = jnp.where(here, 0.5, rate)
            decay = jnp.where(here, 0.0, decay)

        @pl.when(here)
        def _(t=t, part=part):
            if t == 6:
                grad_ref[0:24, :] = p_ref[...]
            elif t == 4:
                for c in range(4):
                    piece = g_ref[4 + c, pl.ds(pl.multiple_of(part * 64, 64), 64), :].astype(F32)
                    for side in range(2):
                        grad_ref[pl.ds(2 * c + side, 64, stride=8), :] = piece[:, side * 128 : (side + 1) * 128]
            else:
                for r in range(4):
                    piece = g_ref[8 + part if t == 5 else t, r * 64 : (r + 1) * 64, :].astype(F32)
                    for side in range(2):
                        grad_ref[pl.ds(r * 128 + side, 64, stride=2), :] = piece[:, side * 128 : (side + 1) * 128]

    @pl.when(limit == 0)
    def _():
        for out in (m_out, v_out, w_out):
            out[...] = jnp.zeros_like(out)

    @pl.when(limit > 0)
    def _():
        scale = 1.0 / (1.0 - 0.5**STEP)
        for r in range(0, ROWS, PIECE):
            rows = slice(r, r + PIECE)
            grad = grad_ref[rows, :]
            valid = lax.broadcasted_iota(jnp.int32, (PIECE, 128), 0) + r < limit
            first_new = 0.5 * m_ref[rows, :] + 0.5 * grad
            second_new = 0.5 * v_ref[rows, :] + 0.5 * grad * grad
            old = w_ref[rows, :]
            update = first_new * scale / (jnp.sqrt(second_new * scale) + adam_eps) + decay * old
            m_out[rows, :] = jnp.where(valid, first_new, 0.0)
            v_out[rows, :] = jnp.where(valid, second_new, 0.0)
            w_out[rows, :] = jnp.where(valid, old - rate * update, 0.0)


PIECE = 64


def adam(owner_list, g, p, f, i, m, v, w):
    blocks = m.shape[0] // ROWS
    tile = pl.BlockSpec((ROWS, 128), lambda b, t: (b, 0))
    states = pl.BlockSpec((f.shape[0] // blocks, D), lambda b, t: (b, 0))
    out = jax.ShapeDtypeStruct(m.shape, F32)
    state = jax.ShapeDtypeStruct(f.shape, F32)
    whole = pl.BlockSpec(memory_space=pltpu.VMEM)
    spec = pltpu.PrefetchScalarGridSpec(
        num_scalar_prefetch=1,
        grid=(blocks,),
        in_specs=[whole, whole, states, states, tile, tile, tile],
        out_specs=[tile, tile, tile, states, states],
        scratch_shapes=[pltpu.VMEM((ROWS, 128), F32)],
    )
    return pl.pallas_call(
        adam_body,
        grid_spec=spec,
        out_shape=[out, out, out, state, state],
        compiler_params=params_of(mib=ADAM_MIB),
        cost_estimate=cost(20 * 524288, 14 << 20),
        name="adam",
    )(owner_list, g, p, f, i, m, v, w)


def per_device(inputs, cotangent, owner_list, master_rows, moment1_rows, moment2_rows):
    n = lax.axis_size("dp")
    rows = D // n
    flat = [r.reshape(-1, 128) for r in (master_rows, moment1_rows, moment2_rows)]
    pk, pp = pack(owner_list, flat[0])
    (xt, a1, q1, kt1, k1, v1, o1, log1, r1, hid, slope, z2, a2, sq1, wt, wot, wut, wdt, small, w, cot) = first_stage(
        n, pk.reshape(3, n, rows, D), pp, inputs, cotangent
    )
    final, sq2, gr, gd, gu, gout, tail, dq, dk, dv = second_stage(a2, z2, cot, w, wt, wot, wut, wdt, small)
    g, p, final, grad = third_stage(
        n, dq, dk, dv, a2, z2, gr, hid, slope, r1, o1, log1, q1, kt1, k1, v1, small, w, gd, gu, gout, tail,
        a1, xt, sq1, sq2, final,
    )
    states = [r.reshape(-1, D) for r in (final, grad)]
    m_new, v_new, w_new, final, grad = adam(owner_list, g.reshape(12, D, D), p, *states, flat[1], flat[2], flat[0])
    sequences = inputs.shape[0] * n
    entries = inputs.shape[1] * lax.axis_size("seq") * D
    squares = p[18:].reshape(-1)[: 2 * sequences].reshape(2, sequences)
    stats = jnp.sqrt(squares / entries + stat_eps)
    back = lambda r: r.reshape(master_rows.shape)
    return (final.reshape(inputs.shape), grad.reshape(inputs.shape), stats, back(m_new), back(v_new), back(w_new))


def solution(mesh):
    placed = (P("dp", "seq", None), P("dp", "seq", None), P(), P("dp", None), P("dp", None), P("dp", None))
    return jax.shard_map(
        per_device,
        mesh=mesh,
        in_specs=placed,
        out_specs=(P("dp", "seq", None), P("dp", "seq", None), P(), P("dp", None), P("dp", None), P("dp", None)),
        check_vma=False,
    )
```

```python
import math
from functools import partial

import jax
import jax.numpy as jnp
from jax import lax
from jax.experimental import pallas as pl
from jax.experimental.pallas import tpu as pltpu
from jax.sharding import PartitionSpec as P

D = 256
HEADS = 4
HD = 64
FF = 1024
STEP = 3
SMALL = 9
BLK = 256
OWN = 4
UNITS = 6
ALL = 8
F32 = jnp.float32
BF16 = jnp.bfloat16
MESH = pl.DeviceIdType.MESH

norm_eps = 1e-05
stat_eps = 1e-06
adam_eps = 1e-08
masked_score = -1e30


def dot(left, right):
    return lax.dot_general(left, right, (((1,), (0,)), ((), ())), preferred_element_type=F32)


def dot_nt(left, right):
    return lax.dot_general(left, right, (((1,), (1,)), ((), ())), preferred_element_type=F32)


def wide(column):
    return jnp.concatenate([column, column], axis=1)


def fold(values):
    return values[:, :128] + values[:, 128:]


def standardize(values):
    average = jnp.mean(values, axis=0, keepdims=True)
    centered = values - average
    spread = jnp.mean(centered * centered, axis=0, keepdims=True)
    inverse = lax.rsqrt(spread + norm_eps)
    return centered * inverse, inverse


def standardize_back(grad, unit_values, inverse):
    average = jnp.mean(grad, axis=0, keepdims=True)
    inner = jnp.mean(grad * unit_values, axis=0, keepdims=True)
    return (grad - average - unit_values * inner) * inverse


def param(small_ref, row):
    return wide(small_ref[row * D : (row + 1) * D, :])


def gelu_parts(e):
    cdf = 0.5 * lax.erf(e * math.sqrt(0.5)) + 0.5
    hid = e * cdf
    slope = cdf + e * (jnp.exp(-0.5 * e * e) * (1.0 / math.sqrt(2.0 * math.pi)))
    return hid, slope


def full(shape):
    return pl.BlockSpec(shape, lambda *args: (0,) * len(shape), pipeline_mode=pl.Buffered(1))


def params_of(ndims=1, mib=56):
    return pltpu.CompilerParams(
        dimension_semantics=("arbitrary",) * ndims, vmem_limit_bytes=mib << 20
    )


def cost(flops, nbytes, trans=0):
    return pl.CostEstimate(flops=int(flops), bytes_accessed=int(nbytes), transcendentals=int(trans))


LOG2E = math.log2(math.e)
VROWS = HD + 16


def unit_place(unit, core):
    later = unit // OWN
    place = (1 - later) * unit + later * (core + (unit - OWN) * (3 - 2 * core))
    return place, later * OWN


def lanes(start, size):
    return pl.ds(pl.multiple_of(start, BLK), size)


def pair_rows(pair):
    return pl.ds(pl.multiple_of(pair * 128, 128), 128)


def matrix(w_ref, kind, part):
    n, rows = w_ref.shape[2:4]
    if rows % 16 == 0:
        return w_ref[kind, part].reshape(D, D)
    return jnp.concatenate([w_ref[kind, part, i] for i in range(n)], axis=0)


def peers_of(seq):
    return {1: seq + 1 - 2 * (seq % 2), 2: (seq + 2) % 4, 3: 3 - seq}


def greet(n, dp, peers, wide_group):
    barrier = pltpu.get_barrier_semaphore()
    count = 0
    for peer in peers:
        pl.semaphore_signal(barrier, inc=1, device_id={"seq": peer}, device_id_type=MESH)
        count += 1
    if wide_group:
        for k in range(1, n):
            pl.semaphore_signal(barrier, inc=1, device_id={"dp": (dp + k) % n}, device_id_type=MESH)
            count += 1
    pl.semaphore_wait(barrier, count)


def send(source, target, sems, index, device):
    return pltpu.make_async_remote_copy(
        src_ref=source,
        dst_ref=target,
        send_sem=sems[0].at[index],
        recv_sem=sems[1].at[index],
        device_id=device,
        device_id_type=MESH,
    )


def pair_of_sems(shape):
    return [pltpu.SemaphoreType.DMA(shape), pltpu.SemaphoreType.DMA(shape)]


def project(j, a, wt_ref, q_ref, kt_ref, vt_ref, k_ref, v_ref):
    where = lanes(j * BLK, BLK)
    q_ref[j] = (dot(wt_ref[0:D], a) * HD ** (-0.5)).astype(BF16)
    kt = dot(wt_ref[D : 2 * D], a).astype(BF16)
    vt = dot(wt_ref[2 * D : 3 * D], a).astype(BF16)
    for h in range(HEADS):
        kt_ref[h, :, where] = kt[h * HD : (h + 1) * HD]
        vt_ref[h, 0:HD, where] = vt[h * HD : (h + 1) * HD]
    k = kt.T
    v = vt.T
    for h in range(2):
        k_ref[h, j] = k[:, h * 128 : (h + 1) * 128]
        v_ref[h, j] = v[:, h * 128 : (h + 1) * 128]


def head_rows(values, half):
    rows = lax.broadcasted_iota(jnp.int32, values.shape, 0)
    keep = (rows < HD) if half == 0 else (rows >= HD)
    return jnp.where(keep, values, jnp.zeros_like(values))


def set_mask(mask_ref):
    keys = lax.broadcasted_iota(jnp.int32, (BLK, BLK), 0)
    queries = lax.broadcasted_iota(jnp.int32, (BLK, BLK), 1)
    mask_ref[...] = jnp.where(keys <= queries, 0.0, masked_score)


def groups(values, op):
    out = values[0:8]
    for i in range(1, values.shape[0] // 8):
        out = op(out, values[i * 8 : (i + 1) * 8])
    return out


SUB = 128
BSUB = 256


def ordered(i):
    return (i + OWN) % UNITS


def attend(core, q_ref, k_ref, vt_ref, o_ref, log_ref, mask_ref, score_ref, prob_ref, progress=None):
    def step(i, carry):
        if progress is not None:
            progress(i)
        unit = ordered(i)
        place, base = unit_place(unit, core)

        def branch(last):
            keys = (last + 1) * BLK
            chunks = [(kb, sub) for kb in range(last + 1) for sub in range(BLK // SUB)]
            queries = [head_rows(q_ref[base + place, (h // 2) * 128 : (h // 2 + 1) * 128, :], h % 2) for h in range(HEADS)]
            tops = [None] * HEADS
            outs = [None] * HEADS

            def scores(h, kb, sub):
                rows = slice(sub * SUB, (sub + 1) * SUB)
                score = dot(k_ref[h // 2, base + kb, rows, :], queries[h])
                if kb == last:
                    score = score + mask_ref[rows, :]
                score_ref[h % 2, kb, rows, :] = score
                peak = groups(score, jnp.maximum)
                tops[h] = peak if tops[h] is None else jnp.maximum(tops[h], peak)

            def weights(h, kb, sub):
                rows = slice(sub * SUB, (sub + 1) * SUB)
                weight = jnp.exp(score_ref[h % 2, kb, rows, :] - tops[h])
                prob_ref[h % 2, kb * BLK + sub * SUB : kb * BLK + (sub + 1) * SUB, :] = weight.astype(BF16)

            def mixed(h, kb):
                part = dot(vt_ref[h, :, lanes((base + kb) * BLK, BLK)], prob_ref[h % 2, kb * BLK : (kb + 1) * BLK, :])
                outs[h] = part if outs[h] is None else outs[h] + part

            for t in range(HEADS + 2):
                if 0 <= t - 1 < HEADS:
                    tops[t - 1] = jnp.max(tops[t - 1], axis=0, keepdims=True)
                for kb, sub in chunks:
                    if t < HEADS:
                        scores(t, kb, sub)
                    if 0 <= t - 1 < HEADS:
                        weights(t - 1, kb, sub)
                    if 0 <= t - 2 < HEADS and sub == 0:
                        mixed(t - 2, kb)
                if 0 <= t - 2 < HEADS:
                    h = t - 2
                    total = outs[h][HD : HD + 1]
                    o_ref[unit, h * HD : (h + 1) * HD, :] = (outs[h][0:HD] / total).astype(BF16)
                    log_ref[unit, h // 2, h % 2 : h % 2 + 1, :] = tops[h] + jnp.log(total)

        for last in range(OWN):
            pl.when(place == last)(partial(branch, last))
        return carry

    lax.fori_loop(0, UNITS, step, 0)


def attend_back(
    core, q_ref, k_ref, kt_ref, v_ref, go_ref, o_ref, log_ref, dq_ref, dk_ref, dv_ref, mask_ref, prob_ref, slope_ref, dk_acc, dv_acc,
    part_ref, got_ref, ds0, ds1, peer, progress=None,
):
    dk_acc[...] = jnp.zeros_like(dk_acc)
    dv_acc[...] = jnp.zeros_like(dv_acc)
    pairs = ((0, dk_acc, dk_ref), (1, dv_acc, dv_ref))

    def piece(acc, j):
        return acc[:, :, j * BLK : (j + 1) * BLK].reshape(D, BLK)

    def swap(which, side):
        position = 1 - core if side == 0 else 2 + core
        return send(part_ref.at[which, position], got_ref.at[which, side], (ds0, ds1), (which, side), {"seq": peer})

    def step(i, carry):
        @pl.when(i == 2)
        def _():
            for which, acc, _ in pairs:
                for position in range(OWN):
                    part_ref[which, position] = piece(acc, OWN + position).astype(BF16)
            for which in range(2):
                for side in range(2):
                    swap(which, side).start()

        if progress is not None:
            progress(i)
        unit = ordered(i)
        place, base = unit_place(unit, core)

        def branch(last):
            chunks = [(kb, sub) for kb in range(last + 1) for sub in range(BLK // BSUB)]
            heads = []
            for h in range(HEADS):
                pair = slice((h // 2) * 128, (h // 2 + 1) * 128)
                block = q_ref[base + place, pair, :]
                go_block = go_ref[unit, pair, :]
                mine = slice((h % 2) * HD, (h % 2 + 1) * HD)
                inner = jnp.sum(
                    go_block[mine].astype(F32) * o_ref[unit, h * HD : (h + 1) * HD, :].astype(F32), axis=0, keepdims=True
                )
                heads.append(
                    (head_rows(block, h % 2), head_rows(go_block, h % 2), log_ref[unit, h // 2, h % 2 : h % 2 + 1, :], inner)
                )
            dqs = [None] * HEADS
            ready = {}

            def products(h, kb, sub):
                rows = slice(sub * BSUB, (sub + 1) * BSUB)
                q, go, _, _ = heads[h]
                ready[h, kb, sub] = (
                    dot(k_ref[h // 2, base + kb, rows, :], q),
                    dot(v_ref[h // 2, base + kb, rows, :], go),
                )

            def elements(h, kb, sub):
                rows = slice(sub * BSUB, (sub + 1) * BSUB)
                to = slice(kb * BLK + sub * BSUB, kb * BLK + (sub + 1) * BSUB)
                _, _, log_total, inner = heads[h]
                score, slope = ready.pop((h, kb, sub))
                if kb == last:
                    score = score + mask_ref[rows, :]
                weight = jnp.exp(score - log_total)
                prob_ref[h % 2, to, :] = weight.astype(BF16)
                slope_ref[h % 2, to, :] = (weight * (slope - inner)).astype(BF16)

            def gradients(h, kb, which):
                rows = slice(kb * BLK, (kb + 1) * BLK)
                where = lanes((base + kb) * BLK, BLK)
                head = slice(h * HD, (h + 1) * HD)
                if which == 0:
                    dv_acc[h, :, where] += dot_nt(go_ref[unit, head, :], prob_ref[h % 2, rows, :])
                elif which == 1:
                    dk_acc[h, :, where] += dot_nt(q_ref[base + place, head, :], slope_ref[h % 2, rows, :])
                else:
                    part = dot(kt_ref[h, :, where], slope_ref[h % 2, rows, :])
                    dqs[h] = part if dqs[h] is None else dqs[h] + part

            work = [(h, kb, sub) for h in range(HEADS) for kb, sub in chunks]
            per = BLK // BSUB
            products(*work[0])
            for at, (h, kb, sub) in enumerate(work):
                if at + 1 < len(work):
                    products(*work[at + 1])
                elements(h, kb, sub)
                if h > 0 and sub == 0:
                    for which in range(3):
                        gradients(h - 1, kb, which)
                if h > 0 and kb == last and sub == per - 1:
                    dq_ref[unit, (h - 1) * HD : h * HD, :] = (dqs[h - 1] * HD ** (-0.5)).astype(BF16)
            for kb in range(last + 1):
                for which in range(3):
                    gradients(HEADS - 1, kb, which)
            dq_ref[unit, (HEADS - 1) * HD :, :] = (dqs[HEADS - 1] * HD ** (-0.5)).astype(BF16)

        for last in range(OWN):
            pl.when(place == last)(partial(branch, last))
        return carry

    lax.fori_loop(0, UNITS, step, 0)
    for which, acc, ref in pairs:
        for j in range(OWN):
            ref[j] = piece(acc, j).astype(BF16)
    for which, acc, ref in pairs:
        for side, position in enumerate((core, 3 - core)):
            swap(which, side).wait()
            ref[OWN + side] = (part_ref[which, position].astype(F32) + got_ref[which, side].astype(F32)).astype(BF16)


def forward_parts(z, o, wot_ref, small_ref):
    r = z + dot(wot_ref[...], o)
    unit_values, inverse = standardize(r)
    m = (unit_values * param(small_ref, 2) + param(small_ref, 3)).astype(BF16)
    return r, unit_values, inverse, m


def squares_of(out):
    return groups(out * out, jnp.add)


def first_stage_body(
    n, pk_ref, pp_ref, x_ref, c_ref,
    xt_ref, a_ref, q_ref, kt_ref, k_ref, v_ref, o_ref, log_ref, r_ref, hid_ref, slope_ref, z_ref, a2_ref, sq_ref,
    wt_ref, wot_ref, wut_ref, wdt_ref, small_ref, w_ref, co_ref,
    vt_ref, mask_ref, score_ref, prob_ref, xo_ref, slot_ref, pslot_ref, chunk_ref,
    ss0, ss1, rs0, rs1, ps0, ps1, gs0, gs1, xs0, xs1, cs0, cs1, ns0, ns1, hid_buf, slope_buf, r_buf, hs, ls,
):
    dp = lax.axis_index("dp")
    seq = lax.axis_index("seq")
    chip, core = seq // 2, seq % 2
    peers = peers_of(seq)

    def scatter(kind, k):
        to = (dp + k) % n
        return send(pk_ref.at[kind, to], slot_ref.at[kind, k], (ss0, ss1), (kind, k), {"dp": to})

    def small(k):
        return send(pp_ref, pslot_ref.at[k], (ps0, ps1), k, {"dp": (dp + k) % n})

    def gather(kind, k):
        return send(chunk_ref.at[kind], w_ref.at[kind, seq, dp], (rs0, rs1), (kind, k), {"dp": (dp + k) % n})

    def side(kind, which):
        part = peers[2] if which == 2 else seq
        to = peers[2] if which == 0 else peers[1]
        return send(w_ref.at[kind, part], w_ref.at[kind, part], (gs0, gs1), (kind, which), {"seq": to})

    def own(o):
        to = peers[o]
        return send(x_ref.at[3 * (to // 2) + to % 2], xo_ref.at[seq], (xs0, xs1), (o, 0), {"seq": to})

    def shared(o):
        if o == 3:
            there = xo_ref.at[OWN + peers[2]]
            return send(there, there, (xs0, xs1), (3, 1), {"seq": peers[1]})
        to = peers[o]
        return send(x_ref.at[3 * (to // 2) + 2], xo_ref.at[OWN + seq], (xs0, xs1), (o, 1), {"seq": to})

    def target(o):
        to = peers[o]
        return send(c_ref.at[3 * (to // 2) + to % 2], co_ref.at[seq], (cs0, cs1), o, {"seq": to})

    def target_shared(o):
        slot = 4 if o == 2 else 5
        return send(c_ref.at[2 if o == 3 else 5], co_ref.at[slot], (cs0, cs1), 4 + o, {"seq": peers[o]})

    def sum_up(kind):
        total = pk_ref[kind, dp].astype(F32)
        for k in range(1, n):
            scatter(kind, k).wait_recv()
            total = total + slot_ref[kind, k].astype(F32)
        chunk_ref[kind] = total.astype(BF16)
        w_ref[kind, seq, dp] = total.astype(BF16)

    def kept():
        return pltpu.make_async_copy(c_ref.at[2], co_ref.at[4], ls.at[3])

    locals_ = (
        pltpu.make_async_copy(x_ref.at[3 * chip + core], xo_ref.at[seq], ls.at[0]),
        pltpu.make_async_copy(x_ref.at[3 * chip + 2], xo_ref.at[OWN + seq], ls.at[1]),
        pltpu.make_async_copy(c_ref.at[3 * chip + core], co_ref.at[seq], ls.at[2]),
    )
    offsets = range(1, n)

    def summed(kind):
        sum_up(kind)
        for k in offsets:
            gather(kind, k).start()

    def sharing(kind):
        for k in offsets:
            gather(kind, k).wait_recv()
        side(kind, 0).start()
        side(kind, 1).start()

    def passing(kind):
        side(kind, 0).wait_recv()
        side(kind, 2).start()

    def targets():
        for o in (2, 3, 1):
            target(o).start()
        pl.when(chip == 0)(lambda: target_shared(2).start())
        pl.when(chip == 1)(lambda: target_shared(3).start())
        pl.when(chip == 1)(lambda: target_shared(1).start())

    greet(n, dp, [peers[1], peers[2], peers[3]], True)
    for k in offsets:
        scatter(0, k).start()
    for o in (2, 1):
        shared(o).start()
    for o in (2, 3, 1):
        own(o).start()
    for k in offsets:
        small(k).start()
    for copy in locals_:
        copy.start()
    pl.when(chip == 0)(lambda: kept().start())
    set_mask(mask_ref)
    vt_ref[:, HD:, :] = jnp.ones((HEADS, VROWS - HD, ALL * BLK), BF16)
    sum_up(0)
    for k in offsets:
        gather(0, k).start()
    for kind in (1, 2):
        for k in offsets:
            scatter(kind, k).start()
    total = pp_ref[...]
    for k in offsets:
        small(k).wait_recv()
        total = total + pslot_ref[k]
    for row in range(SMALL):
        for part in range(2):
            line = jnp.broadcast_to(total[2 * row + part : 2 * row + part + 1, :], (128, 128))
            small_ref[row * D + part * 128 : row * D + (part + 1) * 128, :] = line.T
    shared(2).wait_recv()
    shared(3).start()
    for o in (2, 3, 1):
        own(o).wait_recv()
    shared(1).wait_recv()
    for k in offsets:
        gather(0, k).wait_recv()
    side(0, 0).start()
    side(0, 1).start()
    shared(3).wait_recv()
    for copy in locals_:
        copy.wait()
    pl.when(chip == 0)(lambda: kept().wait())

    def begin(j, carry):
        xt = xo_ref[j].T
        xt_ref[j] = xt
        unit_values, _ = standardize(xt.astype(F32))
        a_ref[j] = (unit_values * param(small_ref, 0) + param(small_ref, 1)).astype(BF16)
        return carry

    lax.fori_loop(0, ALL, begin, 0)
    summed(1)
    side(0, 0).wait_recv()
    side(0, 2).start()
    side(0, 1).wait_recv()
    side(0, 2).wait_recv()
    for t in range(3):
        wt_ref[t * D : (t + 1) * D, :] = matrix(w_ref, 0, t).T
    summed(2)

    def middle(j, carry):
        pl.when(j == 5)(lambda: sharing(1))
        project(j, a_ref[j], wt_ref, q_ref, kt_ref, vt_ref, k_ref, v_ref)
        return carry

    lax.fori_loop(0, ALL, middle, 0)

    def progress(i):
        pl.when(i == 2)(lambda: sharing(2))
        pl.when(i == 3)(targets)
        pl.when(i == 4)(lambda: passing(1))
        pl.when(i == 5)(lambda: passing(2))

    attend(core, q_ref, k_ref, vt_ref, o_ref, log_ref, mask_ref, score_ref, prob_ref, progress)
    wot_ref[...] = matrix(w_ref, 0, 3).T
    for kind in (1, 2):
        side(kind, 1).wait_recv()
        side(kind, 2).wait_recv()
    for c in range(4):
        part = slice(c * D, (c + 1) * D)
        wut_ref[part, :] = matrix(w_ref, 1, c).T
        wdt_ref[:, part] = matrix(w_ref, 2, c).T

    def normal(side):
        there = a2_ref.at[OWN + core if side == 0 else OWN + 3 - core]
        return send(there, there, (ns0, ns1), side, {"seq": peers[1]})

    def store(i):
        slot, u = i % 2, ordered(i)
        return (
            pltpu.make_async_copy(hid_buf.at[slot], hid_ref.at[u], hs.at[0, slot]),
            pltpu.make_async_copy(slope_buf.at[slot], slope_ref.at[u], hs.at[1, slot]),
            pltpu.make_async_copy(r_buf.at[slot], r_ref.at[u], hs.at[2, slot]),
        )

    def feed(i, carry):
        @pl.when(i == 2)
        def _():
            normal(0).start()
            normal(1).start()

        slot = i % 2

        @pl.when(i >= 2)
        def _():
            for copy in store(i - 2):
                copy.wait()

        u = ordered(i)
        place, base = unit_place(u, core)
        x = xt_ref[base + place].astype(F32)
        r, _, _, m = forward_parts(x, o_ref[u], wot_ref, small_ref)
        r_buf[slot] = r
        out = r + param(small_ref, 4)
        for c in range(FF // BLK):
            rows = slice(c * BLK, (c + 1) * BLK)
            e = dot(wut_ref[rows, :], m) + param(small_ref, 5 + c)
            hid, slope = gelu_parts(e)
            hid = hid.astype(BF16)
            hid_buf[slot, rows, :] = hid
            slope_buf[slot, rows, :] = slope.astype(BF16)
            out = out + dot(wdt_ref[:, rows], hid)
        sq_ref[u] = squares_of(out)
        z = out + x
        z_ref[u] = z
        unit_values, _ = standardize(z)
        a2_ref[base + place] = (unit_values * param(small_ref, 0) + param(small_ref, 1)).astype(BF16)
        for copy in store(i):
            copy.start()
        return carry

    lax.fori_loop(0, UNITS, feed, 0)
    for i in (UNITS - 2, UNITS - 1):
        for copy in store(i):
            copy.wait()
    normal(0).wait()
    normal(1).wait()
    for o in (2, 3, 1):
        target(o).wait()
        own(o).wait_send()
        shared(o).wait_send()

    @pl.when(chip == 0)
    def _():
        target_shared(2).wait_send()
        target_shared(3).wait_recv()

    @pl.when(chip == 1)
    def _():
        target_shared(3).wait_send()
        target_shared(1).wait_send()
        target_shared(2).wait_recv()
        target_shared(1).wait_recv()

    for kind in range(3):
        for k in offsets:
            scatter(kind, k).wait_send()
            gather(kind, k).wait_send()
        for which in range(3):
            side(kind, which).wait_send()
    for k in offsets:
        small(k).wait_send()


VM = pl.BlockSpec(memory_space=pltpu.VMEM)
HB = pl.BlockSpec(memory_space=pltpu.HBM)


def shape_of(shape, dtype=BF16):
    return jax.ShapeDtypeStruct(shape, dtype)


KEYS = [
    shape_of((HEADS, HD, ALL * BLK)),
    shape_of((2, ALL, BLK, 128)),
    shape_of((2, ALL, BLK, 128)),
]
ATTEND_SCRATCH = [
    pltpu.VMEM((BLK, BLK), F32),
    pltpu.VMEM((2, OWN, BLK, BLK), F32),
    pltpu.VMEM((2, OWN * BLK, BLK), BF16),
]
BACK_SCRATCH = [
    pltpu.VMEM((BLK, BLK), F32),
    pltpu.VMEM((2, OWN * BLK, BLK), BF16),
    pltpu.VMEM((2, OWN * BLK, BLK), BF16),
    pltpu.VMEM((HEADS, HD, ALL * BLK), F32),
    pltpu.VMEM((HEADS, HD, ALL * BLK), F32),
    pltpu.VMEM((2, OWN, BLK, BLK), BF16),
    pltpu.VMEM((2, 2, BLK, BLK), BF16),
    *pair_of_sems((2, 2)),
]


def stage_call(body, name, args, outs, scratch, mib, flops, hbm_in=(), hbm_out=(), **comm):
    return pl.pallas_call(
        body,
        in_specs=[HB if i in hbm_in else VM for i in range(len(args))],
        out_specs=[HB if i in hbm_out else VM for i in range(len(outs))],
        out_shape=outs,
        scratch_shapes=scratch,
        compiler_params=pltpu.CompilerParams(vmem_limit_bytes=mib << 20, has_side_effects=bool(comm), **comm),
        cost_estimate=cost(flops, 1 << 20),
        name=name,
    )(*args)


def first_stage(n, pk, pp, x, c):
    rows = D // n
    tile, eight = (UNITS, BLK, BLK), (ALL, BLK, BLK)
    outs = [shape_of(eight), shape_of(eight), shape_of(eight)] + KEYS
    outs += [shape_of(tile), shape_of((UNITS, 2, 8, BLK), F32), shape_of(tile, F32)]
    outs += [shape_of((UNITS, FF, BLK)), shape_of((UNITS, FF, BLK)), shape_of(tile, F32), shape_of(eight)]
    outs += [shape_of((UNITS, 8, BLK), F32), shape_of((3 * D, D)), shape_of((D, D)), shape_of((FF, D))]
    outs += [shape_of((D, FF)), shape_of((SMALL * D, 128), F32), shape_of((3, 4, n, rows, D)), shape_of(tile)]
    scratch = [pltpu.VMEM((HEADS, VROWS, ALL * BLK), BF16)] + ATTEND_SCRATCH
    scratch += [
        pltpu.VMEM(eight, BF16),
        pltpu.VMEM((3, n, rows, D), BF16),
        pltpu.VMEM((n, 24, 128), F32),
        pltpu.VMEM((3, rows, D), BF16),
        *pair_of_sems((3, n)),
        *pair_of_sems((3, n)),
        *pair_of_sems((n,)),
        *pair_of_sems((3, 3)),
        *pair_of_sems((4, 2)),
        *pair_of_sems((8,)),
        *pair_of_sems((2,)),
        pltpu.VMEM((2, FF, BLK), BF16),
        pltpu.VMEM((2, FF, BLK), BF16),
        pltpu.VMEM((2, BLK, BLK), F32),
        pltpu.SemaphoreType.DMA((3, 2)),
        pltpu.SemaphoreType.DMA((4,)),
    ]
    return stage_call(
        partial(first_stage_body, n), "first_stage", [pk, pp, x, c], outs, scratch, FIRST_MIB, 8e9, hbm_in=(2, 3), hbm_out=(8, 9, 10),
        collective_id=0,
    )


def feed_back_tail(
    u, g, gy, r_unit, r_inv, m, o, small_ref, parts, w_ref, gr_ref, go_ref, gd_acc, gu_acc, go_acc, tail_acc
):
    tail_acc[2 * D : 3 * D, :] += fold(gy.astype(F32))
    gm = jnp.zeros((D, BLK), F32)
    for c in range(FF // BLK):
        rows = slice(c * BLK, (c + 1) * BLK)
        hid, slope = parts(c)
        gd_acc[rows, :] += dot_nt(hid, gy)
        ge = (dot(matrix(w_ref, 2, c), gy) * slope).astype(BF16)
        gu_acc[:, rows] += dot_nt(m, ge)
        tail_acc[3 * D + c * BLK : 3 * D + (c + 1) * BLK, :] += fold(ge.astype(F32))
        gm = gm + dot(matrix(w_ref, 1, c), ge)
    tail_acc[0:D, :] += fold(gm * r_unit)
    tail_acc[D : 2 * D, :] += fold(gm)
    gr = g + standardize_back(gm * param(small_ref, 2), r_unit, r_inv)
    gr_ref[u] = gr
    ga = gr.astype(BF16)
    go_acc[...] += dot_nt(o, ga)
    go_ref[u] = dot(matrix(w_ref, 0, 3), ga).astype(BF16)


TAIL = 3 * D + FF


def second_stage_body(
    a_ref, z_ref, cot_ref, w_ref, wt_ref, wot_ref, wut_ref, wdt_ref, small_ref,
    final_ref, sq_ref, gr_ref, gd_acc, gu_acc, go_acc, tail_acc, dq_ref, dk_ref, dv_ref,
    q_ref, kt_ref, k_ref, v_ref, vt_ref, o_ref, log_ref, go_ref, score_ref, hid_buf, slope_buf,
    mask_ref, prob_ref, ds_ref, dk_acc, dv_acc, part_ref, got_ref, ds0, ds1,
):
    seq = lax.axis_index("seq")
    core = seq % 2
    peer = peers_of(seq)[1]
    greet(1, 0, [peer], False)
    set_mask(mask_ref)
    vt_ref[:, HD:, :] = jnp.ones((HEADS, VROWS - HD, ALL * BLK), BF16)
    for acc in (gd_acc, gu_acc, go_acc, tail_acc):
        acc[...] = jnp.zeros_like(acc)

    def begin(j, carry):
        project(j, a_ref[j], wt_ref, q_ref, kt_ref, vt_ref, k_ref, v_ref)
        return carry

    lax.fori_loop(0, ALL, begin, 0)
    attend(core, q_ref, k_ref, vt_ref, o_ref, log_ref, mask_ref, score_ref, prob_ref)

    def feed(u, carry):
        r, r_unit, r_inv, m = forward_parts(z_ref[u], o_ref[u], wot_ref, small_ref)
        out = r + param(small_ref, 4)
        for c in range(FF // BLK):
            rows = slice(c * BLK, (c + 1) * BLK)
            e = dot(wut_ref[rows, :], m) + param(small_ref, 5 + c)
            hid, slope = gelu_parts(e)
            hid = hid.astype(BF16)
            hid_buf[rows, :] = hid
            slope_buf[rows, :] = slope
            out = out + dot(wdt_ref[:, rows], hid)
        sq_ref[u] = squares_of(out)
        final_ref[u] = out.T.astype(BF16)
        gy = cot_ref[u].T
        feed_back_tail(
            u, gy.astype(F32), gy, r_unit, r_inv, m, o_ref[u], small_ref,
            lambda c: (hid_buf[c * BLK : (c + 1) * BLK, :], slope_buf[c * BLK : (c + 1) * BLK, :]),
            w_ref, gr_ref, go_ref, gd_acc, gu_acc, go_acc, tail_acc,
        )
        return carry

    lax.fori_loop(0, UNITS, feed, 0)
    attend_back(
        core, q_ref, k_ref, kt_ref, v_ref, go_ref, o_ref, log_ref, dq_ref, dk_ref, dv_ref, mask_ref, prob_ref, ds_ref, dk_acc, dv_acc,
        part_ref, got_ref, ds0, ds1, peer,
    )


def second_stage(a, z, cot, w, wt, wot, wut, wdt, small):
    tile, eight = (UNITS, BLK, BLK), (ALL, BLK, BLK)
    outs = [shape_of(tile), shape_of((UNITS, 8, BLK), F32), shape_of(tile, F32), shape_of((FF, D), F32)]
    outs += [shape_of((D, FF), F32), shape_of((D, D), F32), shape_of((TAIL, 128), F32), shape_of(tile)]
    outs += [shape_of(tile), shape_of(tile)]
    scratch = [pltpu.VMEM(eight, BF16)] + [pltpu.VMEM(s.shape, s.dtype) for s in KEYS]
    scratch += [pltpu.VMEM((HEADS, VROWS, ALL * BLK), BF16), pltpu.VMEM(tile, BF16)]
    scratch += [pltpu.VMEM((UNITS, 2, 8, BLK), F32), pltpu.VMEM(tile, BF16), ATTEND_SCRATCH[1]]
    scratch += [pltpu.VMEM((FF, BLK), BF16), pltpu.VMEM((FF, BLK), F32)] + BACK_SCRATCH
    return stage_call(
        second_stage_body, "second_stage", [a, z, cot, w, wt, wot, wut, wdt, small], outs, scratch, SECOND_MIB, 20e9,
        collective_id=1,
    )


def project_weights(a, dq, dk, dv, gqkv_acc):
    gqkv_acc[0] += dot_nt(a, dq)
    gqkv_acc[1] += dot_nt(a, dk)
    gqkv_acc[2] += dot_nt(a, dv)


def project_back(z, dq, dk, dv, gr, small_ref, w_ref, head_acc):
    grad = dot(matrix(w_ref, 0, 0), dq) + dot(matrix(w_ref, 0, 1), dk) + dot(matrix(w_ref, 0, 2), dv)
    unit_values, inverse = standardize(z)
    head_acc[0:D, :] += fold(grad * unit_values)
    head_acc[D : 2 * D, :] += fold(grad)
    return gr + standardize_back(grad * param(small_ref, 0), unit_values, inverse)


def third_stage_body(
    n, dq_in, dk_in, dv_in, a2_ref, z_ref, gr_in, hid_ref, slope_ref, r_ref, o_ref, log_ref, q_ref, kt_ref, k_ref, v_ref,
    small_ref, w_ref, gd_in, gu_in, go_in, tail_in, a_ref, xt_ref, sq1_ref, sq2_ref, f_ref,
    sum_ref, p_ref, fo_ref, io_ref,
    gz_ref, gr_ref, gd_acc, gu_acc, go_acc, tail_acc, gqkv_acc, head_acc, dq_ref, dk_ref, dv_ref, i_ref,
    g_ref, pp_ref, half_ref, quarter_ref, out_ref, mine_ref, slot_ref, chunk_ref, pslot_ref, psum_ref,
    as0, as1, bs0, bs1, ss0, ss1, rs0, rs1, gs0, gs1, ps0, ps1, xs0, xs1, us0, us1, vs0, vs1,
    go_ref, hid_buf, slope_buf, r_buf, hs, mask_ref, prob_ref, ds_ref, dk_acc, dv_acc, part_ref, got_ref, ds0, ds1,
):
    dp = lax.axis_index("dp")
    seq = lax.axis_index("seq")
    chip, core = seq // 2, seq % 2
    peers = peers_of(seq)
    offsets = range(1, n)

    def half(kind, j):
        part = peers[1] if j == 0 else peers[3]
        return send(g_ref.at[kind, part], half_ref.at[kind, j], (as0, as1), (kind, j), {"seq": peers[1]})

    def cross(kind):
        return send(out_ref.at[kind], quarter_ref.at[kind], (bs0, bs1), kind, {"seq": peers[2]})

    def scatter(kind, k):
        to = (dp + k) % n
        return send(mine_ref.at[kind, to], slot_ref.at[kind, k], (ss0, ss1), (kind, k), {"dp": to})

    def gather(kind, k):
        return send(chunk_ref.at[kind], sum_ref.at[kind, seq, dp], (rs0, rs1), (kind, k), {"dp": (dp + k) % n})

    def side(kind, which):
        part = peers[2] if which == 2 else seq
        to = peers[2] if which == 0 else peers[1]
        return send(sum_ref.at[kind, part], sum_ref.at[kind, part], (gs0, gs1), (kind, which), {"seq": to})

    def chunk(kind):
        return send(chunk_ref.at[kind], sum_ref.at[kind, seq, dp], (us0, us1), kind, {"seq": peers[2]})

    def again(kind, k):
        there = sum_ref.at[kind, peers[2], dp]
        return send(there, there, (vs0, vs1), (kind, k), {"dp": (dp + k) % n})

    def small(k):
        if k == 0:
            return send(pp_ref, pslot_ref.at[0], (ps0, ps1), 0, {"seq": peers[1]})
        if k == 1:
            return send(psum_ref.at[0], pslot_ref.at[1], (ps0, ps1), 1, {"seq": peers[2]})
        return send(psum_ref.at[1], pslot_ref.at[k], (ps0, ps1), k, {"dp": (dp + k - 1) % n})

    def halves(kind):
        half(kind, 0).start()
        half(kind, 1).start()

    def crossing(kind):
        half(kind, 0).wait_recv()
        half(kind, 1).wait_recv()
        out_ref[kind] = (g_ref[kind, peers[2]].astype(F32) + half_ref[kind, 1].astype(F32)).astype(BF16)
        cross(kind).start()

    def scattering(kind):
        cross(kind).wait_recv()
        mine_ref[kind] = (
            g_ref[kind, seq].astype(F32) + half_ref[kind, 0].astype(F32) + quarter_ref[kind].astype(F32)
        ).astype(BF16)
        for k in offsets:
            scatter(kind, k).start()

    def gathering(kind):
        total = mine_ref[kind, dp].astype(F32)
        for k in offsets:
            scatter(kind, k).wait_recv()
            total = total + slot_ref[kind, k].astype(F32)
        chunk_ref[kind] = total.astype(BF16)
        sum_ref[kind, seq, dp] = total.astype(BF16)
        if kind in DOUBLE:
            chunk(kind).start()
        for k in offsets:
            gather(kind, k).start()

    def doubling(kind):
        if kind in DOUBLE:
            chunk(kind).wait_recv()
            for k in offsets:
                again(kind, k).start()

    def sharing(kind):
        for k in offsets:
            gather(kind, k).wait_recv()
        if kind not in DOUBLE:
            side(kind, 0).start()
        side(kind, 1).start()

    def passing(kind):
        if kind in DOUBLE:
            for k in offsets:
                again(kind, k).wait_recv()
        else:
            side(kind, 0).wait_recv()
        side(kind, 2).start()

    def settled(kind):
        side(kind, 1).wait_recv()
        side(kind, 2).wait_recv()

    own = 3 * chip + core

    def move(which, o, source_ref, target_ref):
        return send(source_ref.at[peers[o]], target_ref.at[own], (xs0, xs1), (which, o), {"seq": peers[o]})

    def move_shared(which, o, source_ref, target_ref):
        source = source_ref.at[4 if o == 2 else 5]
        return send(source, target_ref.at[2 if o == 3 else 5], (xs0, xs1), (which, 4 + o), {"seq": peers[o]})

    def start_moves(which, source_ref, target_ref):
        pl.when(chip == 0)(lambda: move_shared(which, 3, source_ref, target_ref).start())
        pl.when(chip == 1)(lambda: move_shared(which, 2, source_ref, target_ref).start())
        pl.when(chip == 1)(lambda: move_shared(which, 1, source_ref, target_ref).start())
        move(which, 1, source_ref, target_ref).start()
        target_ref[own] = source_ref[seq]
        pl.when(chip == 0)(lambda: target_ref.__setitem__(2, source_ref[4]))

    def more_moves(which, source_ref, target_ref):
        for o in (2, 3):
            move(which, o, source_ref, target_ref).start()

    def finish_moves(which, source_ref, target_ref):
        @pl.when(chip == 0)
        def _():
            move_shared(which, 3, source_ref, target_ref).wait_send()
            move_shared(which, 2, source_ref, target_ref).wait_recv()

        @pl.when(chip == 1)
        def _():
            move_shared(which, 2, source_ref, target_ref).wait_send()
            move_shared(which, 1, source_ref, target_ref).wait()
            move_shared(which, 3, source_ref, target_ref).wait_recv()

        for o in (2, 3, 1):
            move(which, o, source_ref, target_ref).wait()

    def fetch(u):
        slot = u % 2
        return (
            pltpu.make_async_copy(hid_ref.at[u], hid_buf.at[slot], hs.at[0, slot]),
            pltpu.make_async_copy(slope_ref.at[u], slope_buf.at[slot], hs.at[1, slot]),
            pltpu.make_async_copy(r_ref.at[u], r_buf.at[slot], hs.at[2, slot]),
        )

    split = lambda values: values.astype(BF16).reshape(g_ref.shape[2:])
    for copy in fetch(0):
        copy.start()
    greet(n, dp, [peers[1], peers[2], peers[3]], True)
    start_moves(0, f_ref, fo_ref)
    more_moves(0, f_ref, fo_ref)
    set_mask(mask_ref)
    gqkv_acc[...] = jnp.zeros_like(gqkv_acc)
    head_acc[...] = jnp.zeros_like(head_acc)
    for acc, given in ((gd_acc, gd_in), (gu_acc, gu_in), (go_acc, go_in), (tail_acc, tail_in)):
        acc[...] = given[...]

    def feed(u, carry):
        @pl.when(u < UNITS - 1)
        def _():
            for copy in fetch(u + 1):
                copy.start()

        for copy in fetch(u):
            copy.wait()
        slot = u % 2
        place, base = unit_place(u, core)
        project_weights(a2_ref[base + place], dq_in[u], dk_in[u], dv_in[u], gqkv_acc)
        g = project_back(z_ref[u], dq_in[u], dk_in[u], dv_in[u], gr_in[u], small_ref, w_ref, head_acc)
        gz_ref[u] = g
        r_unit, r_inv = standardize(r_buf[slot])
        m = (r_unit * param(small_ref, 2) + param(small_ref, 3)).astype(BF16)
        feed_back_tail(
            u, g, g.astype(BF16), r_unit, r_inv, m, o_ref[u], small_ref,
            lambda c: (
                hid_buf[slot, c * BLK : (c + 1) * BLK, :],
                slope_buf[slot, c * BLK : (c + 1) * BLK, :].astype(F32),
            ),
            w_ref, gr_ref, go_ref, gd_acc, gu_acc, go_acc, tail_acc,
        )
        return carry

    lax.fori_loop(0, UNITS, feed, 0)
    for c in range(4):
        g_ref[1, c] = split(gu_acc[:, c * D : (c + 1) * D])
        g_ref[2, c] = split(gd_acc[c * D : (c + 1) * D, :])
    halves(1)
    halves(2)

    def progress(i):
        @pl.when(i == 1)
        def _():
            crossing(1)
            crossing(2)

        pl.when(i == 4)(lambda: scattering(1))
        pl.when(i == 5)(lambda: scattering(2))

    attend_back(
        core, q_ref, k_ref, kt_ref, v_ref, go_ref, o_ref, log_ref, dq_ref, dk_ref, dv_ref, mask_ref, prob_ref, ds_ref, dk_acc, dv_acc,
        part_ref, got_ref, ds0, ds1, peers[1], progress,
    )
    gathering(1)
    gathering(2)

    def early(u, carry):
        place, base = unit_place(u, core)
        project_weights(a_ref[base + place], dq_ref[u], dk_ref[u], dv_ref[u], gqkv_acc)
        return carry

    lax.fori_loop(0, UNITS, early, 0)
    for t in range(3):
        g_ref[0, t] = split(gqkv_acc[t])
    g_ref[0, 3] = split(go_acc[...])
    halves(0)

    def end(u, carry):
        pl.when(u == 1)(lambda: crossing(0))
        pl.when(u == 3)(lambda: doubling(2))
        pl.when(u == 4)(lambda: sharing(1))
        place, base = unit_place(u, core)
        g = project_back(
            xt_ref[base + place].astype(F32), dq_ref[u], dk_ref[u], dv_ref[u], gr_ref[u], small_ref, w_ref, head_acc
        )
        i_ref[u] = (g + gz_ref[u]).T.astype(BF16)
        return carry

    lax.fori_loop(0, UNITS, end, 0)
    start_moves(1, i_ref, io_ref)
    for row in range(SMALL):
        for part in range(2):
            ref, first = (head_acc, row) if row < 2 else (tail_acc, row - 2)
            first = first * D + part * 128
            pp_ref[2 * row + part : 2 * row + part + 1, :] = jnp.sum(ref[first : first + 128, :].T, axis=0, keepdims=True)
    sequences = 6 * n
    place = lax.broadcasted_iota(jnp.int32, (6, 128), 0) * 128 + lax.broadcasted_iota(jnp.int32, (6, 128), 1)
    stats = jnp.zeros((6, 128), F32)
    for i, ref in enumerate((sq1_ref, sq2_ref)):
        lines = [jnp.sum(ref[u], axis=0, keepdims=True) for u in range(UNITS)]
        mine = jnp.sum(lines[0] + lines[1] + lines[2] + lines[3], axis=1, keepdims=True)
        shared = jnp.sum(lines[4] + lines[5], axis=1, keepdims=True)
        start = i * sequences + 6 * dp + 3 * chip
        stats = jnp.where(place == start + core, jnp.broadcast_to(mine, (6, 128)), stats)
        stats = jnp.where(place == start + 2, jnp.broadcast_to(shared, (6, 128)), stats)
    pp_ref[18:24, :] = stats
    small(0).start()
    scattering(0)
    small(0).wait_recv()
    psum_ref[0] = pp_ref[...] + pslot_ref[0]
    small(1).start()
    small(1).wait_recv()
    psum_ref[1] = psum_ref[0] + pslot_ref[1]
    for k in offsets:
        small(1 + k).start()
    sharing(2)
    gathering(0)
    more_moves(1, i_ref, io_ref)
    doubling(0)
    passing(1)
    passing(2)
    total = psum_ref[1]
    for k in offsets:
        small(1 + k).wait_recv()
        total = total + pslot_ref[1 + k]
    p_ref[...] = total
    sharing(0)
    settled(1)
    settled(2)
    passing(0)
    settled(0)
    finish_moves(0, f_ref, fo_ref)
    finish_moves(1, i_ref, io_ref)
    for kind in range(3):
        half(kind, 0).wait_send()
        half(kind, 1).wait_send()
        cross(kind).wait_send()
        for k in offsets:
            scatter(kind, k).wait_send()
            gather(kind, k).wait_send()
        if kind in DOUBLE:
            chunk(kind).wait_send()
            for k in offsets:
                again(kind, k).wait_send()
        for which in (1, 2) if kind in DOUBLE else range(3):
            side(kind, which).wait_send()
    for k in range(n + 1):
        small(k).wait_send()


DOUBLE = (0, 2)


def third_stage(n, *args):
    rows = D // n
    tile = (UNITS, BLK, BLK)
    quarter = (3, n, rows, D)
    outs = [shape_of((3, 4, n, rows, D)), shape_of((24, 128), F32), shape_of(tile), shape_of(tile)]
    scratch = [
        pltpu.VMEM(tile, F32),
        pltpu.VMEM(tile, F32),
        pltpu.VMEM((FF, D), F32),
        pltpu.VMEM((D, FF), F32),
        pltpu.VMEM((D, D), F32),
        pltpu.VMEM((TAIL, 128), F32),
        pltpu.VMEM((3, D, D), F32),
        pltpu.VMEM((2 * D, 128), F32),
        pltpu.VMEM(tile, BF16),
        pltpu.VMEM(tile, BF16),
        pltpu.VMEM(tile, BF16),
        pltpu.VMEM(tile, BF16),
        pltpu.VMEM((3, 4, n, rows, D), BF16),
        pltpu.VMEM((24, 128), F32),
        pltpu.VMEM((3, 2, n, rows, D), BF16),
        pltpu.VMEM(quarter, BF16),
        pltpu.VMEM(quarter, BF16),
        pltpu.VMEM(quarter, BF16),
        pltpu.VMEM(quarter, BF16),
        pltpu.VMEM((3, rows, D), BF16),
        pltpu.VMEM((1 + n, 24, 128), F32),
        pltpu.VMEM((2, 24, 128), F32),
        *pair_of_sems((3, 2)),
        *pair_of_sems((3,)),
        *pair_of_sems((3, n)),
        *pair_of_sems((3, n)),
        *pair_of_sems((3, 3)),
        *pair_of_sems((1 + n,)),
        *pair_of_sems((2, 8)),
        *pair_of_sems((3,)),
        *pair_of_sems((3, n)),
        pltpu.VMEM(tile, BF16),
        pltpu.VMEM((2, FF, BLK), BF16),
        pltpu.VMEM((2, FF, BLK), BF16),
        pltpu.VMEM((2, BLK, BLK), F32),
        pltpu.SemaphoreType.DMA((3, 2)),
        *BACK_SCRATCH,
    ]
    return stage_call(
        partial(third_stage_body, n), "third_stage", args, outs, scratch, THIRD_MIB, 20e9, hbm_in=(6, 7, 8), collective_id=2
    )


FIRST_MIB, SECOND_MIB, THIRD_MIB, ADAM_MIB = 36, 21, 31, 58


def owner_scalars(owner_ref):
    sizes = [D * D] * 4 + [D * FF, FF * D, SMALL * D]
    starts = []
    for t in range(7):
        offset = jnp.int32(0)
        for u in range(t):
            offset = offset + jnp.where(owner_ref[u] == owner_ref[t], sizes[u], 0).astype(jnp.int32)
        starts.append(offset)
    return starts


def pack_body(owner_ref, row_ref, w_ref, p_ref):
    dp = lax.axis_index("dp")
    seq = lax.axis_index("seq")
    starts = owner_scalars(owner_ref)
    square = jnp.where(seq == 0, starts[0], jnp.where(seq == 1, starts[1], jnp.where(seq == 2, starts[2], starts[3])))
    plans = (
        (owner_ref[seq], square // 128, 2),
        (owner_ref[4], starts[4] // 128 + 2 * seq, FF // 128),
        (owner_ref[5], starts[5] // 128 + 2 * D * seq, 2),
    )
    for kind, (owner, base, stride) in enumerate(plans):
        keep = jnp.where(owner == dp, 1.0, 0.0).astype(F32)
        for side in range(2):
            values = row_ref[pl.ds(base + side, D, stride=stride), :]
            w_ref[kind, :, side * 128 : (side + 1) * 128] = (values * keep).astype(BF16)
    keep = jnp.where(owner_ref[6] == dp, 1.0, 0.0).astype(F32)
    values = row_ref[pl.ds(pl.multiple_of(starts[6] // 128, 8), 24), :] * keep
    rows = lax.broadcasted_iota(jnp.int32, (24, 128), 0)
    p_ref[...] = jnp.where(rows < 2 * SMALL, values, 0.0)


def pack(owner_list, row):
    return pl.pallas_call(
        pack_body,
        in_specs=[pl.BlockSpec(memory_space=pltpu.SMEM), pl.BlockSpec(memory_space=pltpu.VMEM)],
        out_specs=[pl.BlockSpec(memory_space=pltpu.VMEM)] * 2,
        out_shape=[jax.ShapeDtypeStruct((3, D, D), BF16), jax.ShapeDtypeStruct((24, 128), F32)],
        compiler_params=pltpu.CompilerParams(vmem_limit_bytes=20 << 20),
        cost_estimate=cost(1, 3 << 20),
        name="pack",
    )(owner_list, row)


ROWS = D * D // 128


def adam_body(
    owner_ref, g_ref, p_ref, f_ref, i_ref, m_ref, v_ref, w_ref, m_out, v_out, w_out, f_out, i_out,
    row_buf, state_buf, grad_ref, ins, outs, states,
):
    dp = lax.axis_index("dp")
    starts = owner_scalars(owner_ref)
    counts = [1, 1, 1, 1, 4, 4, 1]
    blocks = m_ref.shape[0] // ROWS

    def rows_of(block):
        return pl.ds(pl.multiple_of(block * ROWS, ROWS), ROWS)

    def reads(block):
        return [
            pltpu.make_async_copy(ref.at[rows_of(block)], row_buf.at[j, block], ins.at[j, block])
            for j, ref in enumerate((m_ref, v_ref, w_ref))
        ]

    def writes(block):
        return [
            pltpu.make_async_copy(row_buf.at[j, block], ref.at[rows_of(block)], outs.at[j, block])
            for j, ref in enumerate((m_out, v_out, w_out))
        ]

    widened = [
        pltpu.make_async_copy(state_buf.at[j], ref, states.at[j]) for j, ref in enumerate((f_out, i_out))
    ]
    for block in range(blocks):
        for copy in reads(block):
            copy.start()
    for j, ref in enumerate((f_ref, i_ref)):
        for u in range(UNITS):
            state_buf[j, u] = ref[u].astype(F32)
        widened[j].start()

    def step(block, carry):
        rate = jnp.float32(D ** (-0.5))
        decay = jnp.float32(0.1)
        limit = jnp.int32(0)
        for t in range(7):
            first = starts[t] // (D * D)
            here = (owner_ref[t] == dp) & (block >= first) & (block < first + counts[t])
            part = block - first
            limit = jnp.where(here, 2 * SMALL if t == 6 else ROWS, limit)
            if t == 5:
                rate = jnp.where(here, FF ** (-0.5), rate)
            if t == 6:
                rate = jnp.where(here, 0.5, rate)
                decay = jnp.where(here, 0.0, decay)

            @pl.when(here)
            def _(t=t, part=part):
                if t == 6:
                    grad_ref[0:24, :] = p_ref[...]
                elif t == 4:
                    for c in range(4):
                        piece = g_ref[4 + c, pl.ds(pl.multiple_of(part * 64, 64), 64), :].astype(F32)
                        for side in range(2):
                            grad_ref[pl.ds(2 * c + side, 64, stride=8), :] = piece[:, side * 128 : (side + 1) * 128]
                else:
                    for r in range(4):
                        piece = g_ref[8 + part if t == 5 else t, r * 64 : (r + 1) * 64, :].astype(F32)
                        for side in range(2):
                            grad_ref[pl.ds(r * 128 + side, 64, stride=2), :] = piece[:, side * 128 : (side + 1) * 128]

        for copy in reads(block):
            copy.wait()

        @pl.when(limit == 0)
        def _():
            row_buf[:, block] = jnp.zeros((3, ROWS, 128), F32)

        @pl.when(limit > 0)
        def _():
            scale = 1.0 / (1.0 - 0.5**STEP)
            for r in range(0, ROWS, PIECE):
                rows = slice(r, r + PIECE)
                grad = grad_ref[rows, :]
                valid = lax.broadcasted_iota(jnp.int32, (PIECE, 128), 0) + r < limit
                first_new = 0.5 * row_buf[0, block, rows, :] + 0.5 * grad
                second_new = 0.5 * row_buf[1, block, rows, :] + 0.5 * grad * grad
                old = row_buf[2, block, rows, :]
                update = first_new * scale / (jnp.sqrt(second_new * scale) + adam_eps) + decay * old
                row_buf[0, block, rows, :] = jnp.where(valid, first_new, 0.0)
                row_buf[1, block, rows, :] = jnp.where(valid, second_new, 0.0)
                row_buf[2, block, rows, :] = jnp.where(valid, old - rate * update, 0.0)

        for copy in writes(block):
            copy.start()
        return carry

    lax.fori_loop(0, blocks, step, 0)
    for block in range(blocks):
        for copy in writes(block):
            copy.wait()
    for copy in widened:
        copy.wait()


PIECE = 64


def adam(owner_list, g, p, f, i, m, v, w):
    blocks = m.shape[0] // ROWS
    outs = [jax.ShapeDtypeStruct(m.shape, F32)] * 3 + [jax.ShapeDtypeStruct(f.shape, F32)] * 2
    return pl.pallas_call(
        adam_body,
        in_specs=[pl.BlockSpec(memory_space=pltpu.SMEM)] + [VM] * 4 + [HB] * 3,
        out_specs=[HB] * 5,
        out_shape=outs,
        scratch_shapes=[
            pltpu.VMEM((3, blocks, ROWS, 128), F32),
            pltpu.VMEM((2, *f.shape), F32),
            pltpu.VMEM((ROWS, 128), F32),
            pltpu.SemaphoreType.DMA((3, blocks)),
            pltpu.SemaphoreType.DMA((3, blocks)),
            pltpu.SemaphoreType.DMA((2,)),
        ],
        compiler_params=pltpu.CompilerParams(vmem_limit_bytes=ADAM_MIB << 20),
        cost_estimate=cost(20 * 524288, 14 << 20),
        name="adam",
    )(owner_list, g, p, f, i, m, v, w)


def per_device(inputs, cotangent, owner_list, master_rows, moment1_rows, moment2_rows):
    n = lax.axis_size("dp")
    rows = D // n
    flat = [r.reshape(-1, 128) for r in (master_rows, moment1_rows, moment2_rows)]
    pk, pp = pack(owner_list, flat[0])
    (xt, a1, q1, kt1, k1, v1, o1, log1, r1, hid, slope, z2, a2, sq1, wt, wot, wut, wdt, small, w, cot) = first_stage(
        n, pk.reshape(3, n, rows, D), pp, inputs, cotangent
    )
    final, sq2, gr, gd, gu, gout, tail, dq, dk, dv = second_stage(a2, z2, cot, w, wt, wot, wut, wdt, small)
    g, p, final, grad = third_stage(
        n, dq, dk, dv, a2, z2, gr, hid, slope, r1, o1, log1, q1, kt1, k1, v1, small, w, gd, gu, gout, tail,
        a1, xt, sq1, sq2, final,
    )
    m_new, v_new, w_new, final, grad = adam(owner_list, g.reshape(12, D, D), p, final, grad, flat[1], flat[2], flat[0])
    sequences = inputs.shape[0] * n
    entries = inputs.shape[1] * lax.axis_size("seq") * D
    squares = p[18:].reshape(-1)[: 2 * sequences].reshape(2, sequences)
    stats = jnp.sqrt(squares / entries + stat_eps)
    back = lambda r: r.reshape(master_rows.shape)
    return (final.reshape(inputs.shape), grad.reshape(inputs.shape), stats, back(m_new), back(v_new), back(w_new))


def solution(mesh):
    placed = (P("dp", "seq", None), P("dp", "seq", None), P(), P("dp", None), P("dp", None), P("dp", None))
    return jax.shard_map(
        per_device,
        mesh=mesh,
        in_specs=placed,
        out_specs=(P("dp", "seq", None), P("dp", "seq", None), P(), P("dp", None), P("dp", None), P("dp", None)),
        check_vma=False,
    )
```
